8 devices in a mesh: dp: 1 (over z), ei: 2 (over y), eo: 4 (over x, core).
Axes of the slice: x: 2, y: 2, z: 1, core: 2. Of those that a mesh axis runs over, the one named last changes fastest.
Arguments:
- x_tokens: bfloat16 [512, 1024], P(('dp', 'ei', 'eo'))
- expert_idx: int32 [512, 8], P(('dp', 'ei', 'eo'))
- gate_vals: float32 [512, 8], P(('dp', 'ei', 'eo'))
- dy_tokens: bfloat16 [512, 1024], P(('dp', 'ei', 'eo'))
- w_gate: bfloat16 [32, 1024, 512], P(('ei', 'eo'))
- w_up: bfloat16 [32, 1024, 512], P(('ei', 'eo'))
- w_down: bfloat16 [32, 512, 1024], P(('ei', 'eo'))
- x_attn: bfloat16 [8, 64, 1024], P(('dp', 'ei', 'eo'))
- w_query: bfloat16 [1024, 16, 64], P(None, ('ei', 'eo'))
- w_key: bfloat16 [1024, 8, 64], P(None, ('ei', 'eo'))
- w_value: bfloat16 [1024, 8, 64], P(None, ('ei', 'eo'))
- w_out: bfloat16 [16, 64, 1024], P(('ei', 'eo'))
Outputs:
- output 1: bfloat16 [512, 1024], P(('dp', 'ei', 'eo'))
- output 2: bfloat16 [512, 1024], P(('dp', 'ei', 'eo'))
- output 3: float32 [512, 8], P(('dp', 'ei', 'eo'))
- output 4: float32 [32, 1024, 512], P(('dp', 'ei', 'eo'))
- output 5: float32 [32, 1024, 512], P(('dp', 'ei', 'eo'))
- output 6: float32 [32, 512, 1024], P(('dp', 'ei', 'eo'))
- output 7: bfloat16 [8, 64, 1024], P(('dp', 'ei', 'eo'))
All inputs are finite; a program needn't handle non-finite values.
Results may differ from the reference program's by a relative error of at most 0.0135428.
Values are sent between devices in bfloat16 or wider.
A program may use at most 1 GiB of HBM per device.

```python
import jax
import jax.numpy as jnp
import numpy as np
from jax import lax

TOKENS_DEV = 64
SEQ_LEN = 64
NUM_SRC = 8
D_MODEL = 1024
D_FF = 512
EXPERTS = 32
TOP_K = 8
HEADS = 16
KV_HEADS = 8
HEAD_DIM = 64
CAP_MULT = 4

NUM_TOK = NUM_SRC * TOKENS_DEV
NUM_SEQ = NUM_TOK // SEQ_LEN
CAP_SRC = min(TOKENS_DEV, CAP_MULT * TOKENS_DEV * TOP_K // EXPERTS)
CAP_ALL = NUM_SRC * CAP_SRC


def routing_table(key):
    per_dev = TOKENS_DEV * TOP_K
    hot_num = max(1, per_dev // (2 * CAP_SRC))
    rest_asg = per_dev - hot_num * CAP_SRC
    cold_num = EXPERTS - hot_num
    base_cnt = rest_asg // cold_num
    extra_num = rest_asg - base_cnt * cold_num
    counts = np.array([CAP_SRC] * hot_num + [base_cnt + 1] * extra_num + [base_cnt] * (cold_num - extra_num))
    expert_seq = jnp.asarray(np.repeat(np.arange(EXPERTS), counts), dtype=jnp.int32)

    def one_device(dev_key):
        key_perm, key_rows = jax.random.split(dev_key)
        relabel = jax.random.permutation(key_perm, EXPERTS).astype(jnp.int32)
        table = relabel[expert_seq].reshape(TOP_K, TOKENS_DEV).T
        return table[jax.random.permutation(key_rows, TOKENS_DEV)]

    return jax.vmap(one_device)(jax.random.split(key, NUM_SRC)).reshape(NUM_TOK, TOP_K)


def setup_inputs(seed: int = 0, part: int = 0) -> dict:
    shared_key, part_root = jax.random.split(jax.random.key(seed))
    part_keys = jax.random.split(jax.random.fold_in(part_root, part), 5)
    w_keys = jax.random.split(shared_key, 7)

    def normal_bf16(key, shape, scale):
        return (jax.random.normal(key, shape, jnp.float32) * scale).astype(jnp.bfloat16)

    return {
        'x_tokens': normal_bf16(part_keys[0], (NUM_TOK, D_MODEL), 1.0),
        'expert_idx': routing_table(part_keys[1]),
        'gate_vals': jax.random.uniform(part_keys[2], (NUM_TOK, TOP_K), jnp.float32, 0.05, 0.3),
        'dy_tokens': normal_bf16(part_keys[3], (NUM_TOK, D_MODEL), 1.0),
        'w_gate': normal_bf16(w_keys[0], (EXPERTS, D_MODEL, D_FF), D_MODEL ** -0.5),
        'w_up': normal_bf16(w_keys[1], (EXPERTS, D_MODEL, D_FF), D_MODEL ** -0.5),
        'w_down': normal_bf16(w_keys[2], (EXPERTS, D_FF, D_MODEL), D_FF ** -0.5),
        'x_attn': normal_bf16(part_keys[4], (NUM_SEQ, SEQ_LEN, D_MODEL), 1.0),
        'w_query': normal_bf16(w_keys[3], (D_MODEL, HEADS, HEAD_DIM), D_MODEL ** -0.5),
        'w_key': normal_bf16(w_keys[4], (D_MODEL, KV_HEADS, HEAD_DIM), D_MODEL ** -0.5),
        'w_value': normal_bf16(w_keys[5], (D_MODEL, KV_HEADS, HEAD_DIM), D_MODEL ** -0.5),
        'w_out': normal_bf16(w_keys[6], (HEADS, HEAD_DIM, D_MODEL), (HEADS * HEAD_DIM) ** -0.5),
    }


def moe_part(x_tokens, expert_idx, gate_vals, dy_tokens, w_gate, w_up, w_down):
    num_asg = NUM_TOK * TOP_K
    flat_exp = expert_idx.reshape(num_asg)
    onehot = (flat_exp[:, None] == jnp.arange(EXPERTS, dtype=jnp.int32)[None, :]).astype(jnp.int32)
    ranks = jnp.sum((jnp.cumsum(onehot, axis=0) - 1) * onehot, axis=1)
    slot_owner = jnp.full((EXPERTS * CAP_ALL,), num_asg, jnp.int32)
    slot_owner = slot_owner.at[flat_exp * CAP_ALL + ranks].set(jnp.arange(num_asg, dtype=jnp.int32)).reshape(EXPERTS, CAP_ALL)
    slot_tok = jnp.where(slot_owner < num_asg, slot_owner // TOP_K, NUM_TOK)
    zero_row = jnp.zeros((1, D_MODEL), x_tokens.dtype)
    x_pad = jnp.concatenate([x_tokens, zero_row])
    dy_pad = jnp.concatenate([dy_tokens, zero_row])
    gate_pad = jnp.concatenate([gate_vals.reshape(num_asg), jnp.zeros((1,), gate_vals.dtype)])

    def expert_step(carry, per_exp):
        y_acc, dx_acc, dg_acc = carry
        owner_e, tok_e, w_one, w_three, w_two = per_exp
        x_rows = x_pad[tok_e]
        dy_rows = dy_pad[tok_e].astype(jnp.float32)
        gate_e = gate_pad[owner_e][:, None]
        pre_gate = jnp.dot(x_rows, w_one, preferred_element_type=jnp.float32)
        pre_up = jnp.dot(x_rows, w_three, preferred_element_type=jnp.float32)
        sigmoid_g = jax.nn.sigmoid(pre_gate)
        act_gate = pre_gate * sigmoid_g
        hidden = (act_gate * pre_up).astype(jnp.bfloat16)
        out_wide = jnp.dot(hidden, w_two, preferred_element_type=jnp.float32).astype(jnp.bfloat16).astype(jnp.float32)
        y_acc = y_acc.at[tok_e].add(gate_e * out_wide, mode='drop')
        dg_acc = dg_acc.at[owner_e].add(jnp.sum(dy_rows * out_wide, axis=1), mode='drop')
        d_out = (gate_e * dy_rows).astype(jnp.bfloat16)
        d_hidden = jnp.dot(d_out, w_two.T, preferred_element_type=jnp.float32).astype(jnp.bfloat16).astype(jnp.float32)
        d_pre_gate = (d_hidden * pre_up * sigmoid_g * (1.0 + pre_gate * (1.0 - sigmoid_g))).astype(jnp.bfloat16)
        d_pre_up = (d_hidden * act_gate).astype(jnp.bfloat16)
        d_rows = (jnp.dot(d_pre_gate, w_one.T, preferred_element_type=jnp.float32) + jnp.dot(d_pre_up, w_three.T, preferred_element_type=jnp.float32)).astype(jnp.bfloat16)
        dx_acc = dx_acc.at[tok_e].add(d_rows.astype(jnp.float32), mode='drop')
        grads = (jnp.dot(x_rows.T, d_pre_gate, preferred_element_type=jnp.float32), jnp.dot(x_rows.T, d_pre_up, preferred_element_type=jnp.float32), jnp.dot(hidden.T, d_out, preferred_element_type=jnp.float32))
        return (y_acc, dx_acc, dg_acc), grads

    init = (jnp.zeros((NUM_TOK, D_MODEL), jnp.float32), jnp.zeros((NUM_TOK, D_MODEL), jnp.float32), jnp.zeros((num_asg,), jnp.float32))
    (y_acc, dx_acc, dg_acc), (dw_gate, dw_up, dw_down) = lax.scan(expert_step, init, (slot_owner, slot_tok, w_gate, w_up, w_down))
    return y_acc.astype(jnp.bfloat16), dx_acc.astype(jnp.bfloat16), dg_acc.reshape(NUM_TOK, TOP_K), dw_gate, dw_up, dw_down


def attention_part(x_attn, w_query, w_key, w_value, w_out):
    groups = HEADS // KV_HEADS
    causal = jnp.arange(SEQ_LEN)[:, None] >= jnp.arange(SEQ_LEN)[None, :]
    wq_f32 = w_query.astype(jnp.float32)
    wk_f32 = w_key.astype(jnp.float32)
    wv_f32 = w_value.astype(jnp.float32)
    wo_f32 = w_out.astype(jnp.float32)

    def one_seq(seq_x):
        x_f32 = seq_x.astype(jnp.float32)
        query = jnp.einsum('ld,dhe->lhe', x_f32, wq_f32).astype(jnp.bfloat16).reshape(SEQ_LEN, KV_HEADS, groups, HEAD_DIM)
        keys_h = jnp.einsum('ld,dke->lke', x_f32, wk_f32).astype(jnp.bfloat16)
        vals_h = jnp.einsum('ld,dke->lke', x_f32, wv_f32).astype(jnp.bfloat16)
        scores = jnp.einsum('qkge,ske->kgqs', query.astype(jnp.float32), keys_h.astype(jnp.float32)) * HEAD_DIM ** -0.5
        scores = jnp.where(causal, scores, -1e30)
        probs = jax.nn.softmax(scores, axis=-1).astype(jnp.bfloat16)
        context = jnp.einsum('kgqs,ske->qkge', probs.astype(jnp.float32), vals_h.astype(jnp.float32)).astype(jnp.bfloat16)
        context = context.reshape(SEQ_LEN, HEADS, HEAD_DIM)
        return jnp.einsum('qhe,hed->qd', context.astype(jnp.float32), wo_f32).astype(jnp.bfloat16)

    return lax.map(one_seq, x_attn)


def reference(x_tokens, expert_idx, gate_vals, dy_tokens, w_gate, w_up, w_down, x_attn, w_query, w_key, w_value, w_out):
    y_tokens, dx_tokens, d_gates, dw_gate, dw_up, dw_down = moe_part(x_tokens, expert_idx, gate_vals, dy_tokens, w_gate, w_up, w_down)
    attn_out = attention_part(x_attn, w_query, w_key, w_value, w_out)
    return (y_tokens, dx_tokens, d_gates, dw_gate, dw_up, dw_down, attn_out)
```

```python
import functools

import jax
import jax.numpy as jnp
from jax import lax
from jax.experimental import pallas as pl
from jax.experimental.pallas import tpu as pltpu
from jax.sharding import PartitionSpec as P

MESH = pl.DeviceIdType.MESH
GROUP_AXES = ('ei', 'eo')
TOKEN_AXES = ('dp', 'ei', 'eo')
BF = jnp.bfloat16
F32 = jnp.float32

ROWS = 64
TOK = 512
D = 1024
FF = 512
HALF = 512
EXP = 4
TOPK = 8
GATHER_COPIES = 9
RS_COPIES = 8
XA, XT, DY = 0, 1, 2

NT = (((1,), (1,)), ((), ()))
TN = (((0,), (0,)), ((), ()))


def exchange_kernel(x_hbm, dy_hbm, xa_hbm, idx_ref, gate_ref, wg_hbm, wu_hbm, wd_hbm, wqkv_hbm, wo_hbm,
                    y_out, dx_out, dg_out, at_out, xall_out, dyall_out, h_out, da_out, db_out, gt_out,
                    rows, wg, wu, wd, wqkv, wo, hid, dag, dbg, act, gfac, gt, gpad, gsend, grecv,
                    dgs, dsend, drecv, dpad,
                    part, pair, s1, r1, s2, r2,
                    in_sem, w_sem, out_sem, gs_sem, gr_sem, rs_s, rs_r, ag_s, ag_r, dd_s, dd_r):
    y = lax.axis_index('ei')
    o = lax.axis_index('eo')
    z = lax.axis_index('dp')
    x = o // 2
    c = o % 2
    me = y * 4 + o
    q0 = 2 * y + x
    qx = 2 * y + (1 - x)
    qy = 2 * (1 - y) + x
    qd = 2 * (1 - y) + (1 - x)

    def dev(fx, fy, fc):
        xx = (1 - x) if fx else x
        yy = (1 - y) if fy else y
        cc = (1 - c) if fc else c
        return (z, yy, xx * 2 + cc)

    sib, xn, yn = dev(0, 0, 1), dev(1, 0, 0), dev(0, 1, 0)
    rels = [(fx, fy, fc) for fx in (0, 1) for fy in (0, 1) for fc in (0, 1) if fx or fy or fc]

    barrier = pltpu.get_barrier_semaphore()
    for rel in rels:
        pl.semaphore_signal(barrier, inc=1, device_id=dev(*rel), device_id_type=MESH)

    own = pl.ds(pl.multiple_of(me * ROWS, ROWS), ROWS)
    ins = [pltpu.make_async_copy(src, rows.at[t, own], in_sem.at[t])
           for t, src in ((XA, xa_hbm), (XT, x_hbm), (DY, dy_hbm))]
    for cp in ins:
        cp.start()
    wload = [pltpu.make_async_copy(wqkv_hbm, wqkv, w_sem.at[0]), pltpu.make_async_copy(wo_hbm, wo, w_sem.at[1])]
    for n, (src, dst) in enumerate(((wg_hbm, wg), (wu_hbm, wu), (wd_hbm, wd))):
        for e in range(EXP):
            wload.append(pltpu.make_async_copy(src.at[e], dst.at[e], w_sem.at[2 + n * EXP + e]))
    for cp in wload:
        cp.start()

    lane = lax.broadcasted_iota(jnp.int32, (ROWS, 128), 1)
    lane_exp = (lane // 8) * 4 + lane % 4
    is_gate = (lane % 8) < 4
    in_range = lane < 64
    table = jnp.zeros((ROWS, 128), F32)
    for j in range(TOPK):
        hit = (lane_exp == idx_ref[:, j:j + 1]) & in_range
        table = table + jnp.where(hit, jnp.where(is_gate, gate_ref[:, j:j + 1], 1.0), 0.0)
    gpad[...] = jnp.zeros((128, 128), F32)
    gpad[pl.ds(pl.multiple_of(c * ROWS, ROWS), ROWS), :] = table
    table_t = gpad[...].T
    for d in range(8):
        gsend[d] = table_t[d * 8:(d + 1) * 8, :]
    grecv[me] = gsend[me]
    dgs[...] = jnp.zeros((TOK, 128), F32)
    part[1] = jnp.zeros(part.shape[1:], F32)
    part[2] = jnp.zeros(part.shape[1:], F32)

    def blk(t, q, off=0, n=ROWS):
        return rows.at[t, pl.ds(pl.multiple_of(q * 128 + c * ROWS + off, 32), n)]

    def remote(src, dst, ss, rs, where):
        return pltpu.make_async_remote_copy(src, dst, ss, rs, device_id=where, device_id_type=MESH)

    hr = ROWS // 2

    def gather_copies(t):
        def cp(k, ref, where):
            return remote(ref, ref, ag_s.at[t, k], ag_r.at[t, k], where)
        return [cp(0, blk(t, q0), sib), cp(1, blk(t, q0), xn), cp(2, blk(t, q0), yn),
                cp(3, blk(t, qx, 0, hr), yn), cp(4, blk(t, qy, hr, hr), xn),
                cp(5, blk(t, qx), sib), cp(6, blk(t, qy), sib),
                cp(7, blk(t, qd, 0, hr), sib), cp(8, blk(t, qd, hr, hr), sib)]

    ag = [gather_copies(t) for t in range(3)]

    def ag_own(t):
        for k in (1, 2, 0):
            ag[t][k].start()

    def ag_forward(t):
        ag[t][1].wait_recv()
        ag[t][3].start()
        ag[t][5].start()
        ag[t][2].wait_recv()
        ag[t][4].start()
        ag[t][6].start()

    def ag_last(t):
        ag[t][3].wait_recv()
        ag[t][7].start()
        ag[t][4].wait_recv()
        ag[t][8].start()

    def ag_done(t):
        for k in (0, 5, 6, 7, 8):
            ag[t][k].wait_recv()

    def tile_copies(send, recv, ss, rs, chip_tiles):
        cps = []
        for k, (fx, fy, fc) in enumerate(rels):
            where = dev(fx, fy, fc)
            qq = 2 * where[1] + where[2] // 2
            src = send.at[qq] if chip_tiles else send.at[where[1] * 4 + where[2]]
            cps.append(remote(src, recv.at[me], ss.at[k], rs.at[k], where))
        return cps

    gate_cps = tile_copies(gsend, grecv, gs_sem, gr_sem, False)
    dg_cps = tile_copies(dsend, drecv, dd_s, dd_r, True)

    def rs_copies(n):
        def cp(k, src, dst, where):
            return remote(src, dst, rs_s.at[n, k], rs_r.at[n, k], where)
        return [cp(0, part.at[n, 1 - c, 0], pair.at[n, 0], sib), cp(1, part.at[n, 1 - c, 1], pair.at[n, 1], sib),
                cp(2, s1.at[n, 0, 0], r1.at[n, 0, 0], xn), cp(3, s1.at[n, 0, 1], r1.at[n, 0, 1], xn),
                cp(4, s1.at[n, 1, 0], r1.at[n, 1, 0], yn), cp(5, s1.at[n, 1, 1], r1.at[n, 1, 1], yn),
                cp(6, s2.at[n, 0], r2.at[n, 0], yn), cp(7, s2.at[n, 1], r2.at[n, 1], xn)]

    rsc = [rs_copies(n) for n in range(3)]
    first = (qx, qy)
    second = (qy, qx)

    def rs_pair(n):
        rsc[n][0].start()
        rsc[n][1].start()

    def rs_stage1(n):
        for h in range(2):
            rsc[n][h].wait_recv()
            s1[n, h, 0] = part[n, c, h, qd] + pair[n, h, qd]
            rsc[n][2 + 2 * h].start()
        for h in range(2):
            s1[n, h, 1] = part[n, c, h, first[h]] + pair[n, h, first[h]]
            rsc[n][3 + 2 * h].start()

    def rs_stage2(n):
        for h in range(2):
            rsc[n][2 + 2 * h].wait_recv()
            s2[n, h] = part[n, c, h, second[h]] + pair[n, h, second[h]] + r1[n, h, 0]
            rsc[n][6 + h].start()

    def rs_final(n, out_ref):
        for h in range(2):
            rsc[n][3 + 2 * h].wait_recv()
            rsc[n][6 + h].wait_recv()
            total = part[n, c, h, q0] + pair[n, h, q0] + r1[n, h, 1] + r2[n, h]
            out_ref[:, h * HALF:(h + 1) * HALF] = total.astype(BF)

    for cp in ins:
        cp.wait()
    pl.semaphore_wait(barrier, len(rels))
    for cp in gate_cps:
        cp.start()
    ag_own(XA)
    ag_own(XT)
    ag_forward(XA)
    ag_own(DY)
    ag_forward(XT)
    ag_last(XA)

    for cp in gate_cps:
        cp.wait_recv()
    for q in range(4):
        tile = grecv[2 * q] + grecv[2 * q + 1]
        gt[q * 128:(q + 1) * 128, :] = jnp.concatenate([tile, jnp.zeros((120, 128), F32)], axis=0).T

    ag_done(XA)

    wload[0].wait()
    wload[1].wait()
    causal_r = lax.broadcasted_iota(jnp.int32, (256, 128), 0) % 128
    causal_c = lax.broadcasted_iota(jnp.int32, (256, 128), 1)
    keep = (causal_r >= causal_c) & (causal_r // 64 == causal_c // 64)
    for q in range(4):
        xs = rows[XA, q * 128:(q + 1) * 128, :]
        qkv = jnp.dot(xs, wqkv[...], preferred_element_type=F32).astype(BF)
        qs = jnp.concatenate([qkv[:, 0:64], qkv[:, 64:128]], axis=0)
        sc = lax.dot_general(qs, qkv[:, 128:192], NT, preferred_element_type=F32) * (64 ** -0.5)
        sc = jnp.where(keep, sc, -1e30)
        ex = jnp.exp(sc - jnp.max(sc, axis=1, keepdims=True))
        pr = (ex / jnp.sum(ex, axis=1, keepdims=True)).astype(BF)
        ctx = jnp.dot(pr, qkv[:, 192:256], preferred_element_type=F32).astype(BF)
        ctx = jnp.concatenate([ctx[0:128], ctx[128:256]], axis=1)
        out = jnp.dot(ctx, wo[...], preferred_element_type=F32)
        for cc in range(2):
            for h in range(2):
                part[0, cc, h, q] = out[cc * 64:(cc + 1) * 64, h * HALF:(h + 1) * HALF]
    rs_pair(0)
    ag_forward(DY)
    ag_last(XT)
    ag_last(DY)
    rs_stage1(0)
    ag_done(XT)
    ag_done(DY)

    outs = [pltpu.make_async_copy(rows.at[XT], xall_out, out_sem.at[0]),
            pltpu.make_async_copy(rows.at[DY], dyall_out, out_sem.at[1]),
            pltpu.make_async_copy(gt, gt_out, out_sem.at[2])]
    for cp in outs:
        cp.start()
    for cp in wload[2:]:
        cp.wait()
    lane_t = lax.broadcasted_iota(jnp.int32, (256, 128), 1)

    def pick(tile, e):
        return jnp.sum(jnp.where(lane_t == e, tile, 0.0), axis=1, keepdims=True)

    def accumulate(n, m, val):
        for b in range(4):
            q, cc = (m * 4 + b) // 2, b % 2
            for h in range(2):
                part[n, cc, h, q] += val[b * 64:(b + 1) * 64, h * HALF:(h + 1) * HALF]

    def forward(e, carry):
        for m in range(2):
            sl = slice(m * 256, (m + 1) * 256)
            xs = rows[XT, sl, :]
            a = jnp.dot(xs, wg[e], preferred_element_type=F32)
            b = jnp.dot(xs, wu[e], preferred_element_type=F32)
            tile = gt[sl, :]
            mark = pick(tile, e + 4) > 0.5
            sg = jax.nn.sigmoid(a)
            ac = a * sg
            act[e, sl, :] = jnp.where(mark, ac, 0.0)
            gfac[e, sl, :] = jnp.where(mark, b * sg * (1.0 + a * (1.0 - sg)), 0.0)
            hh = jnp.where(mark, ac * b, 0.0).astype(BF)
            hid[e, sl, :] = hh
            ob = jnp.dot(hh, wd[e], preferred_element_type=F32).astype(BF).astype(F32)
            accumulate(1, m, pick(tile, e) * ob)
            dg = jnp.sum(rows[DY, sl, :].astype(F32) * ob, axis=1, keepdims=True)
            dgs[sl, :] += jnp.where(lane_t == e, dg, 0.0)
        pltpu.make_async_copy(hid.at[e], h_out.at[e], out_sem.at[3 + e]).start()

        @pl.when(e == 2)
        def _():
            rs_stage2(0)
        return carry

    lax.fori_loop(0, EXP, forward, 0)
    rs_pair(1)
    for q in range(4):
        dsend[q] = dgs[q * 128:(q + 1) * 128, :].T[0:8, :]
    drecv[me] = dsend[q0]
    for cp in dg_cps:
        cp.start()
    rs_stage1(1)

    def backward(e, carry):
        for m in range(2):
            sl = slice(m * 256, (m + 1) * 256)
            g = pick(gt[sl, :], e)
            do = (g * rows[DY, sl, :].astype(F32)).astype(BF)
            dh = lax.dot_general(do, wd[e], NT, preferred_element_type=F32).astype(BF).astype(F32)
            da = (dh * gfac[e, sl, :]).astype(BF)
            db = (dh * act[e, sl, :]).astype(BF)
            dag[e, sl, :] = da
            dbg[e, sl, :] = db
            dx = (lax.dot_general(da, wg[e], NT, preferred_element_type=F32)
                  + lax.dot_general(db, wu[e], NT, preferred_element_type=F32))
            accumulate(2, m, dx.astype(BF).astype(F32))
        pltpu.make_async_copy(dag.at[e], da_out.at[e], out_sem.at[3 + EXP + e]).start()
        pltpu.make_async_copy(dbg.at[e], db_out.at[e], out_sem.at[3 + 2 * EXP + e]).start()

        @pl.when(e == 1)
        def _():
            rs_stage2(1)
        return carry

    lax.fori_loop(0, EXP, backward, 0)
    rs_pair(2)
    rs_final(0, at_out)
    rs_stage1(2)
    rs_final(1, y_out)
    for cp in dg_cps:
        cp.wait_recv()
    dpad[...] = jnp.zeros((128, 128), F32)
    for d in range(8):
        dpad[d * 8:(d + 1) * 8, :] = drecv[d]
    gpad[...] = dpad[...].T
    mine = gpad[pl.ds(pl.multiple_of(c * ROWS, ROWS), ROWS), :]
    for j in range(TOPK):
        ij = idx_ref[:, j:j + 1]
        hit = lane == (ij // 4) * 8 + ij % 4
        dg_out[:, j:j + 1] = jnp.sum(jnp.where(hit, mine, 0.0), axis=1, keepdims=True)
    rs_stage2(2)
    rs_final(2, dx_out)

    for cp in outs:
        cp.wait()
    for e in range(EXP):
        pltpu.make_async_copy(hid.at[e], h_out.at[e], out_sem.at[3 + e]).wait()
        pltpu.make_async_copy(dag.at[e], da_out.at[e], out_sem.at[3 + EXP + e]).wait()
        pltpu.make_async_copy(dbg.at[e], db_out.at[e], out_sem.at[3 + 2 * EXP + e]).wait()
    for group in ag + rsc + [gate_cps, dg_cps]:
        for cp in group:
            cp.wait_send()


def exchange(x, dy, xa, idx, gates, wg, wu, wd, wqkv, wo):
    any_spec = pl.BlockSpec(memory_space=pl.ANY)
    vmem = pl.BlockSpec(memory_space=pltpu.VMEM)
    sds = jax.ShapeDtypeStruct
    dma = pltpu.SemaphoreType.DMA
    return pl.pallas_call(
        exchange_kernel,
        name='exchange',
        out_shape=[sds((ROWS, D), BF), sds((ROWS, D), BF), sds((ROWS, TOPK), F32), sds((ROWS, D), BF),
                   sds((TOK, D), BF), sds((TOK, D), BF),
                   sds((EXP, TOK, FF), BF), sds((EXP, TOK, FF), BF), sds((EXP, TOK, FF), BF), sds((TOK, 128), F32)],
        in_specs=[any_spec, any_spec, any_spec, vmem, vmem] + [any_spec] * 5,
        out_specs=[vmem] * 4 + [any_spec] * 6,
        scratch_shapes=[
            pltpu.VMEM((3, TOK, D), BF),
            pltpu.VMEM((EXP, D, FF), BF), pltpu.VMEM((EXP, D, FF), BF), pltpu.VMEM((EXP, FF, D), BF),
            pltpu.VMEM((D, 256), BF), pltpu.VMEM((128, D), BF),
            pltpu.VMEM((EXP, TOK, FF), BF), pltpu.VMEM((EXP, TOK, FF), BF), pltpu.VMEM((EXP, TOK, FF), BF),
            pltpu.VMEM((EXP, TOK, FF), F32), pltpu.VMEM((EXP, TOK, FF), F32),
            pltpu.VMEM((TOK, 128), F32), pltpu.VMEM((128, 128), F32),
            pltpu.VMEM((8, 8, 128), F32), pltpu.VMEM((8, 8, 128), F32),
            pltpu.VMEM((TOK, 128), F32), pltpu.VMEM((4, 8, 128), F32), pltpu.VMEM((8, 8, 128), F32),
            pltpu.VMEM((128, 128), F32),
            pltpu.VMEM((3, 2, 2, 4, ROWS, HALF), F32), pltpu.VMEM((3, 2, 4, ROWS, HALF), F32),
            pltpu.VMEM((3, 2, 2, ROWS, HALF), F32), pltpu.VMEM((3, 2, 2, ROWS, HALF), F32),
            pltpu.VMEM((3, 2, ROWS, HALF), F32), pltpu.VMEM((3, 2, ROWS, HALF), F32),
            dma((3,)), dma((2 + 3 * EXP,)), dma((3 + 3 * EXP,)), dma((7,)), dma((7,)),
            dma((3, RS_COPIES)), dma((3, RS_COPIES)), dma((3, GATHER_COPIES)), dma((3, GATHER_COPIES)),
            dma((7,)), dma((7,)),
        ],
        compiler_params=pltpu.CompilerParams(collective_id=0, has_side_effects=True, vmem_limit_bytes=60 * 1024 * 1024),
    )(x, dy, xa, idx, gates, wg, wu, wd, wqkv, wo)


def grads_kernel(x_ref, dy_ref, gt_ref, h_ref, da_ref, db_ref, dwg_ref, dwu_ref, dwd_ref, xt):
    e = pl.program_id(0)

    @pl.when(e == 0)
    def _():
        xt[...] = x_ref[...].T

    dwg_ref[0] = jnp.dot(xt[...], da_ref[0], preferred_element_type=F32)
    dwu_ref[0] = jnp.dot(xt[...], db_ref[0], preferred_element_type=F32)
    lane = lax.broadcasted_iota(jnp.int32, (TOK, 128), 1)
    g = jnp.sum(jnp.where(lane == e, gt_ref[...], 0.0), axis=1, keepdims=True)
    do = (g * dy_ref[...].astype(F32)).astype(BF)
    dwd_ref[0] = lax.dot_general(h_ref[0], do, TN, preferred_element_type=F32)


def weight_grads(xall, dyall, gt, h, da, db):
    sds = jax.ShapeDtypeStruct
    whole = lambda shape: pl.BlockSpec(shape, lambda e: (0, 0))
    per = lambda a, b: pl.BlockSpec((1, a, b), lambda e: (e, 0, 0))
    return pl.pallas_call(
        grads_kernel,
        name='weight_grads',
        grid=(EXP,),
        out_shape=[sds((EXP, D, FF), F32), sds((EXP, D, FF), F32), sds((EXP, FF, D), F32)],
        in_specs=[whole((TOK, D)), whole((TOK, D)), whole((TOK, 128)), per(TOK, FF), per(TOK, FF), per(TOK, FF)],
        out_specs=[per(D, FF), per(D, FF), per(FF, D)],
        scratch_shapes=[pltpu.VMEM((D, TOK), BF)],
        compiler_params=pltpu.CompilerParams(vmem_limit_bytes=48 * 1024 * 1024),
    )(xall, dyall, gt, h, da, db)


def solution(mesh):
    def local_step(x_tokens, expert_idx, gate_vals, dy_tokens, w_gate, w_up, w_down, x_attn, w_query, w_key, w_value, w_out):
        wqkv = jnp.concatenate([w_query.reshape(D, 128), w_key.reshape(D, 64), w_value.reshape(D, 64)], axis=1)
        wo = w_out.reshape(128, D)
        y_t, dx_t, dg, at, xall, dyall, h, da, db, gt = exchange(
            x_tokens, dy_tokens, x_attn.reshape(ROWS, D), expert_idx, gate_vals, w_gate, w_up, w_down, wqkv, wo)
        dwg, dwu, dwd = weight_grads(xall, dyall, gt, h, da, db)
        return y_t, dx_t, dg, dwg, dwu, dwd, at.reshape(1, ROWS, D)

    spec_rows = P(TOKEN_AXES, None)
    spec_seqs = P(TOKEN_AXES, None, None)
    spec_experts = P(GROUP_AXES, None, None)
    spec_heads = P(None, GROUP_AXES, None)
    return jax.shard_map(local_step, mesh=mesh,
                         in_specs=(spec_rows, spec_rows, spec_rows, spec_rows, spec_experts, spec_experts, spec_experts, spec_seqs, spec_heads, spec_heads, spec_heads, spec_experts),
                         out_specs=(spec_rows, spec_rows, spec_rows, spec_seqs, spec_seqs, spec_seqs, spec_seqs),
                         check_vma=False)
```

```python
import functools

import jax
import jax.numpy as jnp
from jax import lax
from jax.experimental import pallas as pl
from jax.experimental.pallas import tpu as pltpu
from jax.sharding import PartitionSpec as P

MESH = pl.DeviceIdType.MESH
GROUP_AXES = ('ei', 'eo')
TOKEN_AXES = ('dp', 'ei', 'eo')
BF = jnp.bfloat16
F32 = jnp.float32

ROWS = 64
TOK = 512
D = 1024
FF = 512
HALF = 512
EXP = 4
TOPK = 8
GATHER_COPIES = 9
RS_COPIES = 8
XA, XT, DY = 0, 1, 2

NT = (((1,), (1,)), ((), ()))
TN = (((0,), (0,)), ((), ()))


def exchange_kernel(x_hbm, dy_hbm, xa_hbm, idx_ref, gate_ref, wg_hbm, wu_hbm, wd_hbm, wq_hbm, wk_hbm, wv_hbm, wo_hbm,
                    y_out, dx_out, dg_out, at_out, xall_out, dyall_out, h_out, da_out, db_out, gt_out,
                    rows, wg, wu, wd, wqkv, wo, hid, dag, dbg, act, gfac, gt, gsend, grecv,
                    dgs, dsend, drecv,
                    part, pair, s1, r1, s2, r2,
                    in_sem, w_sem, out_sem, gs_sem, gr_sem, rs_s, rs_r, ag_s, ag_r, dd_s, dd_r):
    y = lax.axis_index('ei')
    o = lax.axis_index('eo')
    z = lax.axis_index('dp')
    x = o // 2
    c = o % 2
    me = y * 4 + o
    q0 = 2 * y + x
    qx = 2 * y + (1 - x)
    qy = 2 * (1 - y) + x
    qd = 2 * (1 - y) + (1 - x)

    def dev(fx, fy, fc):
        xx = (1 - x) if fx else x
        yy = (1 - y) if fy else y
        cc = (1 - c) if fc else c
        return (z, yy, xx * 2 + cc)

    sib, xn, yn = dev(0, 0, 1), dev(1, 0, 0), dev(0, 1, 0)
    rels = [(fx, fy, fc) for fx in (0, 1) for fy in (0, 1) for fc in (0, 1) if fx or fy or fc]

    barrier = pltpu.get_barrier_semaphore()
    for rel in rels:
        pl.semaphore_signal(barrier, inc=1, device_id=dev(*rel), device_id_type=MESH)

    own = pl.ds(pl.multiple_of(me * ROWS, ROWS), ROWS)
    ins = [pltpu.make_async_copy(src, rows.at[t, own], in_sem.at[t])
           for t, src in ((XA, xa_hbm), (XT, x_hbm), (DY, dy_hbm))]
    for cp in ins:
        cp.start()
    wload = [pltpu.make_async_copy(wq_hbm, wqkv.at[0:128], w_sem.at[0]),
             pltpu.make_async_copy(wk_hbm, wqkv.at[128:192], w_sem.at[1]),
             pltpu.make_async_copy(wv_hbm, wqkv.at[192:256], w_sem.at[2]),
             pltpu.make_async_copy(wo_hbm, wo, w_sem.at[3])]
    for n, (src, dst) in enumerate(((wg_hbm, wg), (wu_hbm, wu), (wd_hbm, wd))):
        for e in range(EXP):
            wload.append(pltpu.make_async_copy(src.at[e], dst.at[e], w_sem.at[4 + n * EXP + e]))
    for cp in wload:
        cp.start()

    row = lax.broadcasted_iota(jnp.int32, (64, ROWS), 0)
    row_exp = (row // 8) * 4 + row % 4
    is_gate = (row % 8) < 4
    table = jnp.zeros((64, ROWS), F32)
    for j in range(TOPK):
        hit = row_exp == idx_ref[j:j + 1, :]
        table = table + jnp.where(hit, jnp.where(is_gate, gate_ref[j:j + 1, :], 1.0), 0.0)
    blank = jnp.zeros((64, ROWS), F32)
    wide = jnp.where(c == 0, jnp.concatenate([table, blank], axis=1), jnp.concatenate([blank, table], axis=1))
    for d in range(8):
        gsend[d] = wide[d * 8:(d + 1) * 8, :]
    grecv[me] = gsend[me]
    dgs[...] = jnp.zeros((TOK, 128), F32)
    part[1] = jnp.zeros(part.shape[1:], F32)
    part[2] = jnp.zeros(part.shape[1:], F32)

    def blk(t, q, off=0, n=ROWS):
        return rows.at[t, pl.ds(pl.multiple_of(q * 128 + c * ROWS + off, 32), n)]

    def remote(src, dst, ss, rs, where):
        return pltpu.make_async_remote_copy(src, dst, ss, rs, device_id=where, device_id_type=MESH)

    hr = ROWS // 2

    def gather_copies(t):
        def cp(k, ref, where):
            return remote(ref, ref, ag_s.at[t, k], ag_r.at[t, k], where)
        return [cp(0, blk(t, q0), sib), cp(1, blk(t, q0), xn), cp(2, blk(t, q0), yn),
                cp(3, blk(t, qx, 0, hr), yn), cp(4, blk(t, qy, hr, hr), xn),
                cp(5, blk(t, qx), sib), cp(6, blk(t, qy), sib),
                cp(7, blk(t, qd, 0, hr), sib), cp(8, blk(t, qd, hr, hr), sib)]

    ag = [gather_copies(t) for t in range(3)]

    def ag_own(t):
        for k in (1, 2, 0):
            ag[t][k].start()

    def ag_forward(t):
        ag[t][1].wait_recv()
        ag[t][3].start()
        ag[t][5].start()
        ag[t][2].wait_recv()
        ag[t][4].start()
        ag[t][6].start()

    def ag_last(t):
        ag[t][3].wait_recv()
        ag[t][7].start()
        ag[t][4].wait_recv()
        ag[t][8].start()

    def ag_done(t):
        for k in (0, 5, 6, 7, 8):
            ag[t][k].wait_recv()

    def tile_copies(send, recv, ss, rs, chip_tiles):
        cps = []
        for k, (fx, fy, fc) in enumerate(rels):
            where = dev(fx, fy, fc)
            qq = 2 * where[1] + where[2] // 2
            src = send.at[qq] if chip_tiles else send.at[where[1] * 4 + where[2]]
            cps.append(remote(src, recv.at[me], ss.at[k], rs.at[k], where))
        return cps

    gate_cps = tile_copies(gsend, grecv, gs_sem, gr_sem, False)
    dg_cps = tile_copies(dsend, drecv, dd_s, dd_r, True)

    def rs_copies(n):
        def cp(k, src, dst, where):
            return remote(src, dst, rs_s.at[n, k], rs_r.at[n, k], where)
        return [cp(0, part.at[n, 1 - c, 0], pair.at[n, 0], sib), cp(1, part.at[n, 1 - c, 1], pair.at[n, 1], sib),
                cp(2, s1.at[n, 0, 0], r1.at[n, 0, 0], xn), cp(3, s1.at[n, 0, 1], r1.at[n, 0, 1], xn),
                cp(4, s1.at[n, 1, 0], r1.at[n, 1, 0], yn), cp(5, s1.at[n, 1, 1], r1.at[n, 1, 1], yn),
                cp(6, s2.at[n, 0], r2.at[n, 0], yn), cp(7, s2.at[n, 1], r2.at[n, 1], xn)]

    rsc = [rs_copies(n) for n in range(3)]
    first = (qx, qy)
    second = (qy, qx)

    def rs_pair(n):
        rsc[n][0].start()
        rsc[n][1].start()

    def rs_stage1(n):
        for h in range(2):
            rsc[n][h].wait_recv()
            s1[n, h, 0] = part[n, c, h, qd] + pair[n, h, qd]
            rsc[n][2 + 2 * h].start()
        for h in range(2):
            s1[n, h, 1] = part[n, c, h, first[h]] + pair[n, h, first[h]]
            rsc[n][3 + 2 * h].start()

    def rs_stage2(n):
        for h in range(2):
            rsc[n][2 + 2 * h].wait_recv()
            s2[n, h] = part[n, c, h, second[h]] + pair[n, h, second[h]] + r1[n, h, 0]
            rsc[n][6 + h].start()

    def rs_final(n, out_ref):
        for h in range(2):
            rsc[n][3 + 2 * h].wait_recv()
            rsc[n][6 + h].wait_recv()
            total = part[n, c, h, q0] + pair[n, h, q0] + r1[n, h, 1] + r2[n, h]
            out_ref[:, h * HALF:(h + 1) * HALF] = total.astype(BF)

    for cp in ins:
        cp.wait()
    pl.semaphore_wait(barrier, len(rels))
    for cp in gate_cps:
        cp.start()
    ag_own(XA)
    ag_own(XT)
    ag_forward(XA)
    ag_own(DY)
    ag_forward(XT)
    ag_last(XA)

    for cp in gate_cps:
        cp.wait_recv()
    for q in range(4):
        tile = grecv[2 * q] + grecv[2 * q + 1]
        gt[q * 128:(q + 1) * 128, :] = jnp.concatenate([tile, jnp.zeros((120, 128), F32)], axis=0).T

    ag_done(XA)

    for cp in wload[:4]:
        cp.wait()
    causal_r = lax.broadcasted_iota(jnp.int32, (256, 128), 0) % 128
    causal_c = lax.broadcasted_iota(jnp.int32, (256, 128), 1)
    keep = (causal_r >= causal_c) & (causal_r // 64 == causal_c // 64)
    for q in range(4):
        xs = rows[XA, q * 128:(q + 1) * 128, :]
        qkv = lax.dot_general(xs, wqkv[...], NT, preferred_element_type=F32).astype(BF)
        qs = jnp.concatenate([qkv[:, 0:64], qkv[:, 64:128]], axis=0)
        sc = lax.dot_general(qs, qkv[:, 128:192], NT, preferred_element_type=F32) * (64 ** -0.5)
        sc = jnp.where(keep, sc, -1e30)
        ex = jnp.exp(sc - jnp.max(sc, axis=1, keepdims=True))
        pr = (ex / jnp.sum(ex, axis=1, keepdims=True)).astype(BF)
        ctx = jnp.dot(pr, qkv[:, 192:256], preferred_element_type=F32).astype(BF)
        ctx = jnp.concatenate([ctx[0:128], ctx[128:256]], axis=1)
        out = jnp.dot(ctx, wo[...], preferred_element_type=F32)
        for cc in range(2):
            for h in range(2):
                part[0, cc, h, q] = out[cc * 64:(cc + 1) * 64, h * HALF:(h + 1) * HALF]
    rs_pair(0)
    ag_forward(DY)
    ag_last(XT)
    ag_last(DY)
    rs_stage1(0)
    ag_done(XT)
    ag_done(DY)

    outs = [pltpu.make_async_copy(rows.at[XT], xall_out, out_sem.at[0]),
            pltpu.make_async_copy(rows.at[DY], dyall_out, out_sem.at[1]),
            pltpu.make_async_copy(gt, gt_out, out_sem.at[2])]
    for cp in outs:
        cp.start()
    for cp in wload[4:]:
        cp.wait()
    lane_t = lax.broadcasted_iota(jnp.int32, (256, 128), 1)

    def pick(tile, e):
        return jnp.sum(jnp.where(lane_t == e, tile, 0.0), axis=1, keepdims=True)

    def accumulate(n, m, val):
        for b in range(4):
            q, cc = (m * 4 + b) // 2, b % 2
            for h in range(2):
                part[n, cc, h, q] += val[b * 64:(b + 1) * 64, h * HALF:(h + 1) * HALF]

    def forward(e, carry):
        for m in range(2):
            sl = slice(m * 256, (m + 1) * 256)
            xs = rows[XT, sl, :]
            a = jnp.dot(xs, wg[e], preferred_element_type=F32)
            b = jnp.dot(xs, wu[e], preferred_element_type=F32)
            tile = gt[sl, :]
            mark = pick(tile, e + 4) > 0.5
            sg = jax.nn.sigmoid(a)
            ac = a * sg
            act[e, sl, :] = jnp.where(mark, ac, 0.0)
            gfac[e, sl, :] = jnp.where(mark, b * sg * (1.0 + a * (1.0 - sg)), 0.0)
            hh = jnp.where(mark, ac * b, 0.0).astype(BF)
            hid[e, sl, :] = hh
            ob = jnp.dot(hh, wd[e], preferred_element_type=F32).astype(BF).astype(F32)
            accumulate(1, m, pick(tile, e) * ob)
            dg = jnp.sum(rows[DY, sl, :].astype(F32) * ob, axis=1, keepdims=True)
            dgs[sl, :] += jnp.where(lane_t == e, dg, 0.0)
        pltpu.make_async_copy(hid.at[e], h_out.at[e], out_sem.at[3 + e]).start()

        @pl.when(e == 2)
        def _():
            rs_stage2(0)
        return carry

    lax.fori_loop(0, EXP, forward, 0)
    rs_pair(1)
    for q in range(4):
        dsend[q] = dgs[q * 128:(q + 1) * 128, :].T[0:8, :]
    drecv[me] = dsend[q0]
    for cp in dg_cps:
        cp.start()
    rs_stage1(1)

    def backward(e, carry):
        for m in range(2):
            sl = slice(m * 256, (m + 1) * 256)
            g = pick(gt[sl, :], e)
            do = (g * rows[DY, sl, :].astype(F32)).astype(BF)
            dh = lax.dot_general(do, wd[e], NT, preferred_element_type=F32).astype(BF).astype(F32)
            da = (dh * gfac[e, sl, :]).astype(BF)
            db = (dh * act[e, sl, :]).astype(BF)
            dag[e, sl, :] = da
            dbg[e, sl, :] = db
            dx = (lax.dot_general(da, wg[e], NT, preferred_element_type=F32)
                  + lax.dot_general(db, wu[e], NT, preferred_element_type=F32))
            accumulate(2, m, dx.astype(BF).astype(F32))
        pltpu.make_async_copy(dag.at[e], da_out.at[e], out_sem.at[3 + EXP + e]).start()
        pltpu.make_async_copy(dbg.at[e], db_out.at[e], out_sem.at[3 + 2 * EXP + e]).start()

        @pl.when(e == 1)
        def _():
            rs_stage2(1)
        return carry

    lax.fori_loop(0, EXP, backward, 0)
    rs_pair(2)
    rs_final(0, at_out)
    rs_stage1(2)
    rs_final(1, y_out)
    for cp in dg_cps:
        cp.wait_recv()
    both = drecv[...].reshape(64, 128)
    mine = jnp.where(c == 0, both[:, 0:ROWS], both[:, ROWS:128])
    for j in range(TOPK):
        hit = row_exp == idx_ref[j:j + 1, :]
        dg_out[j:j + 1, :] = jnp.sum(jnp.where(hit & is_gate, mine, 0.0), axis=0, keepdims=True)
    rs_stage2(2)
    rs_final(2, dx_out)

    for cp in outs:
        cp.wait()
    for e in range(EXP):
        pltpu.make_async_copy(hid.at[e], h_out.at[e], out_sem.at[3 + e]).wait()
        pltpu.make_async_copy(dag.at[e], da_out.at[e], out_sem.at[3 + EXP + e]).wait()
        pltpu.make_async_copy(dbg.at[e], db_out.at[e], out_sem.at[3 + 2 * EXP + e]).wait()
    for group in ag + rsc + [gate_cps, dg_cps]:
        for cp in group:
            cp.wait_send()


def exchange(x, dy, xa, idx, gates, wg, wu, wd, wq, wk, wv, wo):
    any_spec = pl.BlockSpec(memory_space=pl.ANY)
    vmem = pl.BlockSpec(memory_space=pltpu.VMEM)
    sds = jax.ShapeDtypeStruct
    dma = pltpu.SemaphoreType.DMA
    return pl.pallas_call(
        exchange_kernel,
        name='exchange',
        out_shape=[sds((ROWS, D), BF), sds((ROWS, D), BF), sds((TOPK, ROWS), F32), sds((ROWS, D), BF),
                   sds((TOK, D), BF), sds((TOK, D), BF),
                   sds((EXP, TOK, FF), BF), sds((EXP, TOK, FF), BF), sds((EXP, TOK, FF), BF), sds((TOK, 128), F32)],
        in_specs=[any_spec, any_spec, any_spec, vmem, vmem] + [any_spec] * 7,
        out_specs=[vmem] * 4 + [any_spec] * 6,
        scratch_shapes=[
            pltpu.VMEM((3, TOK, D), BF),
            pltpu.VMEM((EXP, D, FF), BF), pltpu.VMEM((EXP, D, FF), BF), pltpu.VMEM((EXP, FF, D), BF),
            pltpu.VMEM((256, D), BF), pltpu.VMEM((128, D), BF),
            pltpu.VMEM((EXP, TOK, FF), BF), pltpu.VMEM((EXP, TOK, FF), BF), pltpu.VMEM((EXP, TOK, FF), BF),
            pltpu.VMEM((EXP, TOK, FF), F32), pltpu.VMEM((EXP, TOK, FF), F32),
            pltpu.VMEM((TOK, 128), F32),
            pltpu.VMEM((8, 8, 128), F32), pltpu.VMEM((8, 8, 128), F32),
            pltpu.VMEM((TOK, 128), F32), pltpu.VMEM((4, 8, 128), F32), pltpu.VMEM((8, 8, 128), F32),
            pltpu.VMEM((3, 2, 2, 4, ROWS, HALF), F32), pltpu.VMEM((3, 2, 4, ROWS, HALF), F32),
            pltpu.VMEM((3, 2, 2, ROWS, HALF), F32), pltpu.VMEM((3, 2, 2, ROWS, HALF), F32),
            pltpu.VMEM((3, 2, ROWS, HALF), F32), pltpu.VMEM((3, 2, ROWS, HALF), F32),
            dma((3,)), dma((4 + 3 * EXP,)), dma((3 + 3 * EXP,)), dma((7,)), dma((7,)),
            dma((3, RS_COPIES)), dma((3, RS_COPIES)), dma((3, GATHER_COPIES)), dma((3, GATHER_COPIES)),
            dma((7,)), dma((7,)),
        ],
        compiler_params=pltpu.CompilerParams(collective_id=0, has_side_effects=True, vmem_limit_bytes=60 * 1024 * 1024),
    )(x, dy, xa, idx, gates, wg, wu, wd, wq, wk, wv, wo)


def grads_kernel(x_ref, dy_ref, gt_ref, h_ref, da_ref, db_ref, y_in, dx_in, at_in, dg_in,
                 dwg_ref, dwu_ref, dwd_ref, y_out, dx_out, at_out, dg_out, xt):
    e = pl.program_id(0)

    @pl.when(e == 0)
    def _():
        xt[...] = x_ref[...].T
        y_out[...] = y_in[...]
        dx_out[...] = dx_in[...]
        at_out[...] = at_in[...]
        dg_out[...] = dg_in[...]

    dwg_ref[0] = jnp.dot(xt[...], da_ref[0], preferred_element_type=F32)
    dwu_ref[0] = jnp.dot(xt[...], db_ref[0], preferred_element_type=F32)
    lane = lax.broadcasted_iota(jnp.int32, (TOK, 128), 1)
    g = jnp.sum(jnp.where(lane == e, gt_ref[...], 0.0), axis=1, keepdims=True)
    do = (g * dy_ref[...].astype(F32)).astype(BF)
    dwd_ref[0] = lax.dot_general(h_ref[0], do, TN, preferred_element_type=F32)


def weight_grads(xall, dyall, gt, h, da, db, y_t, dx_t, at, dg):
    sds = jax.ShapeDtypeStruct
    whole = lambda shape: pl.BlockSpec(shape, lambda e: (0, 0))
    per = lambda a, b: pl.BlockSpec((1, a, b), lambda e: (e, 0, 0))
    return pl.pallas_call(
        grads_kernel,
        name='weight_grads',
        grid=(EXP,),
        out_shape=[sds((EXP, D, FF), F32), sds((EXP, D, FF), F32), sds((EXP, FF, D), F32),
                   sds((ROWS, D), BF), sds((ROWS, D), BF), sds((ROWS, D), BF), sds((TOPK, ROWS), F32)],
        in_specs=[whole((TOK, D)), whole((TOK, D)), whole((TOK, 128)), per(TOK, FF), per(TOK, FF), per(TOK, FF)]
        + [whole((ROWS, D))] * 3 + [whole((TOPK, ROWS))],
        out_specs=[per(D, FF), per(D, FF), per(FF, D)] + [whole((ROWS, D))] * 3 + [whole((TOPK, ROWS))],
        scratch_shapes=[pltpu.VMEM((D, TOK), BF)],
        compiler_params=pltpu.CompilerParams(vmem_limit_bytes=62 * 1024 * 1024),
    )(xall, dyall, gt, h, da, db, y_t, dx_t, at, dg)


def solution(mesh):
    def local_step(x_tokens, expert_idx, gate_vals, dy_tokens, w_gate, w_up, w_down, x_attn, w_query, w_key, w_value, w_out):
        y_p, dx_p, dg_p, at_p, xall, dyall, h, da, db, gt = exchange(
            x_tokens, dy_tokens, x_attn.reshape(ROWS, D), expert_idx.T, gate_vals.T, w_gate, w_up, w_down,
            w_query.transpose(1, 2, 0).reshape(128, D), w_key.transpose(1, 2, 0).reshape(64, D),
            w_value.transpose(1, 2, 0).reshape(64, D), w_out.reshape(128, D))
        dwg, dwu, dwd, y_t, dx_t, at, dg = weight_grads(xall, dyall, gt, h, da, db, y_p, dx_p, at_p, dg_p)
        return y_t, dx_t, dg.T, dwg, dwu, dwd, at.reshape(1, ROWS, D)

    spec_rows = P(TOKEN_AXES, None)
    spec_seqs = P(TOKEN_AXES, None, None)
    spec_experts = P(GROUP_AXES, None, None)
    spec_heads = P(None, GROUP_AXES, None)
    return jax.shard_map(local_step, mesh=mesh,
                         in_specs=(spec_rows, spec_rows, spec_rows, spec_rows, spec_experts, spec_experts, spec_experts, spec_seqs, spec_heads, spec_heads, spec_heads, spec_experts),
                         out_specs=(spec_rows, spec_rows, spec_rows, spec_seqs, spec_seqs, spec_seqs, spec_seqs),
                         check_vma=False)
```

```python
import functools

import jax
import jax.numpy as jnp
from jax import lax
from jax.experimental import pallas as pl
from jax.experimental.pallas import tpu as pltpu
from jax.sharding import PartitionSpec as P

MESH = pl.DeviceIdType.MESH
GROUP_AXES = ('ei', 'eo')
TOKEN_AXES = ('dp', 'ei', 'eo')
BF = jnp.bfloat16
F32 = jnp.float32

ROWS = 64
TOK = 512
D = 1024
FF = 512
HALF = 512
EXP = 4
TOPK = 8
GATHER_COPIES = 11
RS_COPIES = 14
XA, XT, DY = 0, 1, 2

NT = (((1,), (1,)), ((), ()))
TN = (((0,), (0,)), ((), ()))


def exchange_kernel(x_hbm, dy_hbm, xa_hbm, idx_ref, gate_ref, wg_hbm, wu_hbm, wd_hbm, wq_hbm, wk_hbm, wv_hbm, wo_hbm,
                    y_out, dg_out, tox_out, toy_out, own_out, xall_out, dyall_out, h_out, da_out, db_out, gt_out,
                    rows, wg, wu, wd, wqkv, wo, hid, osv, dag, dbg, act, gfac, gt, gsend, grecv,
                    dgs, dsend, drecv,
                    sums, part, pair, s1, r1, s2, r2,
                    in_sem, w_sem, out_sem, gs_sem, gr_sem, rs_s, rs_r, ag_s, ag_r, dd_s, dd_r):
    y = lax.axis_index('ei')
    o = lax.axis_index('eo')
    z = lax.axis_index('dp')
    x = o // 2
    c = o % 2
    me = y * 4 + o
    q0 = 2 * y + x
    qx = 2 * y + (1 - x)
    qy = 2 * (1 - y) + x
    qd = 2 * (1 - y) + (1 - x)

    def dev(fx, fy, fc):
        xx = (1 - x) if fx else x
        yy = (1 - y) if fy else y
        cc = (1 - c) if fc else c
        return (z, yy, xx * 2 + cc)

    sib, xn, yn = dev(0, 0, 1), dev(1, 0, 0), dev(0, 1, 0)
    rels = [(fx, fy, fc) for fx in (0, 1) for fy in (0, 1) for fc in (0, 1) if fx or fy or fc]

    barrier = pltpu.get_barrier_semaphore()
    for rel in rels:
        pl.semaphore_signal(barrier, inc=1, device_id=dev(*rel), device_id_type=MESH)

    own = pl.ds(pl.multiple_of(me * ROWS, ROWS), ROWS)
    ins = [pltpu.make_async_copy(src, rows.at[t, own], in_sem.at[t])
           for t, src in ((XT, x_hbm), (DY, dy_hbm), (XA, xa_hbm))]
    for cp in ins:
        cp.start()

    def expert_load(e):
        return [pltpu.make_async_copy(src.at[e], dst.at[e], w_sem.at[4 + n * EXP + e])
                for n, (src, dst) in enumerate(((wg_hbm, wg), (wu_hbm, wu), (wd_hbm, wd)))]

    for e in range(EXP):
        for cp in expert_load(e):
            cp.start()
    wload = [pltpu.make_async_copy(wq_hbm, wqkv.at[0:128], w_sem.at[0]),
             pltpu.make_async_copy(wk_hbm, wqkv.at[128:192], w_sem.at[1]),
             pltpu.make_async_copy(wv_hbm, wqkv.at[192:256], w_sem.at[2]),
             pltpu.make_async_copy(wo_hbm, wo, w_sem.at[3])]
    for cp in wload:
        cp.start()

    row = lax.broadcasted_iota(jnp.int32, (64, ROWS), 0)
    row_exp = (row // 8) * 4 + row % 4
    is_gate = (row % 8) < 4
    table = jnp.zeros((64, ROWS), F32)
    for j in range(TOPK):
        hit = row_exp == idx_ref[j:j + 1, :]
        table = table + jnp.where(hit, jnp.where(is_gate, gate_ref[j:j + 1, :], 1.0), 0.0)
    blank = jnp.zeros((64, ROWS), F32)
    wide = jnp.where(c == 0, jnp.concatenate([table, blank], axis=1), jnp.concatenate([blank, table], axis=1))
    for d in range(8):
        gsend[d] = wide[d * 8:(d + 1) * 8, :]
    grecv[me] = gsend[me]
    dgs[...] = jnp.zeros((TOK, 128), F32)
    part[1] = jnp.zeros(part.shape[1:], F32)
    part[2] = jnp.zeros(part.shape[1:], F32)

    def blk(t, q, off=0, n=ROWS):
        return rows.at[t, pl.ds(pl.multiple_of(q * 128 + c * ROWS + off, 32), n)]

    def remote(src, dst, ss, rs, where):
        return pltpu.make_async_remote_copy(src, dst, ss, rs, device_id=where, device_id_type=MESH)

    hr = ROWS // 2

    def gather_copies(t):
        def cp(k, ref, where):
            return remote(ref, ref, ag_s.at[t, k], ag_r.at[t, k], where)
        return [cp(0, blk(t, q0), sib),
                cp(1, blk(t, q0, 0, hr), xn), cp(2, blk(t, q0, hr, hr), xn),
                cp(3, blk(t, q0, hr, hr), yn), cp(4, blk(t, q0, 0, hr), yn),
                cp(5, blk(t, qx, 0, hr), yn), cp(6, blk(t, qy, hr, hr), xn),
                cp(7, blk(t, qx), sib), cp(8, blk(t, qy), sib),
                cp(9, blk(t, qd, 0, hr), sib), cp(10, blk(t, qd, hr, hr), sib)]

    ag = [gather_copies(t) for t in range(3)]

    def ag_own(t):
        for k in (1, 3, 2, 4, 0):
            ag[t][k].start()

    def ag_forward(t):
        ag[t][1].wait_recv()
        ag[t][5].start()
        ag[t][3].wait_recv()
        ag[t][6].start()

    def ag_pair(t):
        ag[t][2].wait_recv()
        ag[t][7].start()
        ag[t][4].wait_recv()
        ag[t][8].start()

    def ag_last(t):
        ag[t][5].wait_recv()
        ag[t][9].start()
        ag[t][6].wait_recv()
        ag[t][10].start()

    def ag_wait(t, *ks):
        for k in ks:
            ag[t][k].wait_recv()

    def tile_copies(send, recv, ss, rs, chip_tiles):
        cps = {}
        for k, (fx, fy, fc) in enumerate(rels):
            where = dev(fx, fy, fc)
            qq = 2 * where[1] + where[2] // 2
            src = send.at[qq] if chip_tiles else send.at[where[1] * 4 + where[2]]
            cps[fx, fy, fc] = remote(src, recv.at[me], ss.at[k], rs.at[k], where)
        return cps

    gate_cps = tile_copies(gsend, grecv, gs_sem, gr_sem, False)
    dg_cps = tile_copies(dsend, drecv, dd_s, dd_r, True)
    chips = (q0, qx, qy, qd)
    OWN, X, Y, DI = 0, 1, 2, 3
    first = (X, Y)
    second = (Y, X)

    def rs_copies(n):
        def cp(k, src, dst, where):
            return remote(src, dst, rs_s.at[n, k], rs_r.at[n, k], where)
        cps = [cp(2 * k + h, part.at[n, 1 - c, h, chips[k]], pair.at[n, h, chips[k]], sib) for k in range(4) for h in range(2)]
        for h in range(2):
            one, two = (xn, yn) if h == 0 else (yn, xn)
            cps += [cp(8 + 3 * h, s1.at[n, h, 0], r1.at[n, h, 0], one), cp(9 + 3 * h, s1.at[n, h, 1], r1.at[n, h, 1], one),
                    cp(10 + 3 * h, s2.at[n, h], r2.at[n, h], two)]
        return cps

    rsc = [rs_copies(n) for n in range(3)]

    def rs_pair(n, k):
        rsc[n][2 * k].start()
        rsc[n][2 * k + 1].start()

    def chip_sum(n, h, k):
        return part[n, c, h, chips[k]] + pair[n, h, chips[k]]

    def rs_far(n):
        for h in range(2):
            rsc[n][2 * DI + h].wait_recv()
            s1[n, h, 0] = chip_sum(n, h, DI)
            rsc[n][8 + 3 * h].start()

    def rs_near(n, h):
        k = first[h]
        rsc[n][2 * k + h].wait_recv()
        s1[n, h, 1] = chip_sum(n, h, k)
        rsc[n][9 + 3 * h].start()

    def rs_second(n):
        for h in range(2):
            k = second[h]
            rsc[n][2 * k + h].wait_recv()
            rsc[n][8 + 3 * h].wait_recv()
            s2[n, h] = chip_sum(n, h, k) + r1[n, h, 0]
            rsc[n][10 + 3 * h].start()

    def rs_final(n, out_ref):
        for h in range(2):
            rsc[n][2 * OWN + h].wait_recv()
            rsc[n][9 + 3 * h].wait_recv()
            rsc[n][10 + 3 * h].wait_recv()
            total = chip_sum(n, h, OWN) + r1[n, h, 1] + r2[n, h]
            out_ref[:, h * HALF:(h + 1) * HALF] = total.astype(BF)

    def gate_table(k):
        fx, fy = k % 2, k // 2
        for fc in (0, 1):
            if (fx, fy, fc) in gate_cps:
                gate_cps[fx, fy, fc].wait_recv()
        q = chips[k]
        tile = grecv[2 * q] + grecv[2 * q + 1]
        gt[pl.ds(pl.multiple_of(q * 128, 128), 128), :] = jnp.concatenate([tile, jnp.zeros((120, 128), F32)], axis=0).T

    def pick(tile, e):
        lane = lax.broadcasted_iota(jnp.int32, tile.shape, 1)
        return jnp.sum(jnp.where(lane == e, tile, 0.0), axis=1, keepdims=True)

    def accumulate(n, q, val):
        for cc in range(2):
            for h in range(2):
                part[n, cc, h, q] += val[cc * 64:(cc + 1) * 64, h * HALF:(h + 1) * HALF]

    def experts(step, hooks):
        def body(e, carry):
            step(e)
            for at, fn in hooks.items():
                @pl.when(e == at)
                def _():
                    fn()
            return carry
        lax.fori_loop(0, EXP, body, 0)

    def forward(k, load=False):
        q = chips[k]
        sl = pl.ds(pl.multiple_of(q * 128, 128), 128)

        def step(e):
            if load:
                for cp in expert_load(e):
                    cp.wait()
            xs = rows[XT, sl, :]
            a = jnp.dot(xs, wg[e], preferred_element_type=F32)
            b = jnp.dot(xs, wu[e], preferred_element_type=F32)
            tile = gt[sl, :]
            mark = pick(tile, e + 4) > 0.5
            sg = jax.nn.sigmoid(a)
            ac = a * sg
            act[e, sl, :] = jnp.where(mark, ac, 0.0)
            gfac[e, sl, :] = jnp.where(mark, b * sg * (1.0 + a * (1.0 - sg)), 0.0)
            hh = jnp.where(mark, ac * b, 0.0).astype(BF)
            hid[e, sl, :] = hh
            ob = jnp.dot(hh, wd[e], preferred_element_type=F32).astype(BF)
            osv[e, sl, :] = ob
            accumulate(1, q, pick(tile, e) * ob.astype(F32))
        return step

    def backward(qa, qb, base, gates):
        sl = pl.ds(pl.multiple_of(base, 256), 256)

        def step(e):
            g = pick(gt[sl, :], e)
            dyf = rows[DY, sl, :].astype(F32)
            do = (g * dyf).astype(BF)
            dh = lax.dot_general(do, wd[e], NT, preferred_element_type=F32).astype(BF).astype(F32)
            da = (dh * gfac[e, sl, :]).astype(BF)
            db = (dh * act[e, sl, :]).astype(BF)
            dag[e, sl, :] = da
            dbg[e, sl, :] = db
            if gates:
                lane = lax.broadcasted_iota(jnp.int32, (256, 128), 1)
                for r in (slice(0, 256), slice(256, 512)):
                    dg = jnp.sum(rows[DY, r, :].astype(F32) * osv[e, r, :].astype(F32), axis=1, keepdims=True)
                    dgs[r, :] += jnp.where(lane == e, dg, 0.0)
            dx = (lax.dot_general(da, wg[e], NT, preferred_element_type=F32)
                  + lax.dot_general(db, wu[e], NT, preferred_element_type=F32)).astype(BF).astype(F32)
            accumulate(2, qa, dx[0:128])
            accumulate(2, qb, dx[128:256])
        return step

    def attention_context():
        ag_wait(XA, 0, 7, 8, 9, 10)
        for cp in wload:
            cp.wait()
        causal_r = lax.broadcasted_iota(jnp.int32, (256, 128), 0) % 128
        causal_c = lax.broadcasted_iota(jnp.int32, (256, 128), 1)
        keep = (causal_r >= causal_c) & (causal_r // 64 == causal_c // 64)
        qkv = lax.dot_general(rows[XA], wqkv[...], NT, preferred_element_type=F32).astype(BF)
        qkvs = [qkv[q * 128:(q + 1) * 128] for q in range(4)]
        scs = [lax.dot_general(jnp.concatenate([v[:, 0:64], v[:, 64:128]], axis=0), v[:, 128:192], NT,
                               preferred_element_type=F32) * (64 ** -0.5) for v in qkvs]
        scs = [jnp.where(keep, sc, -1e30) for sc in scs]
        mxs = [jnp.max(sc, axis=1, keepdims=True) for sc in scs]
        exs = [jnp.exp(sc - mx) for sc, mx in zip(scs, mxs)]
        sms = [jnp.sum(ex, axis=1, keepdims=True) for ex in exs]
        prs = [(ex / sm).astype(BF) for ex, sm in zip(exs, sms)]
        ctxs = [jnp.dot(pr, v[:, 192:256], preferred_element_type=F32).astype(BF) for pr, v in zip(prs, qkvs)]
        return jnp.concatenate([jnp.concatenate([v[0:128], v[128:256]], axis=1) for v in ctxs], axis=0)

    def attention_out(ctx):
        for q in range(4):
            out = jnp.dot(ctx[q * 128:(q + 1) * 128], wo[...], preferred_element_type=F32)
            for cc in range(2):
                for h in range(2):
                    part[0, cc, h, q] = out[cc * 64:(cc + 1) * 64, h * HALF:(h + 1) * HALF]

    def leave(i, n):
        for h in range(2):
            cols = slice(h * HALF, (h + 1) * HALF)
            rsc[n][2 * first[h] + h].wait_recv()
            near = chip_sum(n, h, first[h])
            rsc[n][2 * second[h] + h].wait_recv()
            rsc[n][8 + 3 * h].wait_recv()
            far = chip_sum(n, h, second[h]) + r1[n, h, 0]
            rsc[n][2 * OWN + h].wait_recv()
            mine = chip_sum(n, h, OWN)
            sums[X - 1, i, :, cols] = near if h == 0 else far
            sums[Y - 1, i, :, cols] = far if h == 0 else near
            sums[2, i, :, cols] = mine
        cps = [pltpu.make_async_copy(sums.at[k, i], dst.at[i], out_sem.at[6 + 2 * k + i])
               for k, dst in enumerate((tox_out, toy_out, own_out))]
        for cp in cps:
            cp.start()
        return cps

    for cp in ins:
        cp.wait()
    pl.semaphore_wait(barrier, len(rels))
    for cp in gate_cps.values():
        cp.start()
    ag_own(XT)
    ag_own(XA)
    gate_table(OWN)
    ag_wait(XT, 0)
    experts(forward(OWN, True), {2: lambda: ag_forward(XT)})
    rs_pair(1, OWN)
    ag_pair(XT)
    gate_table(X)
    ag_wait(XT, 7)
    experts(forward(X), {0: lambda: (ag_forward(XA), ag_own(DY)), 2: lambda: ag_pair(XA)})
    rs_pair(1, X)
    gate_table(Y)
    ag_wait(XT, 8)
    experts(forward(Y), {0: lambda: ag_last(XT), 2: lambda: ag_last(XA), 3: lambda: (ag_forward(DY), rs_near(1, 0))})
    rs_pair(1, Y)
    gate_table(DI)
    ag_wait(XT, 9, 10)
    gate_out = pltpu.make_async_copy(gt, gt_out, out_sem.at[2])
    gate_out.start()
    rows_out = pltpu.make_async_copy(rows.at[XT], xall_out, out_sem.at[0])
    rows_out.start()
    experts(forward(DI), {1: lambda: rs_near(1, 1), 2: lambda: ag_pair(DY)})
    rs_pair(1, DI)
    hid_out = pltpu.make_async_copy(hid, h_out, out_sem.at[3])
    hid_out.start()
    ctx = attention_context()
    ag_last(DY)
    rs_far(1)
    attention_out(ctx)
    for k in (DI, X, Y, OWN):
        rs_pair(0, k)
    ag_wait(DY, 0, 7, 8, 9, 10)
    dys_out = pltpu.make_async_copy(rows.at[DY], dyall_out, out_sem.at[1])
    dys_out.start()
    experts(backward(2 * (1 - y), 2 * (1 - y) + 1, (1 - y) * 256, True), {1: lambda: rs_far(0)})
    rs_pair(2, DI)
    rs_pair(2, Y)
    for q in range(4):
        dsend[q] = dgs[q * 128:(q + 1) * 128, :].T[0:8, :]
    drecv[me] = dsend[q0]
    for cp in dg_cps.values():
        cp.start()
    experts(backward(2 * y, 2 * y + 1, y * 256, False), {1: lambda: rs_far(2), 3: lambda: rs_second(1)})
    rs_pair(2, X)
    rs_pair(2, OWN)
    da_cp = pltpu.make_async_copy(dag, da_out, out_sem.at[4])
    db_cp = pltpu.make_async_copy(dbg, db_out, out_sem.at[5])
    da_cp.start()
    db_cp.start()
    leaving = leave(0, 0)
    leaving += leave(1, 2)
    for cp in dg_cps.values():
        cp.wait_recv()
    both = drecv[...].reshape(64, 128)
    mine = jnp.where(c == 0, both[:, 0:ROWS], both[:, ROWS:128])
    for j in range(TOPK):
        hit = row_exp == idx_ref[j:j + 1, :]
        dg_out[j:j + 1, :] = jnp.sum(jnp.where(hit & is_gate, mine, 0.0), axis=0, keepdims=True)
    rs_final(1, y_out)

    for cp in [gate_out, rows_out, dys_out, hid_out, da_cp, db_cp] + leaving:
        cp.wait()
    for group in ag + [list(gate_cps.values()), list(dg_cps.values())]:
        for cp in group:
            cp.wait_send()
    for n in range(3):
        for k, cp in enumerate(rsc[n]):
            if n == 1 or k < 8 or k in (8, 11):
                cp.wait_send()


def exchange(x, dy, xa, idx, gates, wg, wu, wd, wq, wk, wv, wo):
    any_spec = pl.BlockSpec(memory_space=pl.ANY)
    vmem = pl.BlockSpec(memory_space=pltpu.VMEM)
    sds = jax.ShapeDtypeStruct
    dma = pltpu.SemaphoreType.DMA
    return pl.pallas_call(
        exchange_kernel,
        name='exchange',
        out_shape=[sds((ROWS, D), BF), sds((TOPK, ROWS), F32)] + [sds((2, ROWS, D), F32)] * 3 + [
                   sds((TOK, D), BF), sds((TOK, D), BF),
                   sds((EXP, TOK, FF), BF), sds((EXP, TOK, FF), BF), sds((EXP, TOK, FF), BF), sds((TOK, 128), F32)],
        in_specs=[any_spec, any_spec, any_spec, vmem, vmem] + [any_spec] * 7,
        out_specs=[vmem] * 2 + [any_spec] * 9,
        scratch_shapes=[
            pltpu.VMEM((3, TOK, D), BF),
            pltpu.VMEM((EXP, D, FF), BF), pltpu.VMEM((EXP, D, FF), BF), pltpu.VMEM((EXP, FF, D), BF),
            pltpu.VMEM((256, D), BF), pltpu.VMEM((128, D), BF),
            pltpu.VMEM((EXP, TOK, FF), BF), pltpu.VMEM((EXP, TOK, D), BF),
            pltpu.VMEM((EXP, TOK, FF), BF), pltpu.VMEM((EXP, TOK, FF), BF),
            pltpu.VMEM((EXP, TOK, FF), F32), pltpu.VMEM((EXP, TOK, FF), F32),
            pltpu.VMEM((TOK, 128), F32),
            pltpu.VMEM((8, 8, 128), F32), pltpu.VMEM((8, 8, 128), F32),
            pltpu.VMEM((TOK, 128), F32), pltpu.VMEM((4, 8, 128), F32), pltpu.VMEM((8, 8, 128), F32),
            pltpu.VMEM((3, 2, ROWS, D), F32),
            pltpu.VMEM((3, 2, 2, 4, ROWS, HALF), F32), pltpu.VMEM((3, 2, 4, ROWS, HALF), F32),
            pltpu.VMEM((3, 2, 2, ROWS, HALF), F32), pltpu.VMEM((3, 2, 2, ROWS, HALF), F32),
            pltpu.VMEM((3, 2, ROWS, HALF), F32), pltpu.VMEM((3, 2, ROWS, HALF), F32),
            dma((3,)), dma((4 + 3 * EXP,)), dma((12,)), dma((7,)), dma((7,)),
            dma((3, RS_COPIES)), dma((3, RS_COPIES)), dma((3, GATHER_COPIES)), dma((3, GATHER_COPIES)),
            dma((7,)), dma((7,)),
        ],
        compiler_params=pltpu.CompilerParams(collective_id=0, has_side_effects=True, vmem_limit_bytes=60 * 1024 * 1024),
    )(x, dy, xa, idx, gates, wg, wu, wd, wq, wk, wv, wo)


def grads_kernel(x_ref, dy_ref, gt_ref, h_ref, da_ref, db_ref, y_in, dg_in,
                 dwg_ref, dwu_ref, dwd_ref, y_out, dg_out, xt):
    e = pl.program_id(0)

    @pl.when(e == 0)
    def _():
        xt[...] = x_ref[...].T
        y_out[...] = y_in[...]
        dg_out[...] = dg_in[...]

    dwg_ref[0] = jnp.dot(xt[...], da_ref[0], preferred_element_type=F32)
    dwu_ref[0] = jnp.dot(xt[...], db_ref[0], preferred_element_type=F32)
    lane = lax.broadcasted_iota(jnp.int32, (TOK, 128), 1)
    g = jnp.sum(jnp.where(lane == e, gt_ref[...], 0.0), axis=1, keepdims=True)
    do = (g * dy_ref[...].astype(F32)).astype(BF)
    dwd_ref[0] = lax.dot_general(h_ref[0], do, TN, preferred_element_type=F32)


def weight_grads(xall, dyall, gt, h, da, db, y_t, dg):
    sds = jax.ShapeDtypeStruct
    whole = lambda shape: pl.BlockSpec(shape, lambda e: (0, 0))
    per = lambda a, b: pl.BlockSpec((1, a, b), lambda e: (e, 0, 0))
    return pl.pallas_call(
        grads_kernel,
        name='weight_grads',
        grid=(EXP,),
        out_shape=[sds((EXP, D, FF), F32), sds((EXP, D, FF), F32), sds((EXP, FF, D), F32),
                   sds((ROWS, D), BF), sds((TOPK, ROWS), F32)],
        in_specs=[whole((TOK, D)), whole((TOK, D)), whole((TOK, 128)), per(TOK, FF), per(TOK, FF), per(TOK, FF)]
        + [whole((ROWS, D))] + [whole((TOPK, ROWS))],
        out_specs=[per(D, FF), per(D, FF), per(FF, D)] + [whole((ROWS, D))] + [whole((TOPK, ROWS))],
        scratch_shapes=[pltpu.VMEM((D, TOK), BF)],
        cost_estimate=pl.CostEstimate(flops=3 * 2 * EXP * TOK * D * FF, bytes_accessed=34 * 1024 * 1024, transcendentals=0),
        compiler_params=pltpu.CompilerParams(vmem_limit_bytes=62 * 1024 * 1024),
    )(xall, dyall, gt, h, da, db, y_t, dg)


def solution(mesh):
    def local_step(x_tokens, expert_idx, gate_vals, dy_tokens, w_gate, w_up, w_down, x_attn, w_query, w_key, w_value, w_out):
        y_p, dg_p, to_x, to_y, own, xall, dyall, h, da, db, gt = exchange(
            x_tokens, dy_tokens, x_attn.reshape(ROWS, D), expert_idx.T, gate_vals.T, w_gate, w_up, w_down,
            w_query.transpose(1, 2, 0).reshape(128, D), w_key.transpose(1, 2, 0).reshape(64, D),
            w_value.transpose(1, 2, 0).reshape(64, D), w_out.reshape(128, D))
        from_x = lax.ppermute(to_x, GROUP_AXES, [(g, g ^ 2) for g in range(8)])
        from_y = lax.ppermute(to_y, GROUP_AXES, [(g, g ^ 4) for g in range(8)])
        dwg, dwu, dwd, y_t, dg = weight_grads(xall, dyall, gt, h, da, db, y_p, dg_p)
        both = (own + from_x + from_y).astype(BF)
        at, dx_t = both[0], both[1]
        return y_t, dx_t, dg.T, dwg, dwu, dwd, at.reshape(1, ROWS, D)

    spec_rows = P(TOKEN_AXES, None)
    spec_seqs = P(TOKEN_AXES, None, None)
    spec_experts = P(GROUP_AXES, None, None)
    spec_heads = P(None, GROUP_AXES, None)
    return jax.shard_map(local_step, mesh=mesh,
                         in_specs=(spec_rows, spec_rows, spec_rows, spec_rows, spec_experts, spec_experts, spec_experts, spec_seqs, spec_heads, spec_heads, spec_heads, spec_experts),
                         out_specs=(spec_rows, spec_rows, spec_rows, spec_seqs, spec_seqs, spec_seqs, spec_seqs),
                         check_vma=False)
```

```python
import functools

import jax
import jax.numpy as jnp
from jax import lax
from jax.experimental import pallas as pl
from jax.experimental.pallas import tpu as pltpu
from jax.sharding import PartitionSpec as P

MESH = pl.DeviceIdType.MESH
GROUP_AXES = ('ei', 'eo')
TOKEN_AXES = ('dp', 'ei', 'eo')
BF = jnp.bfloat16
F32 = jnp.float32

ROWS = 64
TOK = 512
D = 1024
FF = 512
HALF = 512
EXP = 4
TOPK = 8
XA, XT, DY = 0, 1, 2

NT = (((1,), (1,)), ((), ()))
TN = (((0,), (0,)), ((), ()))


def exchange_kernel(x_hbm, dy_hbm, xa_hbm, idx_hbm, gate_hbm, wg_hbm, wu_hbm, wd_hbm, wq_hbm, wk_hbm, wv_hbm, wo_hbm,
                    y_out, dg_out, tox_out, toy_out, own_out, xall_out, dyall_out, h_out, da_out, db_out, gt_out,
                    idx_ref, gate_ref, y_ref, dg_ref, rows, wg, wu, wd, wqkv, wo, hid, osv, dag, dbg, act, gfac, gt, gsend, grecv,
                    dgs, dsend, drecv,
                    sums, part, pair, s1, r1, s2, r2,
                    in_sem, w_sem, out_sem, gs_sem, gr_sem, rs_s, rs_r, ag_s, ag_r, dd_s, dd_r):
    y = lax.axis_index('ei')
    o = lax.axis_index('eo')
    z = lax.axis_index('dp')
    x = o // 2
    c = o % 2
    me = y * 4 + o
    q0 = 2 * y + x
    qx = 2 * y + (1 - x)
    qy = 2 * (1 - y) + x
    qd = 2 * (1 - y) + (1 - x)

    def dev(fx, fy, fc):
        xx = (1 - x) if fx else x
        yy = (1 - y) if fy else y
        cc = (1 - c) if fc else c
        return (z, yy, xx * 2 + cc)

    sib, xn, yn = dev(0, 0, 1), dev(1, 0, 0), dev(0, 1, 0)
    rels = [(fx, fy, fc) for fx in (0, 1) for fy in (0, 1) for fc in (0, 1) if fx or fy or fc]

    barrier = pltpu.get_barrier_semaphore()
    for rel in rels:
        pl.semaphore_signal(barrier, inc=1, device_id=dev(*rel), device_id_type=MESH)

    own = pl.ds(pl.multiple_of(me * ROWS, ROWS), ROWS)
    tables = [pltpu.make_async_copy(idx_hbm, idx_ref, in_sem.at[1]), pltpu.make_async_copy(gate_hbm, gate_ref, in_sem.at[2])]
    for cp in tables:
        cp.start()
    for t, src in ((XT, x_hbm), (DY, dy_hbm), (XA, xa_hbm)):
        pltpu.make_async_copy(src, rows.at[t, own], in_sem.at[0]).start()

    def expert_load(e):
        return [pltpu.make_async_copy(src.at[e], dst.at[e], w_sem.at[1 + e])
                for src, dst in ((wg_hbm, wg), (wu_hbm, wu), (wd_hbm, wd))]

    for e in range(EXP):
        for cp in expert_load(e):
            cp.start()
    wload = [pltpu.make_async_copy(wq_hbm, wqkv.at[0:128], w_sem.at[0]),
             pltpu.make_async_copy(wk_hbm, wqkv.at[128:192], w_sem.at[0]),
             pltpu.make_async_copy(wv_hbm, wqkv.at[192:256], w_sem.at[0]),
             pltpu.make_async_copy(wo_hbm, wo, w_sem.at[0])]
    for cp in wload:
        cp.start()

    for cp in tables:
        cp.wait()
    row = lax.broadcasted_iota(jnp.int32, (64, ROWS), 0)
    row_exp = (row // 8) * 4 + row % 4
    is_gate = (row % 8) < 4
    table = jnp.zeros((64, ROWS), F32)
    for j in range(TOPK):
        hit = row_exp == idx_ref[j:j + 1, :]
        table = table + jnp.where(hit, jnp.where(is_gate, gate_ref[j:j + 1, :], 1.0), 0.0)
    blank = jnp.zeros((64, ROWS), F32)
    wide = jnp.where(c == 0, jnp.concatenate([table, blank], axis=1), jnp.concatenate([blank, table], axis=1))
    for d in range(8):
        gsend[d] = wide[d * 8:(d + 1) * 8, :]
    grecv[me] = gsend[me]
    dgs[...] = jnp.zeros((TOK, 128), F32)
    part[1] = jnp.zeros(part.shape[1:], F32)
    part[2] = jnp.zeros(part.shape[1:], F32)

    def blk(t, q, off=0, n=ROWS):
        return rows.at[t, pl.ds(pl.multiple_of(q * 128 + c * ROWS + off, 32), n)]

    def remote(src, dst, ss, rs, where):
        return pltpu.make_async_remote_copy(src, dst, ss, rs, device_id=where, device_id_type=MESH)

    hr = ROWS // 2

    def gather_slot(t, k):
        if t == XT:
            return min(k, 9)
        return (10 if t == XA else 17) + (k - 1 if 1 <= k <= 6 else 6)

    def gather_copies(t):
        def cp(k, ref, where):
            return remote(ref, ref, ag_s.at[t], ag_r.at[gather_slot(t, k)], where)
        return [cp(0, blk(t, q0), sib),
                cp(1, blk(t, q0, 0, hr), xn), cp(2, blk(t, q0, hr, hr), xn),
                cp(3, blk(t, q0, hr, hr), yn), cp(4, blk(t, q0, 0, hr), yn),
                cp(5, blk(t, qx, 0, hr), yn), cp(6, blk(t, qy, hr, hr), xn),
                cp(7, blk(t, qx), sib), cp(8, blk(t, qy), sib),
                cp(9, blk(t, qd, 0, hr), sib), cp(10, blk(t, qd, hr, hr), sib)]

    ag = [gather_copies(t) for t in range(3)]

    def ag_own(t):
        for k in (1, 3, 2, 4, 0):
            ag[t][k].start()

    def ag_forward(t):
        ag[t][1].wait_recv()
        ag[t][5].start()
        ag[t][3].wait_recv()
        ag[t][6].start()

    def ag_pair(t):
        ag[t][2].wait_recv()
        ag[t][7].start()
        ag[t][4].wait_recv()
        ag[t][8].start()

    def ag_last(t):
        ag[t][5].wait_recv()
        ag[t][9].start()
        ag[t][6].wait_recv()
        ag[t][10].start()

    def ag_rows(t, k, n):
        ref = rows.at[t, 0:n]
        return remote(ref, ref, ag_s.at[t], ag_r.at[gather_slot(t, k)], sib)

    def tile_copies(send, recv, ss, rs, chip_tiles):
        cps = {}
        for fx, fy, fc in rels:
            where = dev(fx, fy, fc)
            qq = 2 * where[1] + where[2] // 2
            src = send.at[qq] if chip_tiles else send.at[where[1] * 4 + where[2]]
            cps[fx, fy, fc] = remote(src, recv.at[me], ss.at[0], rs.at[0 if chip_tiles else fx + 2 * fy], where)
        return cps

    gate_cps = tile_copies(gsend, grecv, gs_sem, gr_sem, False)
    dg_cps = tile_copies(dsend, drecv, dd_s, dd_r, True)
    chips = (q0, qx, qy, qd)
    OWN, X, Y, DI = 0, 1, 2, 3
    first = (X, Y)
    second = (Y, X)

    def rs_slot(n, k):
        if k >= 8:
            kind = (k - 8) % 3
            group = 2 if kind == 0 else 1
        else:
            group = 0 if k // 2 == DI else 1
            if n == 1 and k // 2 in (X, Y):
                group = 3 if k == 2 * X else 4 if k == 2 * Y + 1 else 5
        return (0, 3, 9)[n] + group

    def rs_wait(n, k, count):
        ref = pair.at[n, 0, 0:2] if count == 2 else pair.at[n, :, 0:3] if count == 6 else pair.at[n, 0, 0]
        remote(ref, ref, rs_s.at[n, 0], rs_r.at[rs_slot(n, k)], sib).wait_recv()

    def rs_copies(n):
        def cp(k, src, dst, where):
            return remote(src, dst, rs_s.at[n, 0 if k < 8 else 1], rs_r.at[rs_slot(n, k)], where)
        cps = [cp(2 * k + h, part.at[n, 1 - c, h, chips[k]], pair.at[n, h, chips[k]], sib) for k in range(4) for h in range(2)]
        for h in range(2):
            one, two = (xn, yn) if h == 0 else (yn, xn)
            cps += [cp(8 + 3 * h, s1.at[n, h, 0], r1.at[n, h, 0], one), cp(9 + 3 * h, s1.at[n, h, 1], r1.at[n, h, 1], one),
                    cp(10 + 3 * h, s2.at[n, h], r2.at[n, h], two)]
        return cps

    rsc = [rs_copies(n) for n in range(3)]

    def rs_pair(n, k):
        rsc[n][2 * k].start()
        rsc[n][2 * k + 1].start()

    def chip_sum(n, h, k):
        return part[n, c, h, chips[k]] + pair[n, h, chips[k]]

    def rs_far(n):
        rs_wait(n, 2 * DI, 2)
        for h in range(2):
            s1[n, h, 0] = chip_sum(n, h, DI)
            rsc[n][8 + 3 * h].start()

    def rs_near(n, h):
        k = first[h]
        rs_wait(n, 2 * k + h, 1)
        s1[n, h, 1] = chip_sum(n, h, k)
        rsc[n][9 + 3 * h].start()

    def rs_second(n):
        rs_wait(n, 2 * Y, 2)
        rs_wait(n, 8, 2)
        for h in range(2):
            k = second[h]
            s2[n, h] = chip_sum(n, h, k) + r1[n, h, 0]
            rsc[n][10 + 3 * h].start()

    def rs_final(n, out_ref):
        rs_wait(n, 2 * OWN, 6)
        for h in range(2):
            total = chip_sum(n, h, OWN) + r1[n, h, 1] + r2[n, h]
            out_ref[:, h * HALF:(h + 1) * HALF] = total.astype(BF)

    def gate_table(k):
        tiles = grecv.at[0:1 if k == OWN else 2]
        remote(tiles, tiles, gs_sem.at[0], gr_sem.at[k], sib).wait_recv()
        q = chips[k]
        tile = grecv[2 * q] + grecv[2 * q + 1]
        gt[pl.ds(pl.multiple_of(q * 128, 128), 128), :] = jnp.concatenate([tile, jnp.zeros((120, 128), F32)], axis=0).T

    def pick(tile, e):
        lane = lax.broadcasted_iota(jnp.int32, tile.shape, 1)
        return jnp.sum(jnp.where(lane == e, tile, 0.0), axis=1, keepdims=True)

    def accumulate(n, q, val):
        for cc in range(2):
            for h in range(2):
                part[n, cc, h, q] += val[cc * 64:(cc + 1) * 64, h * HALF:(h + 1) * HALF]

    def experts(step, hooks):
        def body(e, carry):
            step(e)
            for at, fn in hooks.items():
                @pl.when(e == at)
                def _():
                    fn()
            return carry
        lax.fori_loop(0, EXP, body, 0)

    def forward(k, load=False):
        q = chips[k]
        sl = pl.ds(pl.multiple_of(q * 128, 128), 128)

        def step(e):
            if load:
                pltpu.make_async_copy(wg_hbm.at[0:3], wg.at[0:3], w_sem.at[1 + e]).wait()
            xs = rows[XT, sl, :]
            a = jnp.dot(xs, wg[e], preferred_element_type=F32)
            b = jnp.dot(xs, wu[e], preferred_element_type=F32)
            tile = gt[sl, :]
            mark = pick(tile, e + 4) > 0.5
            sg = jax.nn.sigmoid(a)
            ac = a * sg
            act[e, sl, :] = jnp.where(mark, ac, 0.0)
            gfac[e, sl, :] = jnp.where(mark, b * sg * (1.0 + a * (1.0 - sg)), 0.0)
            hh = jnp.where(mark, ac * b, 0.0).astype(BF)
            hid[e, sl, :] = hh
            ob = jnp.dot(hh, wd[e], preferred_element_type=F32).astype(BF)
            osv[e, sl, :] = ob
            accumulate(1, q, pick(tile, e) * ob.astype(F32))
        return step

    def backward(qa, qb, base, gates):
        sl = pl.ds(pl.multiple_of(base, 256), 256)

        def step(e):
            g = pick(gt[sl, :], e)
            dyf = rows[DY, sl, :].astype(F32)
            do = (g * dyf).astype(BF)
            dh = lax.dot_general(do, wd[e], NT, preferred_element_type=F32).astype(BF).astype(F32)
            da = (dh * gfac[e, sl, :]).astype(BF)
            db = (dh * act[e, sl, :]).astype(BF)
            dag[e, sl, :] = da
            dbg[e, sl, :] = db
            if gates:
                lane = lax.broadcasted_iota(jnp.int32, (256, 128), 1)
                for r in (slice(0, 256), slice(256, 512)):
                    dg = jnp.sum(rows[DY, r, :].astype(F32) * osv[e, r, :].astype(F32), axis=1, keepdims=True)
                    dgs[r, :] += jnp.where(lane == e, dg, 0.0)
            dx = (lax.dot_general(da, wg[e], NT, preferred_element_type=F32)
                  + lax.dot_general(db, wu[e], NT, preferred_element_type=F32)).astype(BF).astype(F32)
            accumulate(2, qa, dx[0:128])
            accumulate(2, qb, dx[128:256])
        return step

    def attention_context():
        ag_rows(XA, 0, 4 * ROWS).wait_recv()
        pltpu.make_async_copy(xall_out.at[0:384], rows.at[XA, 0:384], w_sem.at[0]).wait()
        causal_r = lax.broadcasted_iota(jnp.int32, (256, 128), 0) % 128
        causal_c = lax.broadcasted_iota(jnp.int32, (256, 128), 1)
        keep = (causal_r >= causal_c) & (causal_r // 64 == causal_c // 64)
        qkv = lax.dot_general(rows[XA], wqkv[...], NT, preferred_element_type=F32).astype(BF)
        qkvs = [qkv[q * 128:(q + 1) * 128] for q in range(4)]
        scs = [lax.dot_general(jnp.concatenate([v[:, 0:64], v[:, 64:128]], axis=0), v[:, 128:192], NT,
                               preferred_element_type=F32) * (64 ** -0.5) for v in qkvs]
        scs = [jnp.where(keep, sc, -1e30) for sc in scs]
        mxs = [jnp.max(sc, axis=1, keepdims=True) for sc in scs]
        exs = [jnp.exp(sc - mx) for sc, mx in zip(scs, mxs)]
        sms = [jnp.sum(ex, axis=1, keepdims=True) for ex in exs]
        prs = [(ex / sm).astype(BF) for ex, sm in zip(exs, sms)]
        ctxs = [jnp.dot(pr, v[:, 192:256], preferred_element_type=F32).astype(BF) for pr, v in zip(prs, qkvs)]
        return jnp.concatenate([jnp.concatenate([v[0:128], v[128:256]], axis=1) for v in ctxs], axis=0)

    def attention_out(ctx):
        for q in range(4):
            out = jnp.dot(ctx[q * 128:(q + 1) * 128], wo[...], preferred_element_type=F32)
            for cc in range(2):
                for h in range(2):
                    part[0, cc, h, q] = out[cc * 64:(cc + 1) * 64, h * HALF:(h + 1) * HALF]

    def leave(i, n):
        rs_wait(n, 2 * OWN, 6)
        rs_wait(n, 8, 2)
        for h in range(2):
            cols = slice(h * HALF, (h + 1) * HALF)
            near = chip_sum(n, h, first[h])
            far = chip_sum(n, h, second[h]) + r1[n, h, 0]
            mine = chip_sum(n, h, OWN)
            sums[X - 1, i, :, cols] = near if h == 0 else far
            sums[Y - 1, i, :, cols] = far if h == 0 else near
            sums[2, i, :, cols] = mine
        cps = [pltpu.make_async_copy(sums.at[k, i], dst.at[i], out_sem.at[6 + k])
               for k, dst in enumerate((tox_out, toy_out, own_out))]
        for cp in cps:
            cp.start()

    pltpu.make_async_copy(xall_out.at[0:3 * ROWS], rows.at[XA, 0:3 * ROWS], in_sem.at[0]).wait()
    pl.semaphore_wait(barrier, len(rels))
    for cp in gate_cps.values():
        cp.start()
    ag_own(XT)
    ag_own(XA)
    gate_table(OWN)
    ag[XT][0].wait_recv()
    experts(forward(OWN, True), {2: lambda: ag_forward(XT)})
    rs_pair(1, OWN)
    ag_pair(XT)
    gate_table(X)
    ag[XT][7].wait_recv()
    experts(forward(X), {0: lambda: (ag_forward(XA), ag_own(DY)), 2: lambda: ag_pair(XA)})
    rs_pair(1, X)
    gate_table(Y)
    ag[XT][8].wait_recv()
    experts(forward(Y), {0: lambda: ag_last(XT), 2: lambda: ag_last(XA), 3: lambda: (ag_forward(DY), rs_near(1, 0))})
    rs_pair(1, Y)
    gate_table(DI)
    ag_rows(XT, 9, ROWS).wait_recv()
    gate_out = pltpu.make_async_copy(gt, gt_out, out_sem.at[2])
    gate_out.start()
    rows_out = pltpu.make_async_copy(rows.at[XT], xall_out, out_sem.at[0])
    rows_out.start()
    experts(forward(DI), {1: lambda: rs_near(1, 1), 2: lambda: ag_pair(DY)})
    rs_pair(1, DI)
    hid_out = pltpu.make_async_copy(hid, h_out, out_sem.at[3])
    hid_out.start()
    ctx = attention_context()
    ag_last(DY)
    rs_far(1)
    attention_out(ctx)
    for k in (DI, X, Y, OWN):
        rs_pair(0, k)
    ag_rows(DY, 0, 4 * ROWS).wait_recv()
    dys_out = pltpu.make_async_copy(rows.at[DY], dyall_out, out_sem.at[1])
    dys_out.start()
    experts(backward(2 * (1 - y), 2 * (1 - y) + 1, (1 - y) * 256, True), {0: lambda: rs_far(0), 3: lambda: rs_second(1)})
    rs_pair(2, DI)
    rs_pair(2, Y)
    for q in range(4):
        dsend[q] = dgs[q * 128:(q + 1) * 128, :].T[0:8, :]
    drecv[me] = dsend[q0]
    for cp in dg_cps.values():
        cp.start()
    experts(backward(2 * y, 2 * y + 1, y * 256, False), {0: lambda: rs_far(2)})
    rs_pair(2, X)
    rs_pair(2, OWN)
    da_cp = pltpu.make_async_copy(dag, da_out, out_sem.at[4])
    db_cp = pltpu.make_async_copy(dbg, db_out, out_sem.at[5])
    da_cp.start()
    db_cp.start()
    leave(0, 0)
    rs_wait_dg = drecv.at[0:7]
    remote(rs_wait_dg, rs_wait_dg, dd_s.at[0], dd_r.at[0], sib).wait_recv()
    both = drecv[...].reshape(64, 128)
    mine = jnp.where(c == 0, both[:, 0:ROWS], both[:, ROWS:128])
    for j in range(TOPK):
        hit = row_exp == idx_ref[j:j + 1, :]
        dg_ref[j:j + 1, :] = jnp.sum(jnp.where(hit & is_gate, mine, 0.0), axis=0, keepdims=True)
    rs_final(1, y_ref)
    small = [pltpu.make_async_copy(y_ref, y_out, out_sem.at[9]), pltpu.make_async_copy(dg_ref, dg_out, out_sem.at[10])]
    for cp in small:
        cp.start()
    leave(1, 2)

    for cp in [gate_out, rows_out, dys_out, hid_out, da_cp, db_cp] + small:
        cp.wait()
    for k, dst in enumerate((tox_out, toy_out, own_out)):
        pltpu.make_async_copy(sums.at[k], dst, out_sem.at[6 + k]).wait()
    for t in range(3):
        ref = rows.at[t, 0:7 * ROWS]
        remote(ref, ref, ag_s.at[t], ag_r.at[0], sib).wait_send()
    tiles = gsend.at[0:7]
    remote(tiles, tiles, gs_sem.at[0], gr_sem.at[0], sib).wait_send()
    remote(tiles, tiles, dd_s.at[0], dd_r.at[0], sib).wait_send()
    for n in range(3):
        for ref, k in ((part.at[n, 0], 0), (pair.at[n, :, 0:3] if n == 1 else pair.at[n, 0, 0:2], 1)):
            remote(ref, ref, rs_s.at[n, k], rs_r.at[0], sib).wait_send()


def exchange(x, dy, xa, idx, gates, wg, wu, wd, wq, wk, wv, wo):
    any_spec = pl.BlockSpec(memory_space=pl.ANY)
    sds = jax.ShapeDtypeStruct
    dma = pltpu.SemaphoreType.DMA
    return pl.pallas_call(
        exchange_kernel,
        name='exchange',
        out_shape=[sds((ROWS, D), BF), sds((TOPK, ROWS), F32)] + [sds((2, ROWS, D), F32)] * 3 + [
                   sds((TOK, D), BF), sds((TOK, D), BF),
                   sds((EXP, TOK, FF), BF), sds((EXP, TOK, FF), BF), sds((EXP, TOK, FF), BF), sds((TOK, 128), F32)],
        in_specs=[any_spec] * 12,
        out_specs=[any_spec] * 11,
        scratch_shapes=[
            pltpu.VMEM((TOPK, ROWS), jnp.int32), pltpu.VMEM((TOPK, ROWS), F32), pltpu.VMEM((ROWS, D), BF), pltpu.VMEM((TOPK, ROWS), F32),
            pltpu.VMEM((3, TOK, D), BF),
            pltpu.VMEM((EXP, D, FF), BF), pltpu.VMEM((EXP, D, FF), BF), pltpu.VMEM((EXP, FF, D), BF),
            pltpu.VMEM((256, D), BF), pltpu.VMEM((128, D), BF),
            pltpu.VMEM((EXP, TOK, FF), BF), pltpu.VMEM((EXP, TOK, D), BF),
            pltpu.VMEM((EXP, TOK, FF), BF), pltpu.VMEM((EXP, TOK, FF), BF),
            pltpu.VMEM((EXP, TOK, FF), F32), pltpu.VMEM((EXP, TOK, FF), F32),
            pltpu.VMEM((TOK, 128), F32),
            pltpu.VMEM((8, 8, 128), F32), pltpu.VMEM((8, 8, 128), F32),
            pltpu.VMEM((TOK, 128), F32), pltpu.VMEM((4, 8, 128), F32), pltpu.VMEM((8, 8, 128), F32),
            pltpu.VMEM((3, 2, ROWS, D), F32),
            pltpu.VMEM((3, 2, 2, 4, ROWS, HALF), F32), pltpu.VMEM((3, 2, 4, ROWS, HALF), F32),
            pltpu.VMEM((3, 2, 2, ROWS, HALF), F32), pltpu.VMEM((3, 2, 2, ROWS, HALF), F32),
            pltpu.VMEM((3, 2, ROWS, HALF), F32), pltpu.VMEM((3, 2, ROWS, HALF), F32),
            dma((3,)), dma((1 + EXP,)), dma((11,)), dma((1,)), dma((4,)),
            dma((3, 2)), dma((12,)), dma((3,)), dma((24,)), dma((1,)), dma((1,)),
        ],
        compiler_params=pltpu.CompilerParams(collective_id=0, has_side_effects=True, vmem_limit_bytes=60 * 1024 * 1024),
    )(x, dy, xa, idx, gates, wg, wu, wd, wq, wk, wv, wo)


def grads_kernel(x_ref, dy_ref, gt_ref, h_ref, da_ref, db_ref, y_in, dg_in,
                 dwg_ref, dwu_ref, dwd_ref, y_out, dg_out, xt):
    e = pl.program_id(0)

    @pl.when(e == 0)
    def _():
        xt[...] = x_ref[...].T
        y_out[...] = y_in[...]
        dg_out[...] = dg_in[...]

    dwg_ref[0] = jnp.dot(xt[...], da_ref[0], preferred_element_type=F32)
    dwu_ref[0] = jnp.dot(xt[...], db_ref[0], preferred_element_type=F32)
    lane = lax.broadcasted_iota(jnp.int32, (TOK, 128), 1)
    g = jnp.sum(jnp.where(lane == e, gt_ref[...], 0.0), axis=1, keepdims=True)
    do = (g * dy_ref[...].astype(F32)).astype(BF)
    dwd_ref[0] = lax.dot_general(h_ref[0], do, TN, preferred_element_type=F32)


def weight_grads(xall, dyall, gt, h, da, db, y_t, dg):
    sds = jax.ShapeDtypeStruct
    whole = lambda shape: pl.BlockSpec(shape, lambda e: (0, 0))
    per = lambda a, b: pl.BlockSpec((1, a, b), lambda e: (e, 0, 0))
    return pl.pallas_call(
        grads_kernel,
        name='weight_grads',
        grid=(EXP,),
        out_shape=[sds((EXP, D, FF), F32), sds((EXP, D, FF), F32), sds((EXP, FF, D), F32),
                   sds((ROWS, D), BF), sds((TOPK, ROWS), F32)],
        in_specs=[whole((TOK, D)), whole((TOK, D)), whole((TOK, 128)), per(TOK, FF), per(TOK, FF), per(TOK, FF)]
        + [whole((ROWS, D))] + [whole((TOPK, ROWS))],
        out_specs=[per(D, FF), per(D, FF), per(FF, D)] + [whole((ROWS, D))] + [whole((TOPK, ROWS))],
        scratch_shapes=[pltpu.VMEM((D, TOK), BF)],
        cost_estimate=pl.CostEstimate(flops=3 * 2 * EXP * TOK * D * FF, bytes_accessed=34 * 1024 * 1024, transcendentals=0),
        compiler_params=pltpu.CompilerParams(vmem_limit_bytes=62 * 1024 * 1024),
    )(xall, dyall, gt, h, da, db, y_t, dg)


def solution(mesh):
    def local_step(x_tokens, expert_idx, gate_vals, dy_tokens, w_gate, w_up, w_down, x_attn, w_query, w_key, w_value, w_out):
        y_p, dg_p, to_x, to_y, own, xall, dyall, h, da, db, gt = exchange(
            x_tokens, dy_tokens, x_attn.reshape(ROWS, D), expert_idx.T, gate_vals.T, w_gate, w_up, w_down,
            w_query.transpose(1, 2, 0).reshape(128, D), w_key.transpose(1, 2, 0).reshape(64, D),
            w_value.transpose(1, 2, 0).reshape(64, D), w_out.reshape(128, D))
        from_x = lax.ppermute(to_x, GROUP_AXES, [(g, g ^ 2) for g in range(8)])
        from_y = lax.ppermute(to_y, GROUP_AXES, [(g, g ^ 4) for g in range(8)])
        dwg, dwu, dwd, y_t, dg = weight_grads(xall, dyall, gt, h, da, db, y_p, dg_p)
        both = (own + from_x + from_y).astype(BF)
        at, dx_t = both[0], both[1]
        return y_t, dx_t, dg.T, dwg, dwu, dwd, at.reshape(1, ROWS, D)

    spec_rows = P(TOKEN_AXES, None)
    spec_seqs = P(TOKEN_AXES, None, None)
    spec_experts = P(GROUP_AXES, None, None)
    spec_heads = P(None, GROUP_AXES, None)
    return jax.shard_map(local_step, mesh=mesh,
                         in_specs=(spec_rows, spec_rows, spec_rows, spec_rows, spec_experts, spec_experts, spec_experts, spec_seqs, spec_heads, spec_heads, spec_heads, spec_experts),
                         out_specs=(spec_rows, spec_rows, spec_rows, spec_seqs, spec_seqs, spec_seqs, spec_seqs),
                         check_vma=False)
```

```python
import functools

import jax
import jax.numpy as jnp
from jax import lax
from jax.experimental import pallas as pl
from jax.experimental.pallas import tpu as pltpu
from jax.sharding import PartitionSpec as P

MESH = pl.DeviceIdType.MESH
GROUP_AXES = ('ei', 'eo')
TOKEN_AXES = ('dp', 'ei', 'eo')
BF = jnp.bfloat16
F32 = jnp.float32

ROWS = 64
TOK = 512
D = 1024
FF = 512
HALF = 512
EXP = 4
TOPK = 8
XA, XT, DY = 0, 1, 2

NT = (((1,), (1,)), ((), ()))
TN = (((0,), (0,)), ((), ()))


def exchange_kernel(x_hbm, dy_hbm, xa_hbm, idx_hbm, gate_hbm, wg_hbm, wu_hbm, wd_hbm, wq_hbm, wk_hbm, wv_hbm, wo_hbm,
                    y_out, dg_out, tox_out, toy_out, own_out, xall_out, dyall_out, h_out, da_out, db_out, gt_out,
                    idx_ref, gate_ref, y_ref, dg_ref, rows, wg, wu, wd, wqkv, wo, hid, osv, dag, dbg, act, gfac, gt, gsend, grecv,
                    dgs, dsend, drecv,
                    sums, part, pair, s1, r1, s2, r2,
                    in_sem, w_sem, out_sem, gs_sem, gr_sem, rs_s, rs_r, ag_s, ag_r, dd_s, dd_r):
    y = lax.axis_index('ei')
    o = lax.axis_index('eo')
    z = lax.axis_index('dp')
    x = o // 2
    c = o % 2
    me = y * 4 + o
    q0 = 2 * y + x
    qx = 2 * y + (1 - x)
    qy = 2 * (1 - y) + x
    qd = 2 * (1 - y) + (1 - x)

    def dev(fx, fy, fc):
        xx = (1 - x) if fx else x
        yy = (1 - y) if fy else y
        cc = (1 - c) if fc else c
        return (z, yy, xx * 2 + cc)

    sib, xn, yn = dev(0, 0, 1), dev(1, 0, 0), dev(0, 1, 0)
    rels = [(fx, fy, fc) for fx in (0, 1) for fy in (0, 1) for fc in (0, 1) if fx or fy or fc]

    barrier = pltpu.get_barrier_semaphore()
    for rel in rels:
        pl.semaphore_signal(barrier, inc=1, device_id=dev(*rel), device_id_type=MESH)

    own = pl.ds(pl.multiple_of(me * ROWS, ROWS), ROWS)
    tables = [pltpu.make_async_copy(idx_hbm, idx_ref, in_sem.at[1]), pltpu.make_async_copy(gate_hbm, gate_ref, in_sem.at[2])]
    for cp in tables:
        cp.start()
    for t, src in ((XT, x_hbm), (DY, dy_hbm), (XA, xa_hbm)):
        pltpu.make_async_copy(src, rows.at[t, own], in_sem.at[0]).start()

    def expert_load(e):
        return [pltpu.make_async_copy(src.at[e], dst.at[e], w_sem.at[1 + e])
                for src, dst in ((wg_hbm, wg), (wu_hbm, wu), (wd_hbm, wd))]

    for e in range(EXP):
        for cp in expert_load(e):
            cp.start()
    wload = [pltpu.make_async_copy(wq_hbm, wqkv.at[0:128], w_sem.at[0]),
             pltpu.make_async_copy(wk_hbm, wqkv.at[128:192], w_sem.at[0]),
             pltpu.make_async_copy(wv_hbm, wqkv.at[192:256], w_sem.at[0]),
             pltpu.make_async_copy(wo_hbm, wo, w_sem.at[0])]
    for cp in wload:
        cp.start()

    for cp in tables:
        cp.wait()
    row = lax.broadcasted_iota(jnp.int32, (64, ROWS), 0)
    row_exp = (row // 8) * 4 + row % 4
    is_gate = (row % 8) < 4
    table = jnp.zeros((64, ROWS), F32)
    for j in range(TOPK):
        hit = row_exp == idx_ref[j:j + 1, :]
        table = table + jnp.where(hit, jnp.where(is_gate, gate_ref[j:j + 1, :], 1.0), 0.0)
    blank = jnp.zeros((64, ROWS), F32)
    wide = jnp.where(c == 0, jnp.concatenate([table, blank], axis=1), jnp.concatenate([blank, table], axis=1))
    for d in range(8):
        gsend[d] = wide[d * 8:(d + 1) * 8, :]
    grecv[me] = gsend[me]
    dgs[...] = jnp.zeros((TOK, 128), F32)
    part[1] = jnp.zeros(part.shape[1:], F32)
    part[2] = jnp.zeros(part.shape[1:], F32)

    def blk(t, q, off=0, n=ROWS):
        return rows.at[t, pl.ds(pl.multiple_of(q * 128 + c * ROWS + off, 32), n)]

    def remote(src, dst, ss, rs, where):
        return pltpu.make_async_remote_copy(src, dst, ss, rs, device_id=where, device_id_type=MESH)

    hr = ROWS // 2

    def gather_slot(t, k):
        if t == XT:
            return min(k, 9)
        return (10 if t == XA else 17) + (k - 1 if 1 <= k <= 6 else 6)

    def gather_copies(t):
        def cp(k, ref, where):
            return remote(ref, ref, ag_s.at[t], ag_r.at[gather_slot(t, k)], where)
        return [cp(0, blk(t, q0), sib),
                cp(1, blk(t, q0, 0, hr), xn), cp(2, blk(t, q0, hr, hr), xn),
                cp(3, blk(t, q0, hr, hr), yn), cp(4, blk(t, q0, 0, hr), yn),
                cp(5, blk(t, qx, 0, hr), yn), cp(6, blk(t, qy, hr, hr), xn),
                cp(7, blk(t, qx), sib), cp(8, blk(t, qy), sib),
                cp(9, blk(t, qd, 0, hr), sib), cp(10, blk(t, qd, hr, hr), sib)]

    ag = [gather_copies(t) for t in range(3)]

    def ag_own(t):
        for k in (1, 3, 2, 4, 0):
            ag[t][k].start()

    def ag_own_a(t):
        ag[t][1].start()
        ag[t][3].start()

    def ag_own_b(t):
        for k in (2, 4, 0):
            ag[t][k].start()

    def ag_forward(t):
        ag[t][1].wait_recv()
        ag[t][5].start()
        ag[t][3].wait_recv()
        ag[t][6].start()

    def ag_pair(t):
        ag[t][2].wait_recv()
        ag[t][7].start()
        ag[t][4].wait_recv()
        ag[t][8].start()

    def ag_last(t):
        ag[t][5].wait_recv()
        ag[t][9].start()
        ag[t][6].wait_recv()
        ag[t][10].start()

    def ag_rows(t, k, n):
        ref = rows.at[t, 0:n]
        return remote(ref, ref, ag_s.at[t], ag_r.at[gather_slot(t, k)], sib)

    def tile_copies(send, recv, ss, rs, chip_tiles):
        cps = {}
        for fx, fy, fc in rels:
            where = dev(fx, fy, fc)
            qq = 2 * where[1] + where[2] // 2
            src = send.at[qq] if chip_tiles else send.at[where[1] * 4 + where[2]]
            cps[fx, fy, fc] = remote(src, recv.at[me], ss.at[0], rs.at[0 if chip_tiles else fx + 2 * fy], where)
        return cps

    gate_cps = tile_copies(gsend, grecv, gs_sem, gr_sem, False)
    dg_cps = tile_copies(dsend, drecv, dd_s, dd_r, True)
    chips = (q0, qx, qy, qd)
    OWN, X, Y, DI = 0, 1, 2, 3
    first = (X, Y)
    second = (Y, X)

    def rs_slot(n, k):
        if k >= 8:
            kind = (k - 8) % 3
            group = 2 if kind == 0 else 1
        else:
            group = 0 if k // 2 == DI else 1
            if n == 1 and k // 2 in (X, Y):
                group = 3 if k == 2 * X else 4 if k == 2 * Y + 1 else 5
        return (0, 3, 9)[n] + group

    def rs_wait(n, k, count):
        ref = pair.at[n, 0, 0:2] if count == 2 else pair.at[n, :, 0:3] if count == 6 else pair.at[n, 0, 0]
        remote(ref, ref, rs_s.at[n, 0], rs_r.at[rs_slot(n, k)], sib).wait_recv()

    def rs_copies(n):
        def cp(k, src, dst, where):
            return remote(src, dst, rs_s.at[n, 0 if k < 8 else 1], rs_r.at[rs_slot(n, k)], where)
        cps = [cp(2 * k + h, part.at[n, 1 - c, h, chips[k]], pair.at[n, h, chips[k]], sib) for k in range(4) for h in range(2)]
        for h in range(2):
            one, two = (xn, yn) if h == 0 else (yn, xn)
            cps += [cp(8 + 3 * h, s1.at[n, h, 0], r1.at[n, h, 0], one), cp(9 + 3 * h, s1.at[n, h, 1], r1.at[n, h, 1], one),
                    cp(10 + 3 * h, s2.at[n, h], r2.at[n, h], two)]
        return cps

    rsc = [rs_copies(n) for n in range(3)]

    def rs_pair(n, k):
        rsc[n][2 * k].start()
        rsc[n][2 * k + 1].start()

    def chip_sum(n, h, k):
        return part[n, c, h, chips[k]] + pair[n, h, chips[k]]

    def rs_far(n):
        rs_wait(n, 2 * DI, 2)
        for h in range(2):
            s1[n, h, 0] = chip_sum(n, h, DI)
            rsc[n][8 + 3 * h].start()

    def rs_near(n, h):
        k = first[h]
        rs_wait(n, 2 * k + h, 1)
        s1[n, h, 1] = chip_sum(n, h, k)
        rsc[n][9 + 3 * h].start()

    def rs_second(n):
        rs_wait(n, 2 * Y, 2)
        rs_wait(n, 8, 2)
        for h in range(2):
            k = second[h]
            s2[n, h] = chip_sum(n, h, k) + r1[n, h, 0]
            rsc[n][10 + 3 * h].start()

    def rs_final(n, out_ref):
        rs_wait(n, 2 * OWN, 6)
        for h in range(2):
            total = chip_sum(n, h, OWN) + r1[n, h, 1] + r2[n, h]
            out_ref[:, h * HALF:(h + 1) * HALF] = total.astype(BF)

    def gate_table(k):
        tiles = grecv.at[0:1 if k == OWN else 2]
        remote(tiles, tiles, gs_sem.at[0], gr_sem.at[k], sib).wait_recv()
        q = chips[k]
        tile = grecv[2 * q] + grecv[2 * q + 1]
        gt[pl.ds(pl.multiple_of(q * 128, 128), 128), :] = jnp.concatenate([tile, jnp.zeros((120, 128), F32)], axis=0).T

    def pick(tile, e):
        lane = lax.broadcasted_iota(jnp.int32, tile.shape, 1)
        return jnp.sum(jnp.where(lane == e, tile, 0.0), axis=1, keepdims=True)

    def accumulate(n, q, val):
        for cc in range(2):
            for h in range(2):
                part[n, cc, h, q] += val[cc * 64:(cc + 1) * 64, h * HALF:(h + 1) * HALF]

    def experts(step, hooks):
        def body(e, carry):
            step(e)
            for at, fn in hooks.items():
                @pl.when(e == at)
                def _():
                    fn()
            return carry
        lax.fori_loop(0, EXP, body, 0)

    def chip_rows(k):
        return pl.ds(pl.multiple_of(chips[k] * 128, 128), 128)

    def forward(ks, load=False):
        def stack(ref, *at):
            return jnp.concatenate([ref[(*at, chip_rows(k), slice(None))] for k in ks], axis=0)

        def step(e):
            if load:
                pltpu.make_async_copy(wg_hbm.at[0:3], wg.at[0:3], w_sem.at[1 + e]).wait()

            def put(ref, val):
                for i, k in enumerate(ks):
                    ref[e, chip_rows(k), :] = val[i * 128:(i + 1) * 128]

            xs = stack(rows, XT)
            a = jnp.dot(xs, wg[e], preferred_element_type=F32)
            b = jnp.dot(xs, wu[e], preferred_element_type=F32)
            tile = stack(gt)
            mark = pick(tile, e + 4) > 0.5
            sg = jax.nn.sigmoid(a)
            ac = a * sg
            put(act, jnp.where(mark, ac, 0.0))
            put(gfac, jnp.where(mark, b * sg * (1.0 + a * (1.0 - sg)), 0.0))
            hh = jnp.where(mark, ac * b, 0.0).astype(BF)
            put(hid, hh)
            ob = jnp.dot(hh, wd[e], preferred_element_type=F32).astype(BF)
            put(osv, ob)
            yb = pick(tile, e) * ob.astype(F32)
            for i, k in enumerate(ks):
                accumulate(1, chips[k], yb[i * 128:(i + 1) * 128])
        return step

    def backward(qa, qb, base, gates):
        sl = pl.ds(pl.multiple_of(base, 256), 256)

        def step(e):
            g = pick(gt[sl, :], e)
            dyf = rows[DY, sl, :].astype(F32)
            do = (g * dyf).astype(BF)
            dh = lax.dot_general(do, wd[e], NT, preferred_element_type=F32).astype(BF).astype(F32)
            da = (dh * gfac[e, sl, :]).astype(BF)
            db = (dh * act[e, sl, :]).astype(BF)
            dag[e, sl, :] = da
            dbg[e, sl, :] = db
            if gates:
                lane = lax.broadcasted_iota(jnp.int32, (256, 128), 1)
                for r in (slice(0, 256), slice(256, 512)):
                    dg = jnp.sum(rows[DY, r, :].astype(F32) * osv[e, r, :].astype(F32), axis=1, keepdims=True)
                    dgs[r, :] += jnp.where(lane == e, dg, 0.0)
            dx = (lax.dot_general(da, wg[e], NT, preferred_element_type=F32)
                  + lax.dot_general(db, wu[e], NT, preferred_element_type=F32)).astype(BF).astype(F32)
            accumulate(2, qa, dx[0:128])
            accumulate(2, qb, dx[128:256])
        return step

    def attention_context():
        ag_rows(XA, 0, 4 * ROWS).wait_recv()
        pltpu.make_async_copy(xall_out.at[0:384], rows.at[XA, 0:384], w_sem.at[0]).wait()
        causal_r = lax.broadcasted_iota(jnp.int32, (256, 128), 0) % 128
        causal_c = lax.broadcasted_iota(jnp.int32, (256, 128), 1)
        keep = (causal_r >= causal_c) & (causal_r // 64 == causal_c // 64)
        qkv = lax.dot_general(rows[XA], wqkv[...], NT, preferred_element_type=F32).astype(BF)
        qkvs = [qkv[q * 128:(q + 1) * 128] for q in range(4)]
        scs = [lax.dot_general(jnp.concatenate([v[:, 0:64], v[:, 64:128]], axis=0), v[:, 128:192], NT,
                               preferred_element_type=F32) * (64 ** -0.5) for v in qkvs]
        scs = [jnp.where(keep, sc, -1e30) for sc in scs]
        mxs = [jnp.max(sc, axis=1, keepdims=True) for sc in scs]
        exs = [jnp.exp(sc - mx) for sc, mx in zip(scs, mxs)]
        sms = [jnp.sum(ex, axis=1, keepdims=True) for ex in exs]
        prs = [(ex / sm).astype(BF) for ex, sm in zip(exs, sms)]
        ctxs = [jnp.dot(pr, v[:, 192:256], preferred_element_type=F32).astype(BF) for pr, v in zip(prs, qkvs)]
        return jnp.concatenate([jnp.concatenate([v[0:128], v[128:256]], axis=1) for v in ctxs], axis=0)

    def attention_out(ctx):
        for q in range(4):
            out = jnp.dot(ctx[q * 128:(q + 1) * 128], wo[...], preferred_element_type=F32)
            for cc in range(2):
                for h in range(2):
                    part[0, cc, h, q] = out[cc * 64:(cc + 1) * 64, h * HALF:(h + 1) * HALF]

    def leave(i, n):
        rs_wait(n, 2 * OWN, 6)
        rs_wait(n, 8, 2)
        for h in range(2):
            cols = slice(h * HALF, (h + 1) * HALF)
            near = chip_sum(n, h, first[h])
            far = chip_sum(n, h, second[h]) + r1[n, h, 0]
            mine = chip_sum(n, h, OWN)
            sums[X - 1, i, :, cols] = near if h == 0 else far
            sums[Y - 1, i, :, cols] = far if h == 0 else near
            sums[2, i, :, cols] = mine
        cps = [pltpu.make_async_copy(sums.at[k, i], dst.at[i], out_sem.at[6 + k])
               for k, dst in enumerate((tox_out, toy_out, own_out))]
        for cp in cps:
            cp.start()

    pltpu.make_async_copy(xall_out.at[0:3 * ROWS], rows.at[XA, 0:3 * ROWS], in_sem.at[0]).wait()
    pl.semaphore_wait(barrier, len(rels))
    for cp in gate_cps.values():
        cp.start()
    ag_own(XT)
    ag_own(XA)
    gate_table(OWN)
    ag[XT][0].wait_recv()
    experts(forward([OWN], True), {2: lambda: ag_forward(XT)})
    rs_pair(1, OWN)
    ag_pair(XT)
    gate_table(X)
    gate_table(Y)
    ag_own_a(DY)
    ag[XT][7].wait_recv()
    ag[XT][8].wait_recv()
    experts(forward([X, Y]), {0: lambda: (ag_forward(XA), ag_own_b(DY)), 1: lambda: ag_pair(XA), 2: lambda: ag_last(XT)})
    rs_pair(1, X)
    rs_pair(1, Y)
    gate_table(DI)
    ag_forward(DY)
    gate_out = pltpu.make_async_copy(gt, gt_out, out_sem.at[2])
    gate_out.start()
    ag_rows(XT, 9, ROWS).wait_recv()
    rows_out = pltpu.make_async_copy(rows.at[XT], xall_out, out_sem.at[0])
    rows_out.start()
    experts(forward([DI]), {1: lambda: (rs_near(1, 0), rs_near(1, 1), ag_last(XA)), 2: lambda: ag_pair(DY)})
    rs_pair(1, DI)
    hid_out = pltpu.make_async_copy(hid, h_out, out_sem.at[3])
    hid_out.start()
    ctx = attention_context()
    ag_last(DY)
    rs_far(1)
    attention_out(ctx)
    for k in (DI, X, Y, OWN):
        rs_pair(0, k)
    ag_rows(DY, 0, 4 * ROWS).wait_recv()
    dys_out = pltpu.make_async_copy(rows.at[DY], dyall_out, out_sem.at[1])
    dys_out.start()
    experts(backward(2 * (1 - y), 2 * (1 - y) + 1, (1 - y) * 256, True), {0: lambda: rs_far(0), 2: lambda: rs_second(1)})
    rs_pair(2, DI)
    rs_pair(2, Y)
    for q in range(4):
        dsend[q] = dgs[q * 128:(q + 1) * 128, :].T[0:8, :]
    drecv[me] = dsend[q0]
    for cp in dg_cps.values():
        cp.start()
    experts(backward(2 * y, 2 * y + 1, y * 256, False), {0: lambda: rs_far(2)})
    rs_pair(2, X)
    rs_pair(2, OWN)
    da_cp = pltpu.make_async_copy(dag, da_out, out_sem.at[4])
    db_cp = pltpu.make_async_copy(dbg, db_out, out_sem.at[5])
    da_cp.start()
    db_cp.start()
    leave(0, 0)
    rs_wait_dg = drecv.at[0:7]
    remote(rs_wait_dg, rs_wait_dg, dd_s.at[0], dd_r.at[0], sib).wait_recv()
    both = drecv[...].reshape(64, 128)
    mine = jnp.where(c == 0, both[:, 0:ROWS], both[:, ROWS:128])
    for j in range(TOPK):
        hit = row_exp == idx_ref[j:j + 1, :]
        dg_ref[j:j + 1, :] = jnp.sum(jnp.where(hit & is_gate, mine, 0.0), axis=0, keepdims=True)
    rs_final(1, y_ref)
    small = [pltpu.make_async_copy(y_ref, y_out, out_sem.at[9]), pltpu.make_async_copy(dg_ref, dg_out, out_sem.at[10])]
    for cp in small:
        cp.start()
    leave(1, 2)

    for cp in [gate_out, rows_out, dys_out, hid_out, da_cp, db_cp] + small:
        cp.wait()
    for k, dst in enumerate((tox_out, toy_out, own_out)):
        pltpu.make_async_copy(sums.at[k], dst, out_sem.at[6 + k]).wait()
    for t in range(3):
        ref = rows.at[t, 0:7 * ROWS]
        remote(ref, ref, ag_s.at[t], ag_r.at[0], sib).wait_send()
    tiles = gsend.at[0:7]
    remote(tiles, tiles, gs_sem.at[0], gr_sem.at[0], sib).wait_send()
    remote(tiles, tiles, dd_s.at[0], dd_r.at[0], sib).wait_send()
    for n in range(3):
        for ref, k in ((part.at[n, 0], 0), (pair.at[n, :, 0:3] if n == 1 else pair.at[n, 0, 0:2], 1)):
            remote(ref, ref, rs_s.at[n, k], rs_r.at[0], sib).wait_send()


def exchange(x, dy, xa, idx, gates, wg, wu, wd, wq, wk, wv, wo):
    any_spec = pl.BlockSpec(memory_space=pl.ANY)
    sds = jax.ShapeDtypeStruct
    dma = pltpu.SemaphoreType.DMA
    return pl.pallas_call(
        exchange_kernel,
        name='exchange',
        out_shape=[sds((ROWS, D), BF), sds((TOPK, ROWS), F32)] + [sds((2, ROWS, D), F32)] * 3 + [
                   sds((TOK, D), BF), sds((TOK, D), BF),
                   sds((EXP, TOK, FF), BF), sds((EXP, TOK, FF), BF), sds((EXP, TOK, FF), BF), sds((TOK, 128), F32)],
        in_specs=[any_spec] * 12,
        out_specs=[any_spec] * 11,
        scratch_shapes=[
            pltpu.VMEM((TOPK, ROWS), jnp.int32), pltpu.VMEM((TOPK, ROWS), F32), pltpu.VMEM((ROWS, D), BF), pltpu.VMEM((TOPK, ROWS), F32),
            pltpu.VMEM((3, TOK, D), BF),
            pltpu.VMEM((EXP, D, FF), BF), pltpu.VMEM((EXP, D, FF), BF), pltpu.VMEM((EXP, FF, D), BF),
            pltpu.VMEM((256, D), BF), pltpu.VMEM((128, D), BF),
            pltpu.VMEM((EXP, TOK, FF), BF), pltpu.VMEM((EXP, TOK, D), BF),
            pltpu.VMEM((EXP, TOK, FF), BF), pltpu.VMEM((EXP, TOK, FF), BF),
            pltpu.VMEM((EXP, TOK, FF), F32), pltpu.VMEM((EXP, TOK, FF), F32),
            pltpu.VMEM((TOK, 128), F32),
            pltpu.VMEM((8, 8, 128), F32), pltpu.VMEM((8, 8, 128), F32),
            pltpu.VMEM((TOK, 128), F32), pltpu.VMEM((4, 8, 128), F32), pltpu.VMEM((8, 8, 128), F32),
            pltpu.VMEM((3, 2, ROWS, D), F32),
            pltpu.VMEM((3, 2, 2, 4, ROWS, HALF), F32), pltpu.VMEM((3, 2, 4, ROWS, HALF), F32),
            pltpu.VMEM((3, 2, 2, ROWS, HALF), F32), pltpu.VMEM((3, 2, 2, ROWS, HALF), F32),
            pltpu.VMEM((3, 2, ROWS, HALF), F32), pltpu.VMEM((3, 2, ROWS, HALF), F32),
            dma((3,)), dma((1 + EXP,)), dma((11,)), dma((1,)), dma((4,)),
            dma((3, 2)), dma((12,)), dma((3,)), dma((24,)), dma((1,)), dma((1,)),
        ],
        compiler_params=pltpu.CompilerParams(collective_id=0, has_side_effects=True, vmem_limit_bytes=60 * 1024 * 1024),
    )(x, dy, xa, idx, gates, wg, wu, wd, wq, wk, wv, wo)


def grads_kernel(x_ref, dy_ref, gt_ref, h_ref, da_ref, db_ref, y_in, dg_in,
                 dwg_ref, dwu_ref, dwd_ref, y_out, dg_out, xt):
    e = pl.program_id(0)

    @pl.when(e == 0)
    def _():
        xt[...] = x_ref[...].T
        y_out[...] = y_in[...]
        dg_out[...] = dg_in[...]

    dwg_ref[0] = jnp.dot(xt[...], da_ref[0], preferred_element_type=F32)
    dwu_ref[0] = jnp.dot(xt[...], db_ref[0], preferred_element_type=F32)
    lane = lax.broadcasted_iota(jnp.int32, (TOK, 128), 1)
    g = jnp.sum(jnp.where(lane == e, gt_ref[...], 0.0), axis=1, keepdims=True)
    do = (g * dy_ref[...].astype(F32)).astype(BF)
    dwd_ref[0] = lax.dot_general(h_ref[0], do, TN, preferred_element_type=F32)


def weight_grads(xall, dyall, gt, h, da, db, y_t, dg):
    sds = jax.ShapeDtypeStruct
    whole = lambda shape: pl.BlockSpec(shape, lambda e: (0, 0))
    per = lambda a, b: pl.BlockSpec((1, a, b), lambda e: (e, 0, 0))
    return pl.pallas_call(
        grads_kernel,
        name='weight_grads',
        grid=(EXP,),
        out_shape=[sds((EXP, D, FF), F32), sds((EXP, D, FF), F32), sds((EXP, FF, D), F32),
                   sds((ROWS, D), BF), sds((TOPK, ROWS), F32)],
        in_specs=[whole((TOK, D)), whole((TOK, D)), whole((TOK, 128)), per(TOK, FF), per(TOK, FF), per(TOK, FF)]
        + [whole((ROWS, D))] + [whole((TOPK, ROWS))],
        out_specs=[per(D, FF), per(D, FF), per(FF, D)] + [whole((ROWS, D))] + [whole((TOPK, ROWS))],
        scratch_shapes=[pltpu.VMEM((D, TOK), BF)],
        cost_estimate=pl.CostEstimate(flops=3 * 2 * EXP * TOK * D * FF, bytes_accessed=34 * 1024 * 1024, transcendentals=0),
        compiler_params=pltpu.CompilerParams(vmem_limit_bytes=62 * 1024 * 1024),
    )(xall, dyall, gt, h, da, db, y_t, dg)


def solution(mesh):
    def local_step(x_tokens, expert_idx, gate_vals, dy_tokens, w_gate, w_up, w_down, x_attn, w_query, w_key, w_value, w_out):
        y_p, dg_p, to_x, to_y, own, xall, dyall, h, da, db, gt = exchange(
            x_tokens, dy_tokens, x_attn.reshape(ROWS, D), expert_idx.T, gate_vals.T, w_gate, w_up, w_down,
            w_query.transpose(1, 2, 0).reshape(128, D), w_key.transpose(1, 2, 0).reshape(64, D),
            w_value.transpose(1, 2, 0).reshape(64, D), w_out.reshape(128, D))
        from_x = lax.ppermute(to_x, GROUP_AXES, [(g, g ^ 2) for g in range(8)])
        from_y = lax.ppermute(to_y, GROUP_AXES, [(g, g ^ 4) for g in range(8)])
        dwg, dwu, dwd, y_t, dg = weight_grads(xall, dyall, gt, h, da, db, y_p, dg_p)
        both = (own + from_x + from_y).astype(BF)
        at, dx_t = both[0], both[1]
        return y_t, dx_t, dg.T, dwg, dwu, dwd, at.reshape(1, ROWS, D)

    spec_rows = P(TOKEN_AXES, None)
    spec_seqs = P(TOKEN_AXES, None, None)
    spec_experts = P(GROUP_AXES, None, None)
    spec_heads = P(None, GROUP_AXES, None)
    return jax.shard_map(local_step, mesh=mesh,
                         in_specs=(spec_rows, spec_rows, spec_rows, spec_rows, spec_experts, spec_experts, spec_experts, spec_seqs, spec_heads, spec_heads, spec_heads, spec_experts),
                         out_specs=(spec_rows, spec_rows, spec_rows, spec_seqs, spec_seqs, spec_seqs, spec_seqs),
                         check_vma=False)
```

```python
import functools

import jax
import jax.numpy as jnp
from jax import lax
from jax.experimental import pallas as pl
from jax.experimental.pallas import tpu as pltpu
from jax.sharding import PartitionSpec as P

MESH = pl.DeviceIdType.MESH
GROUP_AXES = ('ei', 'eo')
TOKEN_AXES = ('dp', 'ei', 'eo')
BF = jnp.bfloat16
F32 = jnp.float32

ROWS = 64
TOK = 512
D = 1024
FF = 512
HALF = 512
EXP = 4
TOPK = 8
XA, XT, DY = 0, 1, 2

NT = (((1,), (1,)), ((), ()))
TN = (((0,), (0,)), ((), ()))


def exchange_kernel(x_hbm, dy_hbm, xa_hbm, idx_hbm, gate_hbm, wg_hbm, wu_hbm, wd_hbm, wq_hbm, wk_hbm, wv_hbm, wo_hbm,
                    y_out, dg_out, tox, toy, owns, xall, dyall, hid, dag, dbg, gt,
                    idx_ref, gate_ref, rows, wg, wu, wd, wqkv, wo, osv, act, gfac, gsend, grecv,
                    dgs, dsend, drecv,
                    part, pair, s1, r1, s2, r2,
                    in_sem, w_sem, gs_sem, gr_sem, rs_s, rs_r, ag_s, ag_r, dd_s, dd_r):
    y = lax.axis_index('ei')
    o = lax.axis_index('eo')
    z = lax.axis_index('dp')
    x = o // 2
    c = o % 2
    me = y * 4 + o
    q0 = 2 * y + x
    qx = 2 * y + (1 - x)
    qy = 2 * (1 - y) + x
    qd = 2 * (1 - y) + (1 - x)

    def dev(fx, fy, fc):
        xx = (1 - x) if fx else x
        yy = (1 - y) if fy else y
        cc = (1 - c) if fc else c
        return (z, yy, xx * 2 + cc)

    sib, xn, yn = dev(0, 0, 1), dev(1, 0, 0), dev(0, 1, 0)
    rels = [(fx, fy, fc) for fx in (0, 1) for fy in (0, 1) for fc in (0, 1) if fx or fy or fc]

    barrier = pltpu.get_barrier_semaphore()
    for rel in rels:
        pl.semaphore_signal(barrier, inc=1, device_id=dev(*rel), device_id_type=MESH)

    own = pl.ds(pl.multiple_of(me * ROWS, ROWS), ROWS)
    tables = [pltpu.make_async_copy(idx_hbm, idx_ref, in_sem.at[1]), pltpu.make_async_copy(gate_hbm, gate_ref, in_sem.at[2])]
    for cp in tables:
        cp.start()
    for t, src in ((XT, x_hbm), (DY, dy_hbm), (XA, xa_hbm)):
        pltpu.make_async_copy(src, rows.at[t, own], in_sem.at[0]).start()

    def expert_load(e):
        return [pltpu.make_async_copy(src.at[e], dst.at[e], w_sem.at[1 + e])
                for src, dst in ((wg_hbm, wg), (wu_hbm, wu), (wd_hbm, wd))]

    for e in range(EXP):
        for cp in expert_load(e):
            cp.start()
    wload = [pltpu.make_async_copy(wq_hbm, wqkv.at[0:128], w_sem.at[0]),
             pltpu.make_async_copy(wk_hbm, wqkv.at[128:192], w_sem.at[0]),
             pltpu.make_async_copy(wv_hbm, wqkv.at[192:256], w_sem.at[0]),
             pltpu.make_async_copy(wo_hbm, wo, w_sem.at[0])]
    for cp in wload:
        cp.start()

    for cp in tables:
        cp.wait()
    row = lax.broadcasted_iota(jnp.int32, (64, ROWS), 0)
    row_exp = (row // 8) * 4 + row % 4
    is_gate = (row % 8) < 4
    table = jnp.zeros((64, ROWS), F32)
    for j in range(TOPK):
        hit = row_exp == idx_ref[j:j + 1, :]
        table = table + jnp.where(hit, jnp.where(is_gate, gate_ref[j:j + 1, :], 1.0), 0.0)
    blank = jnp.zeros((64, ROWS), F32)
    wide = jnp.where(c == 0, jnp.concatenate([table, blank], axis=1), jnp.concatenate([blank, table], axis=1))
    for d in range(8):
        gsend[d] = wide[d * 8:(d + 1) * 8, :]
    grecv[me] = gsend[me]
    dgs[...] = jnp.zeros((TOK, 128), F32)
    part[1] = jnp.zeros(part.shape[1:], F32)
    part[2] = jnp.zeros(part.shape[1:], F32)

    def blk(t, q, off=0, n=ROWS):
        return rows.at[t, pl.ds(pl.multiple_of(q * 128 + c * ROWS + off, 32), n)]

    def remote(src, dst, ss, rs, where):
        return pltpu.make_async_remote_copy(src, dst, ss, rs, device_id=where, device_id_type=MESH)

    hr = ROWS // 2

    def gather_slot(t, k):
        if t == XT:
            return min(k, 9)
        return (10 if t == XA else 17) + (k - 1 if 1 <= k <= 6 else 6)

    def gather_copies(t):
        def cp(k, ref, where):
            return remote(ref, ref, ag_s.at[t], ag_r.at[gather_slot(t, k)], where)
        return [cp(0, blk(t, q0), sib),
                cp(1, blk(t, q0, 0, hr), xn), cp(2, blk(t, q0, hr, hr), xn),
                cp(3, blk(t, q0, hr, hr), yn), cp(4, blk(t, q0, 0, hr), yn),
                cp(5, blk(t, qx, 0, hr), yn), cp(6, blk(t, qy, hr, hr), xn),
                cp(7, blk(t, qx), sib), cp(8, blk(t, qy), sib),
                cp(9, blk(t, qd, 0, hr), sib), cp(10, blk(t, qd, hr, hr), sib)]

    ag = [gather_copies(t) for t in range(3)]

    def ag_own(t):
        for k in (1, 3, 2, 4, 0):
            ag[t][k].start()

    def ag_own_a(t):
        ag[t][1].start()
        ag[t][3].start()

    def ag_own_b(t):
        for k in (2, 4, 0):
            ag[t][k].start()

    def ag_forward(t):
        ag[t][1].wait_recv()
        ag[t][5].start()
        ag[t][3].wait_recv()
        ag[t][6].start()

    def ag_pair(t):
        ag[t][2].wait_recv()
        ag[t][7].start()
        ag[t][4].wait_recv()
        ag[t][8].start()

    def ag_last(t):
        ag[t][5].wait_recv()
        ag[t][9].start()
        ag[t][6].wait_recv()
        ag[t][10].start()

    def ag_rows(t, k, n):
        ref = rows.at[t, 0:n]
        return remote(ref, ref, ag_s.at[t], ag_r.at[gather_slot(t, k)], sib)

    def tile_copies(send, recv, ss, rs, chip_tiles):
        cps = {}
        for fx, fy, fc in rels:
            where = dev(fx, fy, fc)
            qq = 2 * where[1] + where[2] // 2
            src = send.at[qq] if chip_tiles else send.at[where[1] * 4 + where[2]]
            cps[fx, fy, fc] = remote(src, recv.at[me], ss.at[0], rs.at[0 if chip_tiles else fx + 2 * fy], where)
        return cps

    gate_cps = tile_copies(gsend, grecv, gs_sem, gr_sem, False)
    dg_cps = tile_copies(dsend, drecv, dd_s, dd_r, True)
    chips = (q0, qx, qy, qd)
    OWN, X, Y, DI = 0, 1, 2, 3
    first = (X, Y)
    second = (Y, X)

    def rs_slot(n, k):
        if k >= 8:
            kind = (k - 8) % 3
            group = 2 if kind == 0 else 1
        else:
            group = 0 if k // 2 == DI else 1
            if n == 1 and k // 2 in (X, Y):
                group = 3 if k == 2 * X else 4 if k == 2 * Y + 1 else 5
        return (0, 3, 9)[n] + group

    def rs_wait(n, k, count):
        ref = pair.at[n, 0, 0:2] if count == 2 else pair.at[n, :, 0:3] if count == 6 else pair.at[n, 0, 0]
        remote(ref, ref, rs_s.at[n, 0], rs_r.at[rs_slot(n, k)], sib).wait_recv()

    def rs_copies(n):
        def cp(k, src, dst, where):
            return remote(src, dst, rs_s.at[n, 0 if k < 8 else 1], rs_r.at[rs_slot(n, k)], where)
        cps = [cp(2 * k + h, part.at[n, 1 - c, h, chips[k]], pair.at[n, h, chips[k]], sib) for k in range(4) for h in range(2)]
        for h in range(2):
            one, two = (xn, yn) if h == 0 else (yn, xn)
            cps += [cp(8 + 3 * h, s1.at[n, h, 0], r1.at[n, h, 0], one), cp(9 + 3 * h, s1.at[n, h, 1], r1.at[n, h, 1], one),
                    cp(10 + 3 * h, s2.at[n, h], r2.at[n, h], two)]
        return cps

    rsc = [rs_copies(n) for n in range(3)]

    def rs_pair(n, k):
        rsc[n][2 * k].start()
        rsc[n][2 * k + 1].start()

    def chip_sum(n, h, k):
        return part[n, c, h, chips[k]] + pair[n, h, chips[k]]

    def rs_far(n):
        rs_wait(n, 2 * DI, 2)
        for h in range(2):
            s1[n, h, 0] = chip_sum(n, h, DI)
            rsc[n][8 + 3 * h].start()

    def rs_near(n, h):
        k = first[h]
        rs_wait(n, 2 * k + h, 1)
        s1[n, h, 1] = chip_sum(n, h, k)
        rsc[n][9 + 3 * h].start()

    def rs_second(n):
        rs_wait(n, 2 * Y, 2)
        rs_wait(n, 8, 2)
        for h in range(2):
            k = second[h]
            s2[n, h] = chip_sum(n, h, k) + r1[n, h, 0]
            rsc[n][10 + 3 * h].start()

    def rs_final(n, out_ref):
        rs_wait(n, 2 * OWN, 6)
        for h in range(2):
            total = chip_sum(n, h, OWN) + r1[n, h, 1] + r2[n, h]
            out_ref[:, h * HALF:(h + 1) * HALF] = total.astype(BF)

    def gate_table(k):
        tiles = grecv.at[0:1 if k == OWN else 2]
        remote(tiles, tiles, gs_sem.at[0], gr_sem.at[k], sib).wait_recv()
        q = chips[k]
        tile = grecv[2 * q] + grecv[2 * q + 1]
        gt[pl.ds(pl.multiple_of(q * 128, 128), 128), :] = jnp.concatenate([tile, jnp.zeros((120, 128), F32)], axis=0).T

    def pick(tile, e):
        lane = lax.broadcasted_iota(jnp.int32, tile.shape, 1)
        return jnp.sum(jnp.where(lane == e, tile, 0.0), axis=1, keepdims=True)

    def accumulate(n, q, val):
        for cc in range(2):
            for h in range(2):
                part[n, cc, h, q] += val[cc * 64:(cc + 1) * 64, h * HALF:(h + 1) * HALF]

    def experts(step, hooks):
        def body(e, carry):
            step(e)
            for at, fn in hooks.items():
                @pl.when(e == at)
                def _():
                    fn()
            return carry
        lax.fori_loop(0, EXP, body, 0)

    def chip_rows(k):
        return pl.ds(pl.multiple_of(chips[k] * 128, 128), 128)

    def forward(ks, load=False):
        def stack(ref, *at):
            return jnp.concatenate([ref[(*at, chip_rows(k), slice(None))] for k in ks], axis=0)

        def step(e):
            if load:
                pltpu.make_async_copy(wg_hbm.at[0:3], wg.at[0:3], w_sem.at[1 + e]).wait()

            def put(ref, val):
                for i, k in enumerate(ks):
                    ref[e, chip_rows(k), :] = val[i * 128:(i + 1) * 128]

            xs = stack(rows, XT)
            a = jnp.dot(xs, wg[e], preferred_element_type=F32)
            b = jnp.dot(xs, wu[e], preferred_element_type=F32)
            tile = stack(gt)
            mark = pick(tile, e + 4) > 0.5
            sg = jax.nn.sigmoid(a)
            ac = a * sg
            put(act, jnp.where(mark, ac, 0.0))
            put(gfac, jnp.where(mark, b * sg * (1.0 + a * (1.0 - sg)), 0.0))
            hh = jnp.where(mark, ac * b, 0.0).astype(BF)
            put(hid, hh)
            ob = jnp.dot(hh, wd[e], preferred_element_type=F32).astype(BF)
            put(osv, ob)
            yb = pick(tile, e) * ob.astype(F32)
            for i, k in enumerate(ks):
                accumulate(1, chips[k], yb[i * 128:(i + 1) * 128])
        return step

    def backward(qa, qb, base, gates):
        sl = pl.ds(pl.multiple_of(base, 256), 256)

        def step(e):
            g = pick(gt[sl, :], e)
            dyf = rows[DY, sl, :].astype(F32)
            do = (g * dyf).astype(BF)
            dh = lax.dot_general(do, wd[e], NT, preferred_element_type=F32).astype(BF).astype(F32)
            da = (dh * gfac[e, sl, :]).astype(BF)
            db = (dh * act[e, sl, :]).astype(BF)
            dag[e, sl, :] = da
            dbg[e, sl, :] = db
            if gates:
                lane = lax.broadcasted_iota(jnp.int32, (256, 128), 1)
                for r in (slice(0, 256), slice(256, 512)):
                    dg = jnp.sum(rows[DY, r, :].astype(F32) * osv[e, r, :].astype(F32), axis=1, keepdims=True)
                    dgs[r, :] += jnp.where(lane == e, dg, 0.0)
            dx = (lax.dot_general(da, wg[e], NT, preferred_element_type=F32)
                  + lax.dot_general(db, wu[e], NT, preferred_element_type=F32)).astype(BF).astype(F32)
            accumulate(2, qa, dx[0:128])
            accumulate(2, qb, dx[128:256])
        return step

    def attention_context():
        ag_rows(XA, 0, 4 * ROWS).wait_recv()
        pltpu.make_async_copy(wg_hbm.at[0, 0:768], wg.at[0, 0:768], w_sem.at[0]).wait()
        causal_r = lax.broadcasted_iota(jnp.int32, (256, 128), 0) % 128
        causal_c = lax.broadcasted_iota(jnp.int32, (256, 128), 1)
        keep = (causal_r >= causal_c) & (causal_r // 64 == causal_c // 64)
        qkv = lax.dot_general(rows[XA], wqkv[...], NT, preferred_element_type=F32).astype(BF)
        qkvs = [qkv[q * 128:(q + 1) * 128] for q in range(4)]
        scs = [lax.dot_general(jnp.concatenate([v[:, 0:64], v[:, 64:128]], axis=0), v[:, 128:192], NT,
                               preferred_element_type=F32) * (64 ** -0.5) for v in qkvs]
        scs = [jnp.where(keep, sc, -1e30) for sc in scs]
        mxs = [jnp.max(sc, axis=1, keepdims=True) for sc in scs]
        exs = [jnp.exp(sc - mx) for sc, mx in zip(scs, mxs)]
        sms = [jnp.sum(ex, axis=1, keepdims=True) for ex in exs]
        prs = [(ex / sm).astype(BF) for ex, sm in zip(exs, sms)]
        ctxs = [jnp.dot(pr, v[:, 192:256], preferred_element_type=F32).astype(BF) for pr, v in zip(prs, qkvs)]
        return jnp.concatenate([jnp.concatenate([v[0:128], v[128:256]], axis=1) for v in ctxs], axis=0)

    def attention_out(ctx):
        for q in range(4):
            out = jnp.dot(ctx[q * 128:(q + 1) * 128], wo[...], preferred_element_type=F32)
            for cc in range(2):
                for h in range(2):
                    part[0, cc, h, q] = out[cc * 64:(cc + 1) * 64, h * HALF:(h + 1) * HALF]

    def leave(i, n):
        rs_wait(n, 2 * OWN, 6)
        rs_wait(n, 8, 2)
        for h in range(2):
            cols = slice(h * HALF, (h + 1) * HALF)
            near = chip_sum(n, h, first[h])
            far = chip_sum(n, h, second[h]) + r1[n, h, 0]
            mine = chip_sum(n, h, OWN)
            tox[i, :, cols] = near if h == 0 else far
            toy[i, :, cols] = far if h == 0 else near
            owns[i, :, cols] = mine
    pltpu.make_async_copy(wg_hbm.at[0, 0:6 * ROWS], wg.at[0, 0:6 * ROWS], in_sem.at[0]).wait()
    pl.semaphore_wait(barrier, len(rels))
    for cp in gate_cps.values():
        cp.start()
    ag_own(XT)
    ag_own(XA)
    gate_table(OWN)
    ag[XT][0].wait_recv()
    experts(forward([OWN], True), {2: lambda: ag_forward(XT)})
    rs_pair(1, OWN)
    ag_pair(XT)
    gate_table(X)
    gate_table(Y)
    ag_own_a(DY)
    ag[XT][7].wait_recv()
    ag[XT][8].wait_recv()
    experts(forward([X, Y]), {0: lambda: (ag_forward(XA), ag_own_b(DY)), 1: lambda: ag_pair(XA), 2: lambda: ag_last(XT)})
    rs_pair(1, X)
    rs_pair(1, Y)
    gate_table(DI)
    ag_forward(DY)
    ag_rows(XT, 9, ROWS).wait_recv()
    xall[...] = rows[XT]
    experts(forward([DI]), {1: lambda: (rs_near(1, 0), rs_near(1, 1), ag_last(XA)), 2: lambda: ag_pair(DY)})
    rs_pair(1, DI)
    ctx = attention_context()
    ag_last(DY)
    rs_far(1)
    attention_out(ctx)
    for k in (DI, X, Y, OWN):
        rs_pair(0, k)
    ag_rows(DY, 0, 4 * ROWS).wait_recv()
    dyall[...] = rows[DY]
    experts(backward(2 * (1 - y), 2 * (1 - y) + 1, (1 - y) * 256, True), {0: lambda: rs_far(0), 2: lambda: rs_second(1)})
    rs_pair(2, DI)
    rs_pair(2, Y)
    for q in range(4):
        dsend[q] = dgs[q * 128:(q + 1) * 128, :].T[0:8, :]
    drecv[me] = dsend[q0]
    for cp in dg_cps.values():
        cp.start()
    experts(backward(2 * y, 2 * y + 1, y * 256, False), {0: lambda: rs_far(2)})
    rs_pair(2, X)
    rs_pair(2, OWN)
    leave(0, 0)
    rs_wait_dg = drecv.at[0:7]
    remote(rs_wait_dg, rs_wait_dg, dd_s.at[0], dd_r.at[0], sib).wait_recv()
    both = drecv[...].reshape(64, 128)
    mine = jnp.where(c == 0, both[:, 0:ROWS], both[:, ROWS:128])
    for j in range(TOPK):
        hit = row_exp == idx_ref[j:j + 1, :]
        dg_out[j:j + 1, :] = jnp.sum(jnp.where(hit & is_gate, mine, 0.0), axis=0, keepdims=True)
    rs_final(1, y_out)
    leave(1, 2)

    for t in range(3):
        ref = rows.at[t, 0:7 * ROWS]
        remote(ref, ref, ag_s.at[t], ag_r.at[0], sib).wait_send()
    tiles = gsend.at[0:7]
    remote(tiles, tiles, gs_sem.at[0], gr_sem.at[0], sib).wait_send()
    remote(tiles, tiles, dd_s.at[0], dd_r.at[0], sib).wait_send()
    for n in range(3):
        for ref, k in ((part.at[n, 0], 0), (pair.at[n, :, 0:3] if n == 1 else pair.at[n, 0, 0:2], 1)):
            remote(ref, ref, rs_s.at[n, k], rs_r.at[0], sib).wait_send()


def exchange(x, dy, xa, idx, gates, wg, wu, wd, wq, wk, wv, wo):
    any_spec = pl.BlockSpec(memory_space=pl.ANY)
    vmem = pl.BlockSpec(memory_space=pltpu.VMEM)
    dma = pltpu.SemaphoreType.DMA
    return pl.pallas_call(
        exchange_kernel,
        name='exchange',
        out_shape=[pltpu.VMEM((ROWS, D), BF), pltpu.VMEM((TOPK, ROWS), F32)] + [pltpu.VMEM((2, ROWS, D), F32)] * 3 + [pltpu.VMEM((TOK, D), BF)] * 2
        + [pltpu.VMEM((EXP, TOK, FF), BF)] * 3 + [pltpu.VMEM((TOK, 128), F32)],
        in_specs=[any_spec] * 12,
        out_specs=[vmem] * 11,
        scratch_shapes=[
            pltpu.VMEM((TOPK, ROWS), jnp.int32), pltpu.VMEM((TOPK, ROWS), F32),
            pltpu.VMEM((3, TOK, D), BF),
            pltpu.VMEM((EXP, D, FF), BF), pltpu.VMEM((EXP, D, FF), BF), pltpu.VMEM((EXP, FF, D), BF),
            pltpu.VMEM((256, D), BF), pltpu.VMEM((128, D), BF),
            pltpu.VMEM((EXP, TOK, D), BF),
            pltpu.VMEM((EXP, TOK, FF), F32), pltpu.VMEM((EXP, TOK, FF), F32),
            pltpu.VMEM((8, 8, 128), F32), pltpu.VMEM((8, 8, 128), F32),
            pltpu.VMEM((TOK, 128), F32), pltpu.VMEM((4, 8, 128), F32), pltpu.VMEM((8, 8, 128), F32),
            pltpu.VMEM((3, 2, 2, 4, ROWS, HALF), F32), pltpu.VMEM((3, 2, 4, ROWS, HALF), F32),
            pltpu.VMEM((3, 2, 2, ROWS, HALF), F32), pltpu.VMEM((3, 2, 2, ROWS, HALF), F32),
            pltpu.VMEM((3, 2, ROWS, HALF), F32), pltpu.VMEM((3, 2, ROWS, HALF), F32),
            dma((3,)), dma((1 + EXP,)), dma((1,)), dma((4,)),
            dma((3, 2)), dma((12,)), dma((3,)), dma((24,)), dma((1,)), dma((1,)),
        ],
        compiler_params=pltpu.CompilerParams(collective_id=0, has_side_effects=True, vmem_limit_bytes=50 * 1024 * 1024),
    )(x, dy, xa, idx, gates, wg, wu, wd, wq, wk, wv, wo)


def grads_kernel(x_ref, dy_ref, gt_ref, h_ref, da_ref, db_ref, y_in, dg_in,
                 dwg_ref, dwu_ref, dwd_ref, y_out, dg_out, xt):
    e = pl.program_id(0)

    @pl.when(e == 0)
    def _():
        xt[...] = x_ref[...].T
        y_out[...] = y_in[...]
        dg_out[...] = dg_in[...]

    dwg_ref[0] = jnp.dot(xt[...], da_ref[e], preferred_element_type=F32)
    dwu_ref[0] = jnp.dot(xt[...], db_ref[e], preferred_element_type=F32)
    lane = lax.broadcasted_iota(jnp.int32, (TOK, 128), 1)
    g = jnp.sum(jnp.where(lane == e, gt_ref[...], 0.0), axis=1, keepdims=True)
    do = (g * dy_ref[...].astype(F32)).astype(BF)
    dwd_ref[0] = lax.dot_general(h_ref[e], do, TN, preferred_element_type=F32)


def weight_grads(xall, dyall, gt, h, da, db, y_t, dg):
    sds = jax.ShapeDtypeStruct
    args = [pltpu.with_memory_space_constraint(v, pltpu.VMEM) for v in (xall, dyall, gt, h, da, db, y_t, dg)]
    whole = lambda shape: pl.BlockSpec(shape, lambda e: (0, 0))
    per = lambda a, b: pl.BlockSpec((1, a, b), lambda e: (e, 0, 0))
    return pl.pallas_call(
        grads_kernel,
        name='weight_grads',
        grid=(EXP,),
        out_shape=[sds((EXP, D, FF), F32), sds((EXP, D, FF), F32), sds((EXP, FF, D), F32),
                   sds((ROWS, D), BF), sds((TOPK, ROWS), F32)],
        in_specs=[pl.BlockSpec(memory_space=pltpu.VMEM)] * 8,
        out_specs=[per(D, FF), per(D, FF), per(FF, D)] + [whole((ROWS, D))] + [whole((TOPK, ROWS))],
        scratch_shapes=[pltpu.VMEM((D, TOK), BF)],
        cost_estimate=pl.CostEstimate(flops=3 * 2 * EXP * TOK * D * FF, bytes_accessed=34 * 1024 * 1024, transcendentals=0),
        compiler_params=pltpu.CompilerParams(vmem_limit_bytes=40 * 1024 * 1024),
    )(*args)


def solution(mesh):
    def local_step(x_tokens, expert_idx, gate_vals, dy_tokens, w_gate, w_up, w_down, x_attn, w_query, w_key, w_value, w_out):
        y_p, dg_p, to_x, to_y, own, xall, dyall, h, da, db, gt = exchange(
            x_tokens, dy_tokens, x_attn.reshape(ROWS, D), expert_idx.T, gate_vals.T, w_gate, w_up, w_down,
            w_query.transpose(1, 2, 0).reshape(128, D), w_key.transpose(1, 2, 0).reshape(64, D),
            w_value.transpose(1, 2, 0).reshape(64, D), w_out.reshape(128, D))
        from_x = lax.ppermute(to_x, GROUP_AXES, [(g, g ^ 2) for g in range(8)])
        from_y = lax.ppermute(to_y, GROUP_AXES, [(g, g ^ 4) for g in range(8)])
        dwg, dwu, dwd, y_t, dg = weight_grads(xall, dyall, gt, h, da, db, y_p, dg_p)
        both = (own + from_x + from_y).astype(BF)
        at, dx_t = both[0], both[1]
        return y_t, dx_t, dg.T, dwg, dwu, dwd, at.reshape(1, ROWS, D)

    spec_rows = P(TOKEN_AXES, None)
    spec_seqs = P(TOKEN_AXES, None, None)
    spec_experts = P(GROUP_AXES, None, None)
    spec_heads = P(None, GROUP_AXES, None)
    return jax.shard_map(local_step, mesh=mesh,
                         in_specs=(spec_rows, spec_rows, spec_rows, spec_rows, spec_experts, spec_experts, spec_experts, spec_seqs, spec_heads, spec_heads, spec_heads, spec_experts),
                         out_specs=(spec_rows, spec_rows, spec_rows, spec_seqs, spec_seqs, spec_seqs, spec_seqs),
                         check_vma=False)
```

```python
import functools

import jax
import jax.numpy as jnp
from jax import lax
from jax.experimental import pallas as pl
from jax.experimental.pallas import tpu as pltpu
from jax.sharding import PartitionSpec as P

MESH = pl.DeviceIdType.MESH
GROUP_AXES = ('ei', 'eo')
TOKEN_AXES = ('dp', 'ei', 'eo')
BF = jnp.bfloat16
F32 = jnp.float32

ROWS = 64
TOK = 512
D = 1024
FF = 512
HALF = 512
EXP = 4
TOPK = 8
XA, XT, DY = 0, 1, 2

NT = (((1,), (1,)), ((), ()))
TN = (((0,), (0,)), ((), ()))


def exchange_kernel(x_hbm, dy_hbm, xa_hbm, idx_hbm, gate_hbm, wg_hbm, wu_hbm, wd_hbm, wq_hbm, wk_hbm, wv_hbm, wo_hbm,
                    y_out, dg_out, tox, toy, own_dx, own_at, xt, dyall, hid, dag, dbg, gt,
                    idx_ref, gate_ref, rows, wg, wu, wd, wqkv, wo, wo_in, ctx, ctx_in, osv, act, gfac, gsend, grecv,
                    dgs, dsend, drecv,
                    part, pair, s1, r1, s2, r2,
                    in_sem, w_sem, gs_sem, gr_sem, rs_s, rs_r, ag_s, ag_r, dd_s, dd_r, hd_s, hd_r):
    y = lax.axis_index('ei')
    o = lax.axis_index('eo')
    z = lax.axis_index('dp')
    x = o // 2
    c = o % 2
    me = y * 4 + o
    q0 = 2 * y + x
    qx = 2 * y + (1 - x)
    qy = 2 * (1 - y) + x
    qd = 2 * (1 - y) + (1 - x)

    def dev(fx, fy, fc):
        xx = (1 - x) if fx else x
        yy = (1 - y) if fy else y
        cc = (1 - c) if fc else c
        return (z, yy, xx * 2 + cc)

    sib, xn, yn = dev(0, 0, 1), dev(1, 0, 0), dev(0, 1, 0)
    rels = [(fx, fy, fc) for fx in (0, 1) for fy in (0, 1) for fc in (0, 1) if fx or fy or fc]

    barrier = pltpu.get_barrier_semaphore()
    for rel in rels:
        pl.semaphore_signal(barrier, inc=1, device_id=dev(*rel), device_id_type=MESH)

    own = pl.ds(pl.multiple_of(me * ROWS, ROWS), ROWS)
    tables = [pltpu.make_async_copy(idx_hbm, idx_ref, in_sem.at[1]), pltpu.make_async_copy(gate_hbm, gate_ref, in_sem.at[2])]
    for cp in tables:
        cp.start()
    for t, src in ((XT, x_hbm), (DY, dy_hbm), (XA, xa_hbm)):
        pltpu.make_async_copy(src, rows.at[t, own], in_sem.at[0]).start()

    def expert_load(e):
        return [pltpu.make_async_copy(src.at[e], dst.at[e], w_sem.at[1 + e])
                for src, dst in ((wg_hbm, wg), (wu_hbm, wu), (wd_hbm, wd))]

    for e in range(EXP):
        for cp in expert_load(e):
            cp.start()
    wload = [pltpu.make_async_copy(wq_hbm, wqkv.at[0:128], w_sem.at[0]),
             pltpu.make_async_copy(wk_hbm, wqkv.at[128:192], w_sem.at[0]),
             pltpu.make_async_copy(wv_hbm, wqkv.at[192:256], w_sem.at[0]),
             pltpu.make_async_copy(wo_hbm.at[:, 0:HALF], wo.at[0], w_sem.at[0]),
             pltpu.make_async_copy(wo_hbm.at[:, HALF:D], wo.at[1], w_sem.at[0])]
    for cp in wload:
        cp.start()

    for cp in tables:
        cp.wait()
    row = lax.broadcasted_iota(jnp.int32, (64, ROWS), 0)
    row_exp = (row // 8) * 4 + row % 4
    is_gate = (row % 8) < 4
    table = jnp.zeros((64, ROWS), F32)
    for j in range(TOPK):
        hit = row_exp == idx_ref[j:j + 1, :]
        table = table + jnp.where(hit, jnp.where(is_gate, gate_ref[j:j + 1, :], 1.0), 0.0)
    blank = jnp.zeros((64, ROWS), F32)
    wide = jnp.where(c == 0, jnp.concatenate([table, blank], axis=1), jnp.concatenate([blank, table], axis=1))
    for d in range(8):
        gsend[d] = wide[d * 8:(d + 1) * 8, :]
    grecv[me] = gsend[me]
    dgs[...] = jnp.zeros((TOK, 128), F32)
    part[1] = jnp.zeros(part.shape[1:], F32)
    part[2] = jnp.zeros(part.shape[1:], F32)

    def blk(t, q, off=0, n=ROWS):
        return rows.at[t, pl.ds(pl.multiple_of(q * 128 + c * ROWS + off, 32), n)]

    def remote(src, dst, ss, rs, where):
        return pltpu.make_async_remote_copy(src, dst, ss, rs, device_id=where, device_id_type=MESH)

    hr = ROWS // 2

    def gather_slot(t, k):
        if t == XT:
            return min(k, 9)
        return (10 if t == XA else 17) + (k - 1 if 1 <= k <= 6 else 6)

    def gather_copies(t):
        def cp(k, ref, where):
            return remote(ref, ref, ag_s.at[t], ag_r.at[gather_slot(t, k)], where)
        return [cp(0, blk(t, q0), sib),
                cp(1, blk(t, q0, 0, hr), xn), cp(2, blk(t, q0, hr, hr), xn),
                cp(3, blk(t, q0, hr, hr), yn), cp(4, blk(t, q0, 0, hr), yn),
                cp(5, blk(t, qx, 0, hr), yn), cp(6, blk(t, qy, hr, hr), xn),
                cp(7, blk(t, qx), sib), cp(8, blk(t, qy), sib),
                cp(9, blk(t, qd, 0, hr), sib), cp(10, blk(t, qd, hr, hr), sib)]

    ag = [gather_copies(t) for t in range(3)]

    def ag_own(t):
        for k in (1, 3, 2, 4, 0):
            ag[t][k].start()

    def ag_own_a(t):
        ag[t][1].start()
        ag[t][3].start()

    def ag_own_b(t):
        for k in (2, 4, 0):
            ag[t][k].start()

    def ag_forward(t):
        ag[t][1].wait_recv()
        ag[t][5].start()
        ag[t][3].wait_recv()
        ag[t][6].start()

    def ag_pair(t):
        ag[t][2].wait_recv()
        ag[t][7].start()
        ag[t][4].wait_recv()
        ag[t][8].start()

    def ag_last(t):
        ag[t][5].wait_recv()
        ag[t][9].start()
        ag[t][6].wait_recv()
        ag[t][10].start()

    def ag_rows(t, k, n):
        ref = rows.at[t, 0:n]
        return remote(ref, ref, ag_s.at[t], ag_r.at[gather_slot(t, k)], sib)

    def tile_copies(send, recv, ss, rs, chip_tiles):
        cps = {}
        for fx, fy, fc in rels:
            where = dev(fx, fy, fc)
            qq = 2 * where[1] + where[2] // 2
            src = send.at[qq] if chip_tiles else send.at[where[1] * 4 + where[2]]
            cps[fx, fy, fc] = remote(src, recv.at[me], ss.at[0], rs.at[0 if chip_tiles else fx + 2 * fy], where)
        return cps

    gate_cps = tile_copies(gsend, grecv, gs_sem, gr_sem, False)
    dg_cps = tile_copies(dsend, drecv, dd_s, dd_r, True)
    chips = (q0, qx, qy, qd)
    OWN, X, Y, DI = 0, 1, 2, 3
    first = (X, Y)
    second = (Y, X)

    def rs_slot(n, k):
        if k >= 8:
            kind = (k - 8) % 3
            group = 2 if kind == 0 else 1
        else:
            group = 0 if k // 2 == DI else 1
            if n == 1 and k // 2 in (X, Y):
                group = 3 if k == 2 * X else 4 if k == 2 * Y + 1 else 5
        return (0, 3, 9)[n] + group

    def rs_wait(n, k, count):
        ref = pair.at[n, 0, 0:2] if count == 2 else pair.at[n, :, 0:3] if count == 6 else pair.at[n, 0, 0]
        remote(ref, ref, rs_s.at[n, 0], rs_r.at[rs_slot(n, k)], sib).wait_recv()

    def rs_copies(n):
        def cp(k, src, dst, where):
            return remote(src, dst, rs_s.at[n, 0 if k < 8 else 1], rs_r.at[rs_slot(n, k)], where)
        cps = [cp(2 * k + h, part.at[n, 1 - c, h, chips[k]], pair.at[n, h, chips[k]], sib) for k in range(4) for h in range(2)]
        for h in range(2):
            one, two = (xn, yn) if h == 0 else (yn, xn)
            cps += [cp(8 + 3 * h, s1.at[n, h, 0], r1.at[n, h, 0], one), cp(9 + 3 * h, s1.at[n, h, 1], r1.at[n, h, 1], one),
                    cp(10 + 3 * h, s2.at[n, h], r2.at[n, h], two)]
        return cps

    rsc = [rs_copies(n) for n in range(3)]

    def rs_pair(n, k):
        rsc[n][2 * k].start()
        rsc[n][2 * k + 1].start()

    def chip_sum(n, h, k):
        return part[n, c, h, chips[k]] + pair[n, h, chips[k]]

    def rs_far(n):
        rs_wait(n, 2 * DI, 2)
        for h in range(2):
            s1[n, h, 0] = chip_sum(n, h, DI)
            rsc[n][8 + 3 * h].start()

    def rs_near(n, h):
        k = first[h]
        rs_wait(n, 2 * k + h, 1)
        s1[n, h, 1] = chip_sum(n, h, k)
        rsc[n][9 + 3 * h].start()

    def rs_second(n):
        rs_wait(n, 2 * Y, 2)
        rs_wait(n, 8, 2)
        for h in range(2):
            k = second[h]
            s2[n, h] = chip_sum(n, h, k) + r1[n, h, 0]
            rsc[n][10 + 3 * h].start()

    def rs_final(n, out_ref):
        rs_wait(n, 2 * OWN, 6)
        for h in range(2):
            total = chip_sum(n, h, OWN) + r1[n, h, 1] + r2[n, h]
            out_ref[:, h * HALF:(h + 1) * HALF] = total.astype(BF)

    def head_copy(src, dst, slot, where):
        return remote(src, dst, hd_s.at[slot // 2], hd_r.at[slot], where)

    wo_cps = [head_copy(wo.at[h], wo_in.at[h], h, (xn, yn)[h]) for h in range(2)]
    ctx_cps = [head_copy(ctx.at[q], ctx_in.at[h, i], 2 + h, (xn, yn)[h])
               for h, qn in ((0, qx), (1, qy)) for i, q in ((0, qn), (1, qd))]

    def gate_table(k):
        tiles = grecv.at[0:1 if k == OWN else 2]
        remote(tiles, tiles, gs_sem.at[0], gr_sem.at[k], sib).wait_recv()
        q = chips[k]
        tile = grecv[2 * q] + grecv[2 * q + 1]
        gt[pl.ds(pl.multiple_of(q * 128, 128), 128), :] = jnp.concatenate([tile, jnp.zeros((120, 128), F32)], axis=0).T

    def pick(tile, e):
        lane = lax.broadcasted_iota(jnp.int32, tile.shape, 1)
        return jnp.sum(jnp.where(lane == e, tile, 0.0), axis=1, keepdims=True)

    def accumulate(n, q, val):
        for cc in range(2):
            for h in range(2):
                part[n, cc, h, q] += val[cc * 64:(cc + 1) * 64, h * HALF:(h + 1) * HALF]

    def experts(step, hooks):
        def body(e, carry):
            step(e)
            for at, fn in hooks.items():
                @pl.when(e == at)
                def _():
                    fn()
            return carry
        lax.fori_loop(0, EXP, body, 0)

    def chip_rows(k):
        return pl.ds(pl.multiple_of(chips[k] * 128, 128), 128)

    def forward(ks, load=False):
        def stack(ref, *at):
            return jnp.concatenate([ref[(*at, chip_rows(k), slice(None))] for k in ks], axis=0)

        def step(e):
            if load:
                pltpu.make_async_copy(wg_hbm.at[0:3], wg.at[0:3], w_sem.at[1 + e]).wait()

            def put(ref, val):
                for i, k in enumerate(ks):
                    ref[e, chip_rows(k), :] = val[i * 128:(i + 1) * 128]

            xs = stack(rows, XT)
            a = jnp.dot(xs, wg[e], preferred_element_type=F32)
            b = jnp.dot(xs, wu[e], preferred_element_type=F32)
            tile = stack(gt)
            mark = pick(tile, e + 4) > 0.5
            sg = jax.nn.sigmoid(a)
            ac = a * sg
            put(act, jnp.where(mark, ac, 0.0))
            put(gfac, jnp.where(mark, b * sg * (1.0 + a * (1.0 - sg)), 0.0))
            hh = jnp.where(mark, ac * b, 0.0).astype(BF)
            put(hid, hh)
            ob = jnp.dot(hh, wd[e], preferred_element_type=F32).astype(BF)
            put(osv, ob)
            yb = pick(tile, e) * ob.astype(F32)
            for i, k in enumerate(ks):
                accumulate(1, chips[k], yb[i * 128:(i + 1) * 128])
        return step

    def backward(qa, qb, base, gates):
        sl = pl.ds(pl.multiple_of(base, 256), 256)

        def step(e):
            g = pick(gt[sl, :], e)
            dyf = rows[DY, sl, :].astype(F32)
            do = (g * dyf).astype(BF)
            dh = lax.dot_general(do, wd[e], NT, preferred_element_type=F32).astype(BF).astype(F32)
            da = (dh * gfac[e, sl, :]).astype(BF)
            db = (dh * act[e, sl, :]).astype(BF)
            dag[e, sl, :] = da
            dbg[e, sl, :] = db
            if gates:
                lane = lax.broadcasted_iota(jnp.int32, (256, 128), 1)
                for r in (slice(0, 256), slice(256, 512)):
                    dg = jnp.sum(rows[DY, r, :].astype(F32) * osv[e, r, :].astype(F32), axis=1, keepdims=True)
                    dgs[r, :] += jnp.where(lane == e, dg, 0.0)
            dx = (lax.dot_general(da, wg[e], NT, preferred_element_type=F32)
                  + lax.dot_general(db, wu[e], NT, preferred_element_type=F32)).astype(BF).astype(F32)
            accumulate(2, qa, dx[0:128])
            accumulate(2, qb, dx[128:256])
        return step

    def attention_context():
        ag_rows(XA, 0, 4 * ROWS).wait_recv()
        pltpu.make_async_copy(wg_hbm.at[0, 0:768], wg.at[0, 0:768], w_sem.at[0]).wait()
        causal_r = lax.broadcasted_iota(jnp.int32, (256, 128), 0) % 128
        causal_c = lax.broadcasted_iota(jnp.int32, (256, 128), 1)
        keep = (causal_r >= causal_c) & (causal_r // 64 == causal_c // 64)
        qkv = lax.dot_general(rows[XA], wqkv[...], NT, preferred_element_type=F32).astype(BF)
        qkvs = [qkv[q * 128:(q + 1) * 128] for q in range(4)]
        scs = [lax.dot_general(jnp.concatenate([v[:, 0:64], v[:, 64:128]], axis=0), v[:, 128:192], NT,
                               preferred_element_type=F32) * (64 ** -0.5) for v in qkvs]
        scs = [jnp.where(keep, sc, -1e30) for sc in scs]
        mxs = [jnp.max(sc, axis=1, keepdims=True) for sc in scs]
        exs = [jnp.exp(sc - mx) for sc, mx in zip(scs, mxs)]
        sms = [jnp.sum(ex, axis=1, keepdims=True) for ex in exs]
        prs = [(ex / sm).astype(BF) for ex, sm in zip(exs, sms)]
        ctxs = [jnp.dot(pr, v[:, 192:256], preferred_element_type=F32).astype(BF) for pr, v in zip(prs, qkvs)]
        for q, v in enumerate(ctxs):
            ctx[q] = jnp.concatenate([v[0:128], v[128:256]], axis=1)

    def attention_out():
        for h in range(2):
            wo_cps[h].wait_recv()
            both = ctx_in.at[h]
            head_copy(both, both, 2 + h, sib).wait_recv()
            for i, k in ((0, OWN), (1, second[h])):
                out = (jnp.dot(ctx[chips[k]], wo[h], preferred_element_type=F32)
                       + jnp.dot(ctx_in[h, i], wo_in[h], preferred_element_type=F32))
                for cc in range(2):
                    part[0, cc, h, chips[k]] = out[cc * 64:(cc + 1) * 64]
        for h in range(2):
            rsc[0][2 * OWN + h].start()
            rsc[0][2 * second[h] + h].start()

    def leave_attention():
        ref = pair.at[0, 0]
        remote(ref, ref, rs_s.at[0, 0], rs_r.at[rs_slot(0, 2 * OWN)], sib).wait_recv()
        for h, dst in ((0, toy), (1, tox)):
            dst[:, D:D + HALF] = chip_sum(0, h, second[h])
            own_at[:, h * HALF:(h + 1) * HALF] = chip_sum(0, h, OWN)

    def leave_dx():
        n = 2
        rs_wait(n, 2 * OWN, 6)
        rs_wait(n, 8, 2)
        for h in range(2):
            cols = slice(h * HALF, (h + 1) * HALF)
            near = chip_sum(n, h, first[h])
            far = chip_sum(n, h, second[h]) + r1[n, h, 0]
            tox[:, cols] = near if h == 0 else far
            toy[:, cols] = far if h == 0 else near
            own_dx[:, cols] = chip_sum(n, h, OWN)

    pltpu.make_async_copy(wg_hbm.at[0, 0:6 * ROWS], wg.at[0, 0:6 * ROWS], in_sem.at[0]).wait()
    pl.semaphore_wait(barrier, len(rels))
    for cp in gate_cps.values():
        cp.start()
    ag_own(XT)
    ag_own(XA)
    gate_table(OWN)
    ag[XT][0].wait_recv()
    experts(forward([OWN], True), {2: lambda: ag_forward(XT)})
    rs_pair(1, OWN)
    ag_pair(XT)
    gate_table(X)
    gate_table(Y)
    ag_own_a(DY)
    ag[XT][7].wait_recv()
    ag[XT][8].wait_recv()
    experts(forward([X, Y]), {0: lambda: (ag_forward(XA), ag_own_b(DY)), 1: lambda: ag_pair(XA), 2: lambda: ag_last(XT)})
    rs_pair(1, X)
    rs_pair(1, Y)
    gate_table(DI)
    ag_forward(DY)
    ag_rows(XT, 9, ROWS).wait_recv()
    experts(forward([DI]), {1: lambda: (rs_near(1, 0), rs_near(1, 1), ag_last(XA)), 2: lambda: ag_pair(DY), 3: lambda: ag_last(DY)})
    rs_pair(1, DI)
    attention_context()
    rs_far(1)
    for cp in ctx_cps + wo_cps:
        cp.start()
    ag_rows(DY, 0, 4 * ROWS).wait_recv()
    dyall[...] = rows[DY]
    experts(backward(2 * (1 - y), 2 * (1 - y) + 1, (1 - y) * 256, True), {3: lambda: rs_second(1)})
    rs_pair(2, DI)
    rs_pair(2, Y)
    for q in range(4):
        dsend[q] = dgs[q * 128:(q + 1) * 128, :].T[0:8, :]
    drecv[me] = dsend[q0]
    for cp in dg_cps.values():
        cp.start()
    experts(backward(2 * y, 2 * y + 1, y * 256, False), {0: lambda: rs_far(2)})
    rs_pair(2, X)
    rs_pair(2, OWN)
    attention_out()
    rs_wait_dg = drecv.at[0:7]
    remote(rs_wait_dg, rs_wait_dg, dd_s.at[0], dd_r.at[0], sib).wait_recv()
    both = drecv[...].reshape(64, 128)
    mine = jnp.where(c == 0, both[:, 0:ROWS], both[:, ROWS:128])
    for j in range(TOPK):
        hit = row_exp == idx_ref[j:j + 1, :]
        dg_out[j:j + 1, :] = jnp.sum(jnp.where(hit & is_gate, mine, 0.0), axis=0, keepdims=True)
    rs_final(1, y_out)
    leave_attention()
    xt[...] = rows[XT].T
    leave_dx()

    for t in range(3):
        ref = rows.at[t, 0:7 * ROWS]
        remote(ref, ref, ag_s.at[t], ag_r.at[0], sib).wait_send()
    tiles = gsend.at[0:7]
    remote(tiles, tiles, gs_sem.at[0], gr_sem.at[0], sib).wait_send()
    remote(tiles, tiles, dd_s.at[0], dd_r.at[0], sib).wait_send()
    for ref, n, k in ((pair.at[0, 0], 0, 0), (part.at[1, 0], 1, 0), (part.at[2, 0], 2, 0),
                      (pair.at[1, :, 0:3], 1, 1), (pair.at[2, 0, 0:2], 2, 1)):
        remote(ref, ref, rs_s.at[n, k], rs_r.at[0], sib).wait_send()
    remote(wo, wo, hd_s.at[0], hd_r.at[0], sib).wait_send()
    remote(ctx, ctx, hd_s.at[1], hd_r.at[0], sib).wait_send()


def exchange(x, dy, xa, idx, gates, wg, wu, wd, wq, wk, wv, wo):
    any_spec = pl.BlockSpec(memory_space=pl.ANY)
    vmem = pl.BlockSpec(memory_space=pltpu.VMEM)
    dma = pltpu.SemaphoreType.DMA
    return pl.pallas_call(
        exchange_kernel,
        name='exchange',
        out_shape=[pltpu.VMEM((ROWS, D), BF), pltpu.VMEM((TOPK, ROWS), F32)] + [pltpu.VMEM((ROWS, D + HALF), F32)] * 2 + [pltpu.VMEM((ROWS, D), F32)] * 2 + [pltpu.VMEM((D, TOK), BF), pltpu.VMEM((TOK, D), BF)]
        + [pltpu.VMEM((EXP, TOK, FF), BF)] * 3 + [pltpu.VMEM((TOK, 128), F32)],
        in_specs=[any_spec] * 12,
        out_specs=[vmem] * 12,
        scratch_shapes=[
            pltpu.VMEM((TOPK, ROWS), jnp.int32), pltpu.VMEM((TOPK, ROWS), F32),
            pltpu.VMEM((3, TOK, D), BF),
            pltpu.VMEM((EXP, D, FF), BF), pltpu.VMEM((EXP, D, FF), BF), pltpu.VMEM((EXP, FF, D), BF),
            pltpu.VMEM((256, D), BF), pltpu.VMEM((2, 128, HALF), BF), pltpu.VMEM((2, 128, HALF), BF),
            pltpu.VMEM((4, 128, 128), BF), pltpu.VMEM((2, 2, 128, 128), BF),
            pltpu.VMEM((EXP, TOK, D), BF),
            pltpu.VMEM((EXP, TOK, FF), F32), pltpu.VMEM((EXP, TOK, FF), F32),
            pltpu.VMEM((8, 8, 128), F32), pltpu.VMEM((8, 8, 128), F32),
            pltpu.VMEM((TOK, 128), F32), pltpu.VMEM((4, 8, 128), F32), pltpu.VMEM((8, 8, 128), F32),
            pltpu.VMEM((3, 2, 2, 4, ROWS, HALF), F32), pltpu.VMEM((3, 2, 4, ROWS, HALF), F32),
            pltpu.VMEM((3, 2, 2, ROWS, HALF), F32), pltpu.VMEM((3, 2, 2, ROWS, HALF), F32),
            pltpu.VMEM((3, 2, ROWS, HALF), F32), pltpu.VMEM((3, 2, ROWS, HALF), F32),
            dma((3,)), dma((1 + EXP,)), dma((1,)), dma((4,)),
            dma((3, 2)), dma((12,)), dma((3,)), dma((24,)), dma((1,)), dma((1,)), dma((2,)), dma((4,)),
        ],
        compiler_params=pltpu.CompilerParams(collective_id=0, has_side_effects=True, vmem_limit_bytes=50 * 1024 * 1024),
    )(x, dy, xa, idx, gates, wg, wu, wd, wq, wk, wv, wo)


def grads_kernel(xt_ref, dy_ref, gt_ref, h_ref, da_ref, db_ref, y_in, dg_in, dwg_out, dwu_out, dwd_out, y_out, dg_out,
                 gate_buf, up_buf, down_buf, sem, small_sem):
    small = [pltpu.make_async_copy(y_in, y_out, small_sem.at[0]), pltpu.make_async_copy(dg_in, dg_out, small_sem.at[1])]
    for cp in small:
        cp.start()

    def leave(e, slot, n):
        buf, out = ((gate_buf, dwg_out), (up_buf, dwu_out), (down_buf, dwd_out))[n]
        return pltpu.make_async_copy(buf.at[slot], out.at[e], sem.at[n, slot])

    def body(e, carry):
        slot = e % 2

        @pl.when(e >= 2)
        def _():
            for n in range(3):
                leave(e - 2, slot, n).wait()
        gate_buf[slot] = jnp.dot(xt_ref[...], da_ref[e], preferred_element_type=F32)
        leave(e, slot, 0).start()
        up_buf[slot] = jnp.dot(xt_ref[...], db_ref[e], preferred_element_type=F32)
        leave(e, slot, 1).start()
        lane = lax.broadcasted_iota(jnp.int32, (TOK, 128), 1)
        g = jnp.sum(jnp.where(lane == e, gt_ref[...], 0.0), axis=1, keepdims=True)
        do = (g * dy_ref[...].astype(F32)).astype(BF)
        down_buf[slot] = lax.dot_general(h_ref[e], do, TN, preferred_element_type=F32)
        leave(e, slot, 2).start()
        return carry

    lax.fori_loop(0, EXP, body, 0)
    for e in (EXP - 2, EXP - 1):
        for n in range(3):
            leave(e, e % 2, n).wait()
    for cp in small:
        cp.wait()


def weight_grads(*args):
    sds = jax.ShapeDtypeStruct
    args = [pltpu.with_memory_space_constraint(v, pltpu.VMEM) for v in args]
    return pl.pallas_call(
        grads_kernel,
        name='weight_grads',
        out_shape=[sds((EXP, D, FF), F32), sds((EXP, D, FF), F32), sds((EXP, FF, D), F32),
                   sds((ROWS, D), BF), sds((TOPK, ROWS), F32)],
        in_specs=[pl.BlockSpec(memory_space=pltpu.VMEM)] * 8,
        out_specs=[pl.BlockSpec(memory_space=pl.ANY)] * 5,
        scratch_shapes=[pltpu.VMEM((2, D, FF), F32), pltpu.VMEM((2, D, FF), F32), pltpu.VMEM((2, FF, D), F32),
                        pltpu.SemaphoreType.DMA((3, 2)), pltpu.SemaphoreType.DMA((2,))],
        cost_estimate=pl.CostEstimate(flops=3 * 2 * EXP * TOK * D * FF, bytes_accessed=34 * 1024 * 1024, transcendentals=0),
        compiler_params=pltpu.CompilerParams(vmem_limit_bytes=40 * 1024 * 1024),
    )(*args)


def combine_kernel(dx_ref, at_ref, x_ref, y_ref, dx_out, at_out):
    dx_out[...] = (dx_ref[...] + x_ref[:, 0:D] + y_ref[:, 0:D]).astype(BF)
    at_out[:, 0:HALF] = (at_ref[:, 0:HALF] + y_ref[:, D:D + HALF]).astype(BF)
    at_out[:, HALF:D] = (at_ref[:, HALF:D] + x_ref[:, D:D + HALF]).astype(BF)


def combine(*args):
    sds = jax.ShapeDtypeStruct
    args = [pltpu.with_memory_space_constraint(v, pltpu.VMEM) for v in args]
    vmem = pl.BlockSpec(memory_space=pltpu.VMEM)
    return pl.pallas_call(combine_kernel, name='combine', out_shape=[sds((ROWS, D), BF)] * 2,
                          in_specs=[vmem] * 4, out_specs=[vmem] * 2)(*args)


def solution(mesh):
    def local_step(x_tokens, expert_idx, gate_vals, dy_tokens, w_gate, w_up, w_down, x_attn, w_query, w_key, w_value, w_out):
        y_p, dg_p, to_x, to_y, own_dx, own_at, xt, dyall, h, da, db, gt = exchange(
            x_tokens, dy_tokens, x_attn.reshape(ROWS, D), expert_idx.T, gate_vals.T, w_gate, w_up, w_down,
            w_query.transpose(1, 2, 0).reshape(128, D), w_key.transpose(1, 2, 0).reshape(64, D),
            w_value.transpose(1, 2, 0).reshape(64, D), w_out.reshape(128, D))
        from_x = lax.ppermute(to_x, GROUP_AXES, [(g, g ^ 2) for g in range(8)])
        from_y = lax.ppermute(to_y, GROUP_AXES, [(g, g ^ 4) for g in range(8)])
        dwg, dwu, dwd, y_t, dg = weight_grads(xt, dyall, gt, h, da, db, y_p, dg_p)
        dx_t, at = combine(own_dx, own_at, from_x, from_y)
        return y_t, dx_t, dg.T, dwg, dwu, dwd, at.reshape(1, ROWS, D)

    spec_rows = P(TOKEN_AXES, None)
    spec_seqs = P(TOKEN_AXES, None, None)
    spec_experts = P(GROUP_AXES, None, None)
    spec_heads = P(None, GROUP_AXES, None)
    return jax.shard_map(local_step, mesh=mesh,
                         in_specs=(spec_rows, spec_rows, spec_rows, spec_rows, spec_experts, spec_experts, spec_experts, spec_seqs, spec_heads, spec_heads, spec_heads, spec_experts),
                         out_specs=(spec_rows, spec_rows, spec_rows, spec_seqs, spec_seqs, spec_seqs, spec_seqs),
                         check_vma=False)
```

```python
import functools

import jax
import jax.numpy as jnp
from jax import lax
from jax.experimental import pallas as pl
from jax.experimental.pallas import tpu as pltpu
from jax.sharding import PartitionSpec as P

MESH = pl.DeviceIdType.MESH
GROUP_AXES = ('ei', 'eo')
TOKEN_AXES = ('dp', 'ei', 'eo')
BF = jnp.bfloat16
F32 = jnp.float32

ROWS = 64
TOK = 512
D = 1024
FF = 512
HALF = 512
EXP = 4
TOPK = 8
XA, XT, DY = 0, 1, 2

NT = (((1,), (1,)), ((), ()))
TN = (((0,), (0,)), ((), ()))


def exchange_kernel(x_hbm, dy_hbm, xa_hbm, idx_hbm, gate_hbm, wg_hbm, wu_hbm, wd_hbm, wq_hbm, wk_hbm, wv_hbm, wo_hbm,
                    y_out, dg_out, tox, toy, own_dx, own_at, xt, dyall, hid, dag, dbg, gt,
                    idx_ref, gate_ref, rows, wg, wu, wd, wqkv, wo, wo_in, ctx, ctx_in, osv, act, gfac, gsend, grecv,
                    dgs, dsend, drecv,
                    part, pair, s1, r1, s2, r2,
                    in_sem, w_sem, gs_sem, gr_sem, rs_s, rs_r, ag_s, ag_r, dd_s, dd_r, hd_s, hd_r):
    y = lax.axis_index('ei')
    o = lax.axis_index('eo')
    z = lax.axis_index('dp')
    x = o // 2
    c = o % 2
    me = y * 4 + o
    q0 = 2 * y + x
    qx = 2 * y + (1 - x)
    qy = 2 * (1 - y) + x
    qd = 2 * (1 - y) + (1 - x)

    def dev(fx, fy, fc):
        xx = (1 - x) if fx else x
        yy = (1 - y) if fy else y
        cc = (1 - c) if fc else c
        return (z, yy, xx * 2 + cc)

    sib, xn, yn = dev(0, 0, 1), dev(1, 0, 0), dev(0, 1, 0)
    rels = [(fx, fy, fc) for fx in (0, 1) for fy in (0, 1) for fc in (0, 1) if fx or fy or fc]

    barrier = pltpu.get_barrier_semaphore()
    for rel in rels:
        pl.semaphore_signal(barrier, inc=1, device_id=dev(*rel), device_id_type=MESH)

    own = pl.ds(pl.multiple_of(me * ROWS, ROWS), ROWS)
    tables = [pltpu.make_async_copy(idx_hbm, idx_ref, in_sem.at[1]), pltpu.make_async_copy(gate_hbm, gate_ref, in_sem.at[2])]
    for cp in tables:
        cp.start()
    for t, src in ((XT, x_hbm), (DY, dy_hbm), (XA, xa_hbm)):
        pltpu.make_async_copy(src, rows.at[t, own], in_sem.at[0 if t == XT else 3]).start()

    def expert_load(e):
        return [pltpu.make_async_copy(src.at[e], dst.at[e], w_sem.at[1 + e])
                for src, dst in ((wg_hbm, wg), (wu_hbm, wu), (wd_hbm, wd))]

    for e in range(EXP):
        for cp in expert_load(e):
            cp.start()
    wload = [pltpu.make_async_copy(wq_hbm, wqkv.at[0:128], w_sem.at[0]),
             pltpu.make_async_copy(wk_hbm, wqkv.at[128:192], w_sem.at[0]),
             pltpu.make_async_copy(wv_hbm, wqkv.at[192:256], w_sem.at[0]),
             pltpu.make_async_copy(wo_hbm.at[:, 0:HALF], wo.at[0], w_sem.at[0]),
             pltpu.make_async_copy(wo_hbm.at[:, HALF:D], wo.at[1], w_sem.at[0])]
    for cp in wload:
        cp.start()

    for cp in tables:
        cp.wait()
    exp_row = lax.broadcasted_iota(jnp.int32, (32, ROWS), 0)
    table = jnp.zeros((32, ROWS), F32)
    marks = jnp.zeros((32, ROWS), F32)
    for j in range(TOPK):
        hit = exp_row == idx_ref[j:j + 1, :]
        table = table + jnp.where(hit, gate_ref[j:j + 1, :], 0.0)
        marks = marks + jnp.where(hit, 1.0, 0.0)
    wide = jnp.concatenate([table, marks], axis=1)
    for d in range(8):
        gsend[d] = wide[d * EXP:(d + 1) * EXP, :]
    grecv[me] = gsend[me]

    def blk(t, q, off=0, n=ROWS):
        return rows.at[t, pl.ds(pl.multiple_of(q * 128 + c * ROWS + off, 32), n)]

    def remote(src, dst, ss, rs, where):
        return pltpu.make_async_remote_copy(src, dst, ss, rs, device_id=where, device_id_type=MESH)

    hr = ROWS // 2

    def gather_slot(t, k):
        if 1 <= k <= 6:
            return 3 * t + (0 if k in (1, 3) else 1 if k in (2, 4) else 2)
        return 9 + t if t != XT else {0: 12, 7: 13, 8: 14}.get(k, 10)

    def gather_copies(t):
        def cp(k, ref, where):
            return remote(ref, ref, ag_s.at[t], ag_r.at[gather_slot(t, k)], where)
        return [cp(0, blk(t, q0), sib),
                cp(1, blk(t, q0, 0, hr), xn), cp(2, blk(t, q0, hr, hr), xn),
                cp(3, blk(t, q0, hr, hr), yn), cp(4, blk(t, q0, 0, hr), yn),
                cp(5, blk(t, qx, 0, hr), yn), cp(6, blk(t, qy, hr, hr), xn),
                cp(7, blk(t, qx), sib), cp(8, blk(t, qy), sib),
                cp(9, blk(t, qd, 0, hr), sib), cp(10, blk(t, qd, hr, hr), sib)]

    ag = [gather_copies(t) for t in range(3)]

    def ag_own(t):
        for k in (1, 3, 2, 4, 0):
            ag[t][k].start()

    def ag_own_a(t):
        ag[t][1].start()
        ag[t][3].start()

    def ag_own_b(t):
        for k in (2, 4, 0):
            ag[t][k].start()

    def ag_forward(t):
        ag_rows(t, 1, ROWS).wait_recv()
        ag[t][5].start()
        ag[t][6].start()

    def ag_pair(t):
        ag_rows(t, 2, ROWS).wait_recv()
        ag[t][7].start()
        ag[t][8].start()

    def ag_last(t):
        ag_rows(t, 5, ROWS).wait_recv()
        ag[t][9].start()
        ag[t][10].start()

    def ag_rows(t, k, n):
        ref = rows.at[t, 0:n]
        return remote(ref, ref, ag_s.at[t], ag_r.at[gather_slot(t, k)], sib)

    def tile_copies(send, recv, ss, rs, chip_tiles):
        cps = {}
        for fx, fy, fc in rels:
            where = dev(fx, fy, fc)
            qq = 2 * where[1] + where[2] // 2
            src = send.at[qq] if chip_tiles else send.at[where[1] * 4 + where[2]]
            cps[fx, fy, fc] = remote(src, recv.at[me], ss.at[0], rs.at[0 if chip_tiles else fx + 2 * fy], where)
        return cps

    gate_cps = tile_copies(gsend, grecv, gs_sem, gr_sem, False)
    dg_cps = tile_copies(dsend, drecv, dd_s, dd_r, True)
    chips = (q0, qx, qy, qd)
    OWN, X, Y, DI = 0, 1, 2, 3
    first = (X, Y)
    second = (Y, X)

    def rs_slot(n, k):
        if k >= 8:
            kind = (k - 8) % 3
            group = 2 if kind == 0 else 1
        else:
            group = 0 if k // 2 == DI else 1
            if n == 1 and k // 2 in (X, Y):
                group = 3 if k == 2 * X else 4 if k == 2 * Y + 1 else 5
        return (0, 3, 9)[n] + group

    def rs_wait(n, k, count):
        ref = pair.at[n, 0, 0:2] if count == 2 else pair.at[n, :, 0:3] if count == 6 else pair.at[n, 0, 0]
        remote(ref, ref, rs_s.at[n, 0], rs_r.at[rs_slot(n, k)], sib).wait_recv()

    def rs_copies(n):
        def cp(k, src, dst, where):
            return remote(src, dst, rs_s.at[n, 0 if k < 8 else 1], rs_r.at[rs_slot(n, k)], where)
        cps = [cp(2 * k + h, part.at[n, 1 - c, h, chips[k]], pair.at[n, h, chips[k]], sib) for k in range(4) for h in range(2)]
        for h in range(2):
            one, two = (xn, yn) if h == 0 else (yn, xn)
            cps += [cp(8 + 3 * h, s1.at[n, h, 0], r1.at[n, h, 0], one), cp(9 + 3 * h, s1.at[n, h, 1], r1.at[n, h, 1], one),
                    cp(10 + 3 * h, s2.at[n, h], r2.at[n, h], two)]
        return cps

    rsc = [rs_copies(n) for n in range(3)]

    def rs_pair(n, k):
        rsc[n][2 * k].start()
        rsc[n][2 * k + 1].start()

    def chip_sum(n, h, k):
        return part[n, c, h, chips[k]] + pair[n, h, chips[k]]

    def rs_far(n):
        rs_wait(n, 2 * DI, 2)
        for h in range(2):
            s1[n, h, 0] = chip_sum(n, h, DI)
            rsc[n][8 + 3 * h].start()

    def rs_near(n, h):
        k = first[h]
        rs_wait(n, 2 * k + h, 1)
        s1[n, h, 1] = chip_sum(n, h, k)
        rsc[n][9 + 3 * h].start()

    def rs_second(n):
        rs_wait(n, 2 * Y, 2)
        rs_wait(n, 8, 2)
        for h in range(2):
            k = second[h]
            s2[n, h] = chip_sum(n, h, k) + r1[n, h, 0]
            rsc[n][10 + 3 * h].start()

    def rs_final(n, out_ref):
        rs_wait(n, 2 * OWN, 6)
        for h in range(2):
            total = chip_sum(n, h, OWN) + r1[n, h, 1] + r2[n, h]
            out_ref[:, h * HALF:(h + 1) * HALF] = total.astype(BF)

    def head_copy(src, dst, slot, where):
        return remote(src, dst, hd_s.at[slot // 2], hd_r.at[slot], where)

    wo_cps = [head_copy(wo.at[h, r:r + 64], wo_in.at[h, r:r + 64], h, (xn, yn)[h]) for r in (0, 64) for h in range(2)]
    ctx_cps = [head_copy(ctx.at[q], ctx_in.at[h, i], 2 + h, (xn, yn)[h])
               for h, qn in ((0, qx), (1, qy)) for i, q in ((0, qn), (1, qd))]

    def gate_table(k):
        tiles = grecv.at[0:1 if k == OWN else 2]
        remote(tiles, tiles, gs_sem.at[0], gr_sem.at[k], sib).wait_recv()
        q = chips[k]
        t0, t1 = grecv[2 * q], grecv[2 * q + 1]
        tile = jnp.concatenate([jnp.concatenate([t0[:, :ROWS], t1[:, :ROWS]], axis=1),
                                jnp.concatenate([t0[:, ROWS:], t1[:, ROWS:]], axis=1)], axis=0)
        gt[pl.ds(pl.multiple_of(q * 128, 128), 128), :] = jnp.concatenate([tile, jnp.zeros((120, 128), F32)], axis=0).T

    def pick(tile, e):
        lane = lax.broadcasted_iota(jnp.int32, tile.shape, 1)
        return jnp.sum(jnp.where(lane == e, tile, 0.0), axis=1, keepdims=True)

    def accumulate(n, q, val):
        for cc in range(2):
            for h in range(2):
                part[n, cc, h, q] += val[cc * 64:(cc + 1) * 64, h * HALF:(h + 1) * HALF]

    def experts(step, hooks):
        def body(e, carry):
            step(e)
            for at, fn in hooks.items():
                @pl.when(e == at)
                def _():
                    fn()
            return carry
        lax.fori_loop(0, EXP, body, 0)

    def chip_rows(k):
        return pl.ds(pl.multiple_of(chips[k] * 128, 128), 128)

    def forward(ks, load=False):
        def stack(ref, *at):
            return jnp.concatenate([ref[(*at, chip_rows(k), slice(None))] for k in ks], axis=0)

        def step(e):
            if load:
                pltpu.make_async_copy(wg_hbm.at[0:3], wg.at[0:3], w_sem.at[1 + e]).wait()

            def put(ref, val):
                for i, k in enumerate(ks):
                    ref[e, chip_rows(k), :] = val[i * 128:(i + 1) * 128]

            xs = stack(rows, XT)
            a = jnp.dot(xs, wg[e], preferred_element_type=F32)
            b = jnp.dot(xs, wu[e], preferred_element_type=F32)
            tile = stack(gt)
            mark = pick(tile, e + 4) > 0.5
            sg = jax.nn.sigmoid(a)
            ac = a * sg
            put(act, jnp.where(mark, ac, 0.0))
            put(gfac, jnp.where(mark, b * sg * (1.0 + a * (1.0 - sg)), 0.0))
            hh = jnp.where(mark, ac * b, 0.0).astype(BF)
            put(hid, hh)
            ob = jnp.dot(hh, wd[e], preferred_element_type=F32).astype(BF)
            put(osv, ob)
            yb = pick(tile, e) * ob.astype(F32)
            for i, k in enumerate(ks):
                accumulate(1, chips[k], yb[i * 128:(i + 1) * 128])
        return step

    def backward(qa, qb, base, gates):
        sl = pl.ds(pl.multiple_of(base, 256), 256)

        def step(e):
            g = pick(gt[sl, :], e)
            dyf = rows[DY, sl, :].astype(F32)
            do = (g * dyf).astype(BF)
            dh = lax.dot_general(do, wd[e], NT, preferred_element_type=F32).astype(BF).astype(F32)
            da = (dh * gfac[e, sl, :]).astype(BF)
            db = (dh * act[e, sl, :]).astype(BF)
            dag[e, sl, :] = da
            dbg[e, sl, :] = db
            if gates:
                lane = lax.broadcasted_iota(jnp.int32, (256, 128), 1)
                for r in (slice(0, 256), slice(256, 512)):
                    dg = jnp.sum(rows[DY, r, :].astype(F32) * osv[e, r, :].astype(F32), axis=1, keepdims=True)
                    dgs[r, :] += jnp.where(lane == e, dg, 0.0)
            dx = (lax.dot_general(da, wg[e], NT, preferred_element_type=F32)
                  + lax.dot_general(db, wu[e], NT, preferred_element_type=F32)).astype(BF).astype(F32)
            accumulate(2, qa, dx[0:128])
            accumulate(2, qb, dx[128:256])
        return step

    def attention_context():
        ag_rows(XA, 0, 4 * ROWS).wait_recv()
        causal_r = lax.broadcasted_iota(jnp.int32, (256, 128), 0) % 128
        causal_c = lax.broadcasted_iota(jnp.int32, (256, 128), 1)
        keep = (causal_r >= causal_c) & (causal_r // 64 == causal_c // 64)
        qkv = lax.dot_general(rows[XA], wqkv[...], NT, preferred_element_type=F32).astype(BF)
        qkvs = [qkv[q * 128:(q + 1) * 128] for q in range(4)]
        scs = [lax.dot_general(jnp.concatenate([v[:, 0:64], v[:, 64:128]], axis=0), v[:, 128:192], NT,
                               preferred_element_type=F32) * (64 ** -0.5) for v in qkvs]
        scs = [jnp.where(keep, sc, -1e30) for sc in scs]
        mxs = [jnp.max(sc, axis=1, keepdims=True) for sc in scs]
        exs = [jnp.exp(sc - mx) for sc, mx in zip(scs, mxs)]
        sms = [jnp.sum(ex, axis=1, keepdims=True) for ex in exs]
        prs = [(ex / sm).astype(BF) for ex, sm in zip(exs, sms)]
        ctxs = [jnp.dot(pr, v[:, 192:256], preferred_element_type=F32).astype(BF) for pr, v in zip(prs, qkvs)]
        for q, v in enumerate(ctxs):
            ctx[q] = jnp.concatenate([v[0:128], v[128:256]], axis=1)

    def attention_out():
        for h in range(2):
            head_copy(wo_in.at[h], wo_in.at[h], h, sib).wait_recv()
            both = ctx_in.at[h]
            head_copy(both, both, 2 + h, sib).wait_recv()
            for i, k in ((0, OWN), (1, second[h])):
                out = (jnp.dot(ctx[chips[k]], wo[h], preferred_element_type=F32)
                       + jnp.dot(ctx_in[h, i], wo_in[h], preferred_element_type=F32))
                for cc in range(2):
                    part[0, cc, h, chips[k]] = out[cc * 64:(cc + 1) * 64]
        for h in range(2):
            rsc[0][2 * OWN + h].start()
            rsc[0][2 * second[h] + h].start()

    def leave_attention():
        ref = pair.at[0, 0]
        remote(ref, ref, rs_s.at[0, 0], rs_r.at[rs_slot(0, 2 * OWN)], sib).wait_recv()
        for h, dst in ((0, toy), (1, tox)):
            dst[:, D:D + HALF] = chip_sum(0, h, second[h])
            own_at[:, h * HALF:(h + 1) * HALF] = chip_sum(0, h, OWN)

    def leave_dx():
        n = 2
        rs_wait(n, 2 * OWN, 6)
        rs_wait(n, 8, 2)
        for h in range(2):
            cols = slice(h * HALF, (h + 1) * HALF)
            near = chip_sum(n, h, first[h])
            far = chip_sum(n, h, second[h]) + r1[n, h, 0]
            tox[:, cols] = near if h == 0 else far
            toy[:, cols] = far if h == 0 else near
            own_dx[:, cols] = chip_sum(n, h, OWN)

    pltpu.make_async_copy(x_hbm, rows.at[XT, own], in_sem.at[0]).wait()
    pl.semaphore_wait(barrier, len(rels))
    ag_own(XT)
    for cp in gate_cps.values():
        cp.start()
    pltpu.make_async_copy(wg_hbm.at[0, 0:4 * ROWS], wg.at[0, 0:4 * ROWS], in_sem.at[3]).wait()
    ag_own(XA)
    dgs[...] = jnp.zeros((TOK, 128), F32)
    part[1] = jnp.zeros(part.shape[1:], F32)
    part[2] = jnp.zeros(part.shape[1:], F32)
    gate_table(OWN)
    ag[XT][0].wait_recv()
    experts(forward([OWN], True), {2: lambda: ag_forward(XT)})
    rs_pair(1, OWN)
    ag_pair(XT)
    gate_table(X)
    gate_table(Y)
    ag_own_a(DY)
    ag[XT][7].wait_recv()
    ag[XT][8].wait_recv()
    experts(forward([X, Y]), {0: lambda: (ag_forward(XA), ag_own_b(DY)), 1: lambda: ag_pair(XA), 2: lambda: ag_last(XT)})
    rs_pair(1, X)
    rs_pair(1, Y)
    gate_table(DI)
    ag_forward(DY)
    pltpu.make_async_copy(wg_hbm.at[0, 0:768], wg.at[0, 0:768], w_sem.at[0]).wait()
    for cp in wo_cps[:2]:
        cp.start()
    ag_rows(XT, 9, ROWS).wait_recv()
    experts(forward([DI]), {1: lambda: (rs_near(1, 0), rs_near(1, 1), ag_last(XA)), 2: lambda: ag_pair(DY)})
    rs_pair(1, DI)
    ag_last(DY)
    attention_context()
    rs_far(1)
    for cp in ctx_cps + wo_cps[2:]:
        cp.start()
    ag_rows(DY, 0, 4 * ROWS).wait_recv()
    dyall[...] = rows[DY]
    experts(backward(2 * (1 - y), 2 * (1 - y) + 1, (1 - y) * 256, True), {3: lambda: rs_second(1)})
    rs_pair(2, DI)
    rs_pair(2, Y)
    for q in range(4):
        dsend[q] = dgs[q * 128:(q + 1) * 128, :].T[0:EXP, :]
    drecv[me] = dsend[q0]
    for cp in dg_cps.values():
        cp.start()
    experts(backward(2 * y, 2 * y + 1, y * 256, False), {0: lambda: rs_far(2)})
    rs_pair(2, X)
    rs_pair(2, OWN)
    attention_out()
    rs_wait_dg = drecv.at[0:7]
    remote(rs_wait_dg, rs_wait_dg, dd_s.at[0], dd_r.at[0], sib).wait_recv()
    both = jnp.concatenate([drecv[d] for d in range(8)], axis=0)
    mine = jnp.where(c == 0, both[:, 0:ROWS], both[:, ROWS:128])
    for j in range(TOPK):
        hit = exp_row == idx_ref[j:j + 1, :]
        dg_out[j:j + 1, :] = jnp.sum(jnp.where(hit, mine, 0.0), axis=0, keepdims=True)
    rs_final(1, y_out)
    leave_attention()
    xt[...] = rows[XT].T
    leave_dx()

    for t in range(3):
        ref = rows.at[t, 0:7 * ROWS]
        remote(ref, ref, ag_s.at[t], ag_r.at[0], sib).wait_send()
    tiles = gsend.at[0:7]
    remote(tiles, tiles, gs_sem.at[0], gr_sem.at[0], sib).wait_send()
    remote(tiles, tiles, dd_s.at[0], dd_r.at[0], sib).wait_send()
    for ref, n, k in ((pair.at[0, 0], 0, 0), (part.at[1, 0], 1, 0), (part.at[2, 0], 2, 0),
                      (pair.at[1, :, 0:3], 1, 1), (pair.at[2, 0, 0:2], 2, 1)):
        remote(ref, ref, rs_s.at[n, k], rs_r.at[0], sib).wait_send()
    remote(wo, wo, hd_s.at[0], hd_r.at[0], sib).wait_send()
    remote(ctx, ctx, hd_s.at[1], hd_r.at[0], sib).wait_send()


def exchange(x, dy, xa, idx, gates, wg, wu, wd, wq, wk, wv, wo):
    any_spec = pl.BlockSpec(memory_space=pl.ANY)
    vmem = pl.BlockSpec(memory_space=pltpu.VMEM)
    dma = pltpu.SemaphoreType.DMA
    return pl.pallas_call(
        exchange_kernel,
        name='exchange',
        out_shape=[pltpu.VMEM((ROWS, D), BF), pltpu.VMEM((TOPK, ROWS), F32)] + [pltpu.VMEM((ROWS, D + HALF), F32)] * 2 + [pltpu.VMEM((ROWS, D), F32)] * 2 + [pltpu.VMEM((D, TOK), BF), pltpu.VMEM((TOK, D), BF)]
        + [pltpu.VMEM((EXP, TOK, FF), BF)] * 3 + [pltpu.VMEM((TOK, 128), F32)],
        in_specs=[any_spec] * 12,
        out_specs=[vmem] * 12,
        scratch_shapes=[
            pltpu.VMEM((TOPK, ROWS), jnp.int32), pltpu.VMEM((TOPK, ROWS), F32),
            pltpu.VMEM((3, TOK, D), BF),
            pltpu.VMEM((EXP, D, FF), BF), pltpu.VMEM((EXP, D, FF), BF), pltpu.VMEM((EXP, FF, D), BF),
            pltpu.VMEM((256, D), BF), pltpu.VMEM((2, 128, HALF), BF), pltpu.VMEM((2, 128, HALF), BF),
            pltpu.VMEM((4, 128, 128), BF), pltpu.VMEM((2, 2, 128, 128), BF),
            pltpu.VMEM((EXP, TOK, D), BF),
            pltpu.VMEM((EXP, TOK, FF), F32), pltpu.VMEM((EXP, TOK, FF), F32),
            pltpu.VMEM((8, EXP, 128), F32), pltpu.VMEM((8, EXP, 128), F32),
            pltpu.VMEM((TOK, 128), F32), pltpu.VMEM((4, EXP, 128), F32), pltpu.VMEM((8, EXP, 128), F32),
            pltpu.VMEM((3, 2, 2, 4, ROWS, HALF), F32), pltpu.VMEM((3, 2, 4, ROWS, HALF), F32),
            pltpu.VMEM((3, 2, 2, ROWS, HALF), F32), pltpu.VMEM((3, 2, 2, ROWS, HALF), F32),
            pltpu.VMEM((3, 2, ROWS, HALF), F32), pltpu.VMEM((3, 2, ROWS, HALF), F32),
            dma((4,)), dma((1 + EXP,)), dma((1,)), dma((4,)),
            dma((3, 2)), dma((12,)), dma((3,)), dma((15,)), dma((1,)), dma((1,)), dma((2,)), dma((4,)),
        ],
        compiler_params=pltpu.CompilerParams(collective_id=0, has_side_effects=True, vmem_limit_bytes=50 * 1024 * 1024),
    )(x, dy, xa, idx, gates, wg, wu, wd, wq, wk, wv, wo)


def grads_kernel(xt_ref, dy_ref, gt_ref, h_ref, da_ref, db_ref, y_in, dg_in, dwg_out, dwu_out, dwd_out, y_out, dg_out,
                 gate_buf, up_buf, down_buf, sem, small_sem):
    small = [pltpu.make_async_copy(y_in, y_out, small_sem.at[0]), pltpu.make_async_copy(dg_in, dg_out, small_sem.at[1])]
    for cp in small:
        cp.start()

    def leave(e, slot, n):
        buf, out = ((gate_buf, dwg_out), (up_buf, dwu_out), (down_buf, dwd_out))[n]
        return pltpu.make_async_copy(buf.at[slot], out.at[e], sem.at[n, slot])

    def body(e, carry):
        slot = e % 2

        @pl.when(e >= 2)
        def _():
            for n in range(3):
                leave(e - 2, slot, n).wait()
        gate_buf[slot] = jnp.dot(xt_ref[...], da_ref[e], preferred_element_type=F32)
        leave(e, slot, 0).start()
        up_buf[slot] = jnp.dot(xt_ref[...], db_ref[e], preferred_element_type=F32)
        leave(e, slot, 1).start()
        lane = lax.broadcasted_iota(jnp.int32, (TOK, 128), 1)
        g = jnp.sum(jnp.where(lane == e, gt_ref[...], 0.0), axis=1, keepdims=True)
        do = (g * dy_ref[...].astype(F32)).astype(BF)
        down_buf[slot] = lax.dot_general(h_ref[e], do, TN, preferred_element_type=F32)
        leave(e, slot, 2).start()
        return carry

    lax.fori_loop(0, EXP, body, 0)
    for e in (EXP - 2, EXP - 1):
        for n in range(3):
            leave(e, e % 2, n).wait()
    for cp in small:
        cp.wait()


def weight_grads(*args):
    sds = jax.ShapeDtypeStruct
    args = [pltpu.with_memory_space_constraint(v, pltpu.VMEM) for v in args]
    return pl.pallas_call(
        grads_kernel,
        name='weight_grads',
        out_shape=[sds((EXP, D, FF), F32), sds((EXP, D, FF), F32), sds((EXP, FF, D), F32),
                   sds((ROWS, D), BF), sds((TOPK, ROWS), F32)],
        in_specs=[pl.BlockSpec(memory_space=pltpu.VMEM)] * 8,
        out_specs=[pl.BlockSpec(memory_space=pl.ANY)] * 5,
        scratch_shapes=[pltpu.VMEM((2, D, FF), F32), pltpu.VMEM((2, D, FF), F32), pltpu.VMEM((2, FF, D), F32),
                        pltpu.SemaphoreType.DMA((3, 2)), pltpu.SemaphoreType.DMA((2,))],
        cost_estimate=pl.CostEstimate(flops=3 * 2 * EXP * TOK * D * FF, bytes_accessed=34 * 1024 * 1024, transcendentals=0),
        compiler_params=pltpu.CompilerParams(vmem_limit_bytes=40 * 1024 * 1024),
    )(*args)


def combine_kernel(dx_ref, at_ref, x_ref, y_ref, dx_out, at_out):
    dx_out[...] = (dx_ref[...] + x_ref[:, 0:D] + y_ref[:, 0:D]).astype(BF)
    at_out[:, 0:HALF] = (at_ref[:, 0:HALF] + y_ref[:, D:D + HALF]).astype(BF)
    at_out[:, HALF:D] = (at_ref[:, HALF:D] + x_ref[:, D:D + HALF]).astype(BF)


def combine(*args):
    sds = jax.ShapeDtypeStruct
    args = [pltpu.with_memory_space_constraint(v, pltpu.VMEM) for v in args]
    vmem = pl.BlockSpec(memory_space=pltpu.VMEM)
    return pl.pallas_call(combine_kernel, name='combine', out_shape=[sds((ROWS, D), BF)] * 2,
                          in_specs=[vmem] * 4, out_specs=[vmem] * 2)(*args)


def solution(mesh):
    def local_step(x_tokens, expert_idx, gate_vals, dy_tokens, w_gate, w_up, w_down, x_attn, w_query, w_key, w_value, w_out):
        y_p, dg_p, to_x, to_y, own_dx, own_at, xt, dyall, h, da, db, gt = exchange(
            x_tokens, dy_tokens, x_attn.reshape(ROWS, D), expert_idx.T, gate_vals.T, w_gate, w_up, w_down,
            w_query.transpose(1, 2, 0).reshape(128, D), w_key.transpose(1, 2, 0).reshape(64, D),
            w_value.transpose(1, 2, 0).reshape(64, D), w_out.reshape(128, D))
        from_x = lax.ppermute(to_x, GROUP_AXES, [(g, g ^ 2) for g in range(8)])
        from_y = lax.ppermute(to_y, GROUP_AXES, [(g, g ^ 4) for g in range(8)])
        dwg, dwu, dwd, y_t, dg = weight_grads(xt, dyall, gt, h, da, db, y_p, dg_p)
        dx_t, at = combine(own_dx, own_at, from_x, from_y)
        return y_t, dx_t, dg.T, dwg, dwu, dwd, at.reshape(1, ROWS, D)

    spec_rows = P(TOKEN_AXES, None)
    spec_seqs = P(TOKEN_AXES, None, None)
    spec_experts = P(GROUP_AXES, None, None)
    spec_heads = P(None, GROUP_AXES, None)
    return jax.shard_map(local_step, mesh=mesh,
                         in_specs=(spec_rows, spec_rows, spec_rows, spec_rows, spec_experts, spec_experts, spec_experts, spec_seqs, spec_heads, spec_heads, spec_heads, spec_experts),
                         out_specs=(spec_rows, spec_rows, spec_rows, spec_seqs, spec_seqs, spec_seqs, spec_seqs),
                         check_vma=False)
```

```python
import functools

import jax
import jax.numpy as jnp
from jax import lax
from jax.experimental import pallas as pl
from jax.experimental.pallas import tpu as pltpu
from jax.sharding import PartitionSpec as P

MESH = pl.DeviceIdType.MESH
GROUP_AXES = ('ei', 'eo')
TOKEN_AXES = ('dp', 'ei', 'eo')
BF = jnp.bfloat16
F32 = jnp.float32

ROWS = 64
TOK = 512
D = 1024
FF = 512
HALF = 512
EXP = 4
TOPK = 8
XA, XT, DY = 0, 1, 2

NT = (((1,), (1,)), ((), ()))
TN = (((0,), (0,)), ((), ()))


def exchange_kernel(x_hbm, dy_hbm, xa_hbm, idx_hbm, gate_hbm, wg_hbm, wu_hbm, wd_hbm, wq_hbm, wk_hbm, wv_hbm, wo_hbm,
                    y_out, dg_out, tox, toy, own_dx, own_at, xt, dyall, hid, dag, dbg, gt,
                    idx_ref, gate_ref, rows, wg, wu, wd, wqkv, wo, wo_in, ctx, ctx_in, osv, act, gfac, gsend, grecv,
                    dgs, dsend, drecv,
                    part, pair, s1, r1, s2, r2,
                    in_sem, w_sem, gs_sem, gr_sem, rs_s, rs_r, ag_s, ag_r, dd_r, hd_s, hd_r):
    y = lax.axis_index('ei')
    o = lax.axis_index('eo')
    z = lax.axis_index('dp')
    x = o // 2
    c = o % 2
    me = y * 4 + o
    q0 = 2 * y + x
    qx = 2 * y + (1 - x)
    qy = 2 * (1 - y) + x
    qd = 2 * (1 - y) + (1 - x)

    def dev(fx, fy, fc):
        xx = (1 - x) if fx else x
        yy = (1 - y) if fy else y
        cc = (1 - c) if fc else c
        return (z, yy, xx * 2 + cc)

    sib, xn, yn = dev(0, 0, 1), dev(1, 0, 0), dev(0, 1, 0)
    rels = [(fx, fy, fc) for fx in (0, 1) for fy in (0, 1) for fc in (0, 1) if fx or fy or fc]

    barrier = pltpu.get_barrier_semaphore()
    for rel in rels:
        pl.semaphore_signal(barrier, inc=1, device_id=dev(*rel), device_id_type=MESH)

    own = pl.ds(pl.multiple_of(me * ROWS, ROWS), ROWS)
    tables = [pltpu.make_async_copy(idx_hbm, idx_ref, in_sem.at[1]), pltpu.make_async_copy(gate_hbm, gate_ref, in_sem.at[2])]
    for cp in tables:
        cp.start()
    for t, src in ((XT, x_hbm), (DY, dy_hbm), (XA, xa_hbm)):
        pltpu.make_async_copy(src, rows.at[t, own], in_sem.at[0 if t == XT else 3]).start()

    def expert_load(e):
        return [pltpu.make_async_copy(src.at[e], dst.at[e], w_sem.at[1 + e])
                for src, dst in ((wg_hbm, wg), (wu_hbm, wu), (wd_hbm, wd))]

    for e in range(EXP):
        for cp in expert_load(e):
            cp.start()
    wload = [pltpu.make_async_copy(wq_hbm, wqkv.at[0:128], w_sem.at[0]),
             pltpu.make_async_copy(wk_hbm, wqkv.at[128:192], w_sem.at[0]),
             pltpu.make_async_copy(wv_hbm, wqkv.at[192:256], w_sem.at[0]),
             pltpu.make_async_copy(wo_hbm.at[:, 0:HALF], wo.at[0], w_sem.at[0]),
             pltpu.make_async_copy(wo_hbm.at[:, HALF:D], wo.at[1], w_sem.at[0])]
    for cp in wload:
        cp.start()

    def blk(t, q, off=0, n=ROWS):
        return rows.at[t, pl.ds(pl.multiple_of(q * 128 + c * ROWS + off, 32), n)]

    def remote(src, dst, ss, rs, where):
        return pltpu.make_async_remote_copy(src, dst, ss, rs, device_id=where, device_id_type=MESH)

    hr = ROWS // 2

    def gather_slot(t, k):
        if 1 <= k <= 6:
            return 3 * t + (0 if k in (1, 3) else 1 if k in (2, 4) else 2)
        return 9 + t if t != XT else {0: 12, 7: 13, 8: 14}.get(k, 10)

    def gather_copies(t):
        def cp(k, ref, where):
            return remote(ref, ref, ag_s.at[0], ag_r.at[gather_slot(t, k)], where)
        return [cp(0, blk(t, q0), sib),
                cp(1, blk(t, q0, 0, hr), xn), cp(2, blk(t, q0, hr, hr), xn),
                cp(3, blk(t, q0, hr, hr), yn), cp(4, blk(t, q0, 0, hr), yn),
                cp(5, blk(t, qx, 0, hr), yn), cp(6, blk(t, qy, hr, hr), xn),
                cp(7, blk(t, qx), sib), cp(8, blk(t, qy), sib),
                cp(9, blk(t, qd, 0, hr), sib), cp(10, blk(t, qd, hr, hr), sib)]

    ag = [gather_copies(t) for t in range(3)]

    def ag_own(t):
        for k in (1, 3, 2, 4, 0):
            ag[t][k].start()

    def ag_own_a(t):
        ag[t][1].start()
        ag[t][3].start()

    def ag_own_b(t):
        for k in (2, 4, 0):
            ag[t][k].start()

    def ag_forward(t):
        ag_rows(t, 1, ROWS).wait_recv()
        ag[t][5].start()
        ag[t][6].start()

    def ag_pair(t):
        ag_rows(t, 2, ROWS).wait_recv()
        ag[t][7].start()
        ag[t][8].start()

    def ag_last(t):
        ag_rows(t, 5, ROWS).wait_recv()
        ag[t][9].start()
        ag[t][10].start()

    def ag_rows(t, k, n):
        ref = rows.at[t, 0:n]
        return remote(ref, ref, ag_s.at[0], ag_r.at[gather_slot(t, k)], sib)

    def tile_copies(send, recv, ss, rs, chip_tiles):
        cps = {}
        for fx, fy, fc in rels:
            where = dev(fx, fy, fc)
            qq = 2 * where[1] + where[2] // 2
            src = send.at[qq] if chip_tiles else send.at[where[1] * 4 + where[2]]
            cps[fx, fy, fc] = remote(src, recv.at[me], ss.at[0], rs.at[0 if chip_tiles else fx + 2 * fy], where)
        return cps

    gate_cps = tile_copies(gsend, grecv, gs_sem, gr_sem, False)
    dg_cps = tile_copies(dsend, drecv, gs_sem, dd_r, True)
    chips = (q0, qx, qy, qd)
    OWN, X, Y, DI = 0, 1, 2, 3
    first = (X, Y)
    second = (Y, X)

    def rs_slot(n, k):
        if k >= 8:
            kind = (k - 8) % 3
            group = 2 if kind == 0 else 1
        else:
            group = 0 if k // 2 == DI else 1
            if n == 1 and k // 2 in (X, Y):
                group = 3 if k == 2 * X else 4 if k == 2 * Y + 1 else 5
        return (-1, 1, 7)[n] + group

    def rs_wait(n, k, count):
        ref = pair.at[n, 0, 0:2] if count == 2 else pair.at[n, :, 0:3] if count == 6 else pair.at[n, 0, 0]
        remote(ref, ref, rs_s.at[0], rs_r.at[rs_slot(n, k)], sib).wait_recv()

    def rs_copies(n):
        def cp(k, src, dst, where):
            return remote(src, dst, rs_s.at[0], rs_r.at[rs_slot(n, k)], where)
        cps = [cp(2 * k + h, part.at[n, 1 - c, h, chips[k]], pair.at[n, h, chips[k]], sib) for k in range(4) for h in range(2)]
        for h in range(2):
            one, two = (xn, yn) if h == 0 else (yn, xn)
            cps += [cp(8 + 3 * h, s1.at[n, h, 0], r1.at[n, h, 0], one), cp(9 + 3 * h, s1.at[n, h, 1], r1.at[n, h, 1], one),
                    cp(10 + 3 * h, s2.at[n, h], r2.at[n, h], two)]
        return cps

    rsc = [rs_copies(n) for n in range(3)]

    def rs_pair(n, k):
        rsc[n][2 * k].start()
        rsc[n][2 * k + 1].start()

    def chip_sum(n, h, k):
        return part[n, c, h, chips[k]] + pair[n, h, chips[k]]

    def rs_far(n):
        rs_wait(n, 2 * DI, 2)
        for h in range(2):
            s1[n, h, 0] = chip_sum(n, h, DI)
            rsc[n][8 + 3 * h].start()

    def rs_near(n, h):
        k = first[h]
        rs_wait(n, 2 * k + h, 1)
        s1[n, h, 1] = chip_sum(n, h, k)
        rsc[n][9 + 3 * h].start()

    def rs_second(n):
        rs_wait(n, 2 * Y, 2)
        rs_wait(n, 8, 2)
        for h in range(2):
            k = second[h]
            s2[n, h] = chip_sum(n, h, k) + r1[n, h, 0]
            rsc[n][10 + 3 * h].start()

    def rs_final(n, out_ref):
        rs_wait(n, 2 * OWN, 6)
        for h in range(2):
            total = chip_sum(n, h, OWN) + r1[n, h, 1] + r2[n, h]
            out_ref[:, h * HALF:(h + 1) * HALF] = total.astype(BF)

    def head_copy(src, dst, slot, where):
        return remote(src, dst, hd_s.at[0], hd_r.at[slot], where)

    wo_cps = [head_copy(wo.at[h, r:r + 64], wo_in.at[h, r:r + 64], h, (xn, yn)[h]) for r in (0, 64) for h in range(2)]
    ctx_cps = [head_copy(ctx.at[q], ctx_in.at[h, i], 2 + h, (xn, yn)[h])
               for h, qn in ((0, qx), (1, qy)) for i, q in ((0, qn), (1, qd))]

    def gate_table(k):
        tiles = grecv.at[0:1 if k == OWN else 2]
        remote(tiles, tiles, gs_sem.at[0], gr_sem.at[k], sib).wait_recv()
        q = chips[k]
        t0, t1 = grecv[2 * q], grecv[2 * q + 1]
        tile = jnp.concatenate([jnp.concatenate([t0[:, :ROWS], t1[:, :ROWS]], axis=1),
                                jnp.concatenate([t0[:, ROWS:], t1[:, ROWS:]], axis=1)], axis=0)
        gt[pl.ds(pl.multiple_of(q * 128, 128), 128), :] = jnp.concatenate([tile, jnp.zeros((120, 128), F32)], axis=0).T

    def pick(tile, e):
        lane = lax.broadcasted_iota(jnp.int32, tile.shape, 1)
        return jnp.sum(jnp.where(lane == e, tile, 0.0), axis=1, keepdims=True)

    def accumulate(n, q, val):
        for cc in range(2):
            for h in range(2):
                part[n, cc, h, q] += val[cc * 64:(cc + 1) * 64, h * HALF:(h + 1) * HALF]

    def experts(step, hooks):
        def body(e, carry):
            step(e)
            for at, fn in hooks.items():
                @pl.when(e == at)
                def _():
                    fn()
            return carry
        lax.fori_loop(0, EXP, body, 0)

    def chip_rows(k):
        return pl.ds(pl.multiple_of(chips[k] * 128, 128), 128)

    def forward(ks, load=False):
        def stack(ref, *at):
            return jnp.concatenate([ref[(*at, chip_rows(k), slice(None))] for k in ks], axis=0)

        def step(e):
            if load:
                pltpu.make_async_copy(wg_hbm.at[0:3], wg.at[0:3], w_sem.at[1 + e]).wait()

            def put(ref, val):
                for i, k in enumerate(ks):
                    ref[e, chip_rows(k), :] = val[i * 128:(i + 1) * 128]

            xs = stack(rows, XT)
            a = jnp.dot(xs, wg[e], preferred_element_type=F32)
            b = jnp.dot(xs, wu[e], preferred_element_type=F32)
            tile = stack(gt)
            mark = pick(tile, e + 4) > 0.5
            sg = jax.nn.sigmoid(a)
            ac = a * sg
            put(act, jnp.where(mark, ac, 0.0))
            put(gfac, jnp.where(mark, b * sg * (1.0 + a * (1.0 - sg)), 0.0))
            hh = jnp.where(mark, ac * b, 0.0).astype(BF)
            put(hid, hh)
            ob = jnp.dot(hh, wd[e], preferred_element_type=F32).astype(BF)
            put(osv, ob)
            yb = pick(tile, e) * ob.astype(F32)
            for i, k in enumerate(ks):
                accumulate(1, chips[k], yb[i * 128:(i + 1) * 128])
        return step

    def backward(qa, qb, base, gates):
        sl = pl.ds(pl.multiple_of(base, 256), 256)

        def step(e):
            g = pick(gt[sl, :], e)
            dyf = rows[DY, sl, :].astype(F32)
            do = (g * dyf).astype(BF)
            dh = lax.dot_general(do, wd[e], NT, preferred_element_type=F32).astype(BF).astype(F32)
            da = (dh * gfac[e, sl, :]).astype(BF)
            db = (dh * act[e, sl, :]).astype(BF)
            dag[e, sl, :] = da
            dbg[e, sl, :] = db
            if gates:
                lane = lax.broadcasted_iota(jnp.int32, (256, 128), 1)
                for r in (slice(0, 256), slice(256, 512)):
                    dg = jnp.sum(rows[DY, r, :].astype(F32) * osv[e, r, :].astype(F32), axis=1, keepdims=True)
                    dgs[r, :] += jnp.where(lane == e, dg, 0.0)
            dx = (lax.dot_general(da, wg[e], NT, preferred_element_type=F32)
                  + lax.dot_general(db, wu[e], NT, preferred_element_type=F32)).astype(BF).astype(F32)
            accumulate(2, qa, dx[0:128])
            accumulate(2, qb, dx[128:256])
        return step

    def attention_context():
        ag_rows(XA, 0, 4 * ROWS).wait_recv()
        causal_r = lax.broadcasted_iota(jnp.int32, (256, 128), 0) % 128
        causal_c = lax.broadcasted_iota(jnp.int32, (256, 128), 1)
        keep = (causal_r >= causal_c) & (causal_r // 64 == causal_c // 64)
        qkv = lax.dot_general(rows[XA], wqkv[...], NT, preferred_element_type=F32).astype(BF)
        qkvs = [qkv[q * 128:(q + 1) * 128] for q in range(4)]
        scs = [lax.dot_general(jnp.concatenate([v[:, 0:64], v[:, 64:128]], axis=0), v[:, 128:192], NT,
                               preferred_element_type=F32) * (64 ** -0.5) for v in qkvs]
        scs = [jnp.where(keep, sc, -1e30) for sc in scs]
        mxs = [jnp.max(sc, axis=1, keepdims=True) for sc in scs]
        exs = [jnp.exp(sc - mx) for sc, mx in zip(scs, mxs)]
        sms = [jnp.sum(ex, axis=1, keepdims=True) for ex in exs]
        prs = [(ex / sm).astype(BF) for ex, sm in zip(exs, sms)]
        ctxs = [jnp.dot(pr, v[:, 192:256], preferred_element_type=F32).astype(BF) for pr, v in zip(prs, qkvs)]
        for q, v in enumerate(ctxs):
            ctx[q] = jnp.concatenate([v[0:128], v[128:256]], axis=1)

    def attention_out():
        for h in range(2):
            head_copy(wo_in.at[h], wo_in.at[h], h, sib).wait_recv()
            both = ctx_in.at[h]
            head_copy(both, both, 2 + h, sib).wait_recv()
            for i, k in ((0, OWN), (1, second[h])):
                out = (jnp.dot(ctx[chips[k]], wo[h], preferred_element_type=F32)
                       + jnp.dot(ctx_in[h, i], wo_in[h], preferred_element_type=F32))
                for cc in range(2):
                    part[0, cc, h, chips[k]] = out[cc * 64:(cc + 1) * 64]
        for h in range(2):
            rsc[0][2 * OWN + h].start()
            rsc[0][2 * second[h] + h].start()

    def leave_attention():
        ref = pair.at[0, 0]
        remote(ref, ref, rs_s.at[0], rs_r.at[rs_slot(0, 2 * OWN)], sib).wait_recv()
        for h, dst in ((0, toy), (1, tox)):
            dst[:, D:D + HALF] = chip_sum(0, h, second[h])
            own_at[:, h * HALF:(h + 1) * HALF] = chip_sum(0, h, OWN)

    def leave_dx():
        n = 2
        rs_wait(n, 2 * OWN, 6)
        rs_wait(n, 8, 2)
        for h in range(2):
            cols = slice(h * HALF, (h + 1) * HALF)
            near = chip_sum(n, h, first[h])
            far = chip_sum(n, h, second[h]) + r1[n, h, 0]
            tox[:, cols] = near if h == 0 else far
            toy[:, cols] = far if h == 0 else near
            own_dx[:, cols] = chip_sum(n, h, OWN)

    pltpu.make_async_copy(x_hbm, rows.at[XT, own], in_sem.at[0]).wait()
    pl.semaphore_wait(barrier, len(rels))
    ag_own(XT)
    for cp in tables:
        cp.wait()

    exp_row = lax.broadcasted_iota(jnp.int32, (32, ROWS), 0)
    table = jnp.zeros((32, ROWS), F32)
    marks = jnp.zeros((32, ROWS), F32)
    for j in range(TOPK):
        hit = exp_row == idx_ref[j:j + 1, :]
        table = table + jnp.where(hit, gate_ref[j:j + 1, :], 0.0)
        marks = marks + jnp.where(hit, 1.0, 0.0)
    wide = jnp.concatenate([table, marks], axis=1)
    for d in range(8):
        gsend[d] = wide[d * EXP:(d + 1) * EXP, :]
    grecv[me] = gsend[me]
    for cp in gate_cps.values():
        cp.start()
    pltpu.make_async_copy(wg_hbm.at[0, 0:4 * ROWS], wg.at[0, 0:4 * ROWS], in_sem.at[3]).wait()
    ag_own(XA)
    dgs[...] = jnp.zeros((TOK, 128), F32)
    part[1] = jnp.zeros(part.shape[1:], F32)
    part[2] = jnp.zeros(part.shape[1:], F32)
    gate_table(OWN)
    ag[XT][0].wait_recv()
    experts(forward([OWN], True), {2: lambda: ag_forward(XT)})
    rs_pair(1, OWN)
    ag_pair(XT)
    gate_table(X)
    gate_table(Y)
    ag_own_a(DY)
    ag[XT][7].wait_recv()
    ag[XT][8].wait_recv()
    experts(forward([X, Y]), {0: lambda: (ag_forward(XA), ag_own_b(DY)), 1: lambda: ag_pair(XA), 2: lambda: ag_last(XT)})
    rs_pair(1, X)
    rs_pair(1, Y)
    gate_table(DI)
    ag_forward(DY)
    pltpu.make_async_copy(wg_hbm.at[0, 0:768], wg.at[0, 0:768], w_sem.at[0]).wait()
    for cp in wo_cps[:2]:
        cp.start()
    ag_rows(XT, 9, ROWS).wait_recv()
    experts(forward([DI]), {1: lambda: (rs_near(1, 0), rs_near(1, 1), ag_last(XA)), 2: lambda: ag_pair(DY)})
    rs_pair(1, DI)
    ag_last(DY)
    attention_context()
    rs_far(1)
    for cp in ctx_cps + wo_cps[2:]:
        cp.start()
    ag_rows(DY, 0, 4 * ROWS).wait_recv()
    dyall[...] = rows[DY]
    experts(backward(2 * (1 - y), 2 * (1 - y) + 1, (1 - y) * 256, True), {3: lambda: rs_second(1)})
    rs_pair(2, DI)
    rs_pair(2, Y)
    for q in range(4):
        dsend[q] = dgs[q * 128:(q + 1) * 128, :].T[0:EXP, :]
    drecv[me] = dsend[q0]
    for cp in dg_cps.values():
        cp.start()
    experts(backward(2 * y, 2 * y + 1, y * 256, False), {0: lambda: rs_far(2)})
    rs_pair(2, X)
    rs_pair(2, OWN)
    attention_out()
    rs_wait_dg = drecv.at[0:7]
    remote(rs_wait_dg, rs_wait_dg, gs_sem.at[0], dd_r.at[0], sib).wait_recv()
    both = jnp.concatenate([drecv[d] for d in range(8)], axis=0)
    mine = jnp.where(c == 0, both[:, 0:ROWS], both[:, ROWS:128])
    for j in range(TOPK):
        hit = exp_row == idx_ref[j:j + 1, :]
        dg_out[j:j + 1, :] = jnp.sum(jnp.where(hit, mine, 0.0), axis=0, keepdims=True)
    rs_final(1, y_out)
    leave_attention()
    xt[...] = rows[XT].T
    leave_dx()

    for ref, sem in ((rows.at[:, 0:7 * ROWS], ag_s), (act.at[:, 0:7 * ROWS], rs_s), (gt.at[0:56], gs_sem), (rows.at[:, 0:ROWS], hd_s)):
        remote(ref, ref, sem.at[0], gr_sem.at[0], sib).wait_send()


def exchange(x, dy, xa, idx, gates, wg, wu, wd, wq, wk, wv, wo):
    any_spec = pl.BlockSpec(memory_space=pl.ANY)
    vmem = pl.BlockSpec(memory_space=pltpu.VMEM)
    dma = pltpu.SemaphoreType.DMA
    return pl.pallas_call(
        exchange_kernel,
        name='exchange',
        out_shape=[pltpu.VMEM((ROWS, D), BF), pltpu.VMEM((TOPK, ROWS), F32)] + [pltpu.VMEM((ROWS, D + HALF), F32)] * 2 + [pltpu.VMEM((ROWS, D), F32)] * 2 + [pltpu.VMEM((D, TOK), BF), pltpu.VMEM((TOK, D), BF)]
        + [pltpu.VMEM((EXP, TOK, FF), BF)] * 3 + [pltpu.VMEM((TOK, 128), F32)],
        in_specs=[any_spec] * 12,
        out_specs=[vmem] * 12,
        scratch_shapes=[
            pltpu.VMEM((TOPK, ROWS), jnp.int32), pltpu.VMEM((TOPK, ROWS), F32),
            pltpu.VMEM((3, TOK, D), BF),
            pltpu.VMEM((EXP, D, FF), BF), pltpu.VMEM((EXP, D, FF), BF), pltpu.VMEM((EXP, FF, D), BF),
            pltpu.VMEM((256, D), BF), pltpu.VMEM((2, 128, HALF), BF), pltpu.VMEM((2, 128, HALF), BF),
            pltpu.VMEM((4, 128, 128), BF), pltpu.VMEM((2, 2, 128, 128), BF),
            pltpu.VMEM((EXP, TOK, D), BF),
            pltpu.VMEM((EXP, TOK, FF), F32), pltpu.VMEM((EXP, TOK, FF), F32),
            pltpu.VMEM((8, EXP, 128), F32), pltpu.VMEM((8, EXP, 128), F32),
            pltpu.VMEM((TOK, 128), F32), pltpu.VMEM((4, EXP, 128), F32), pltpu.VMEM((8, EXP, 128), F32),
            pltpu.VMEM((3, 2, 2, 4, ROWS, HALF), F32), pltpu.VMEM((3, 2, 4, ROWS, HALF), F32),
            pltpu.VMEM((3, 2, 2, ROWS, HALF), F32), pltpu.VMEM((3, 2, 2, ROWS, HALF), F32),
            pltpu.VMEM((3, 2, ROWS, HALF), F32), pltpu.VMEM((3, 2, ROWS, HALF), F32),
            dma((4,)), dma((1 + EXP,)), dma((1,)), dma((4,)),
            dma((1,)), dma((10,)), dma((1,)), dma((15,)), dma((1,)), dma((1,)), dma((4,)),
        ],
        compiler_params=pltpu.CompilerParams(collective_id=0, has_side_effects=True, vmem_limit_bytes=50 * 1024 * 1024),
    )(x, dy, xa, idx, gates, wg, wu, wd, wq, wk, wv, wo)


def grads_kernel(xt_ref, dy_ref, gt_ref, h_ref, da_ref, db_ref, y_in, dg_in, dwg_out, dwu_out, dwd_out, y_out, dg_out,
                 gate_buf, up_buf, down_buf, sem, small_sem):
    small = [pltpu.make_async_copy(y_in, y_out, small_sem.at[0]), pltpu.make_async_copy(dg_in, dg_out, small_sem.at[1])]
    for cp in small:
        cp.start()

    def leave(e, slot, n):
        buf, out = ((gate_buf, dwg_out), (up_buf, dwu_out), (down_buf, dwd_out))[n]
        return pltpu.make_async_copy(buf.at[slot], out.at[e], sem.at[n, slot])

    def body(e, carry):
        slot = e % 2

        @pl.when(e >= 2)
        def _():
            for n in range(3):
                leave(e - 2, slot, n).wait()
        gate_buf[slot] = jnp.dot(xt_ref[...], da_ref[e], preferred_element_type=F32)
        leave(e, slot, 0).start()
        up_buf[slot] = jnp.dot(xt_ref[...], db_ref[e], preferred_element_type=F32)
        leave(e, slot, 1).start()
        lane = lax.broadcasted_iota(jnp.int32, (TOK, 128), 1)
        g = jnp.sum(jnp.where(lane == e, gt_ref[...], 0.0), axis=1, keepdims=True)
        do = (g * dy_ref[...].astype(F32)).astype(BF)
        down_buf[slot] = lax.dot_general(h_ref[e], do, TN, preferred_element_type=F32)
        leave(e, slot, 2).start()
        return carry

    lax.fori_loop(0, EXP, body, 0)
    for e in (EXP - 2, EXP - 1):
        for n in range(3):
            leave(e, e % 2, n).wait()
    for cp in small:
        cp.wait()


def weight_grads(*args):
    sds = jax.ShapeDtypeStruct
    args = [pltpu.with_memory_space_constraint(v, pltpu.VMEM) for v in args]
    return pl.pallas_call(
        grads_kernel,
        name='weight_grads',
        out_shape=[sds((EXP, D, FF), F32), sds((EXP, D, FF), F32), sds((EXP, FF, D), F32),
                   sds((ROWS, D), BF), sds((TOPK, ROWS), F32)],
        in_specs=[pl.BlockSpec(memory_space=pltpu.VMEM)] * 8,
        out_specs=[pl.BlockSpec(memory_space=pl.ANY)] * 5,
        scratch_shapes=[pltpu.VMEM((2, D, FF), F32), pltpu.VMEM((2, D, FF), F32), pltpu.VMEM((2, FF, D), F32),
                        pltpu.SemaphoreType.DMA((3, 2)), pltpu.SemaphoreType.DMA((2,))],
        cost_estimate=pl.CostEstimate(flops=3 * 2 * EXP * TOK * D * FF, bytes_accessed=34 * 1024 * 1024, transcendentals=0),
        compiler_params=pltpu.CompilerParams(vmem_limit_bytes=40 * 1024 * 1024),
    )(*args)


def combine_kernel(dx_ref, at_ref, x_ref, y_ref, dx_out, at_out):
    dx_out[...] = (dx_ref[...] + x_ref[:, 0:D] + y_ref[:, 0:D]).astype(BF)
    at_out[:, 0:HALF] = (at_ref[:, 0:HALF] + y_ref[:, D:D + HALF]).astype(BF)
    at_out[:, HALF:D] = (at_ref[:, HALF:D] + x_ref[:, D:D + HALF]).astype(BF)


def combine(*args):
    sds = jax.ShapeDtypeStruct
    args = [pltpu.with_memory_space_constraint(v, pltpu.VMEM) for v in args]
    vmem = pl.BlockSpec(memory_space=pltpu.VMEM)
    return pl.pallas_call(combine_kernel, name='combine', out_shape=[sds((ROWS, D), BF)] * 2,
                          in_specs=[vmem] * 4, out_specs=[vmem] * 2)(*args)


def solution(mesh):
    def local_step(x_tokens, expert_idx, gate_vals, dy_tokens, w_gate, w_up, w_down, x_attn, w_query, w_key, w_value, w_out):
        y_p, dg_p, to_x, to_y, own_dx, own_at, xt, dyall, h, da, db, gt = exchange(
            x_tokens, dy_tokens, x_attn.reshape(ROWS, D), expert_idx.T, gate_vals.T, w_gate, w_up, w_down,
            w_query.transpose(1, 2, 0).reshape(128, D), w_key.transpose(1, 2, 0).reshape(64, D),
            w_value.transpose(1, 2, 0).reshape(64, D), w_out.reshape(128, D))
        from_x = lax.ppermute(to_x, GROUP_AXES, [(g, g ^ 2) for g in range(8)])
        from_y = lax.ppermute(to_y, GROUP_AXES, [(g, g ^ 4) for g in range(8)])
        dwg, dwu, dwd, y_t, dg = weight_grads(xt, dyall, gt, h, da, db, y_p, dg_p)
        dx_t, at = combine(own_dx, own_at, from_x, from_y)
        return y_t, dx_t, dg.T, dwg, dwu, dwd, at.reshape(1, ROWS, D)

    spec_rows = P(TOKEN_AXES, None)
    spec_seqs = P(TOKEN_AXES, None, None)
    spec_experts = P(GROUP_AXES, None, None)
    spec_heads = P(None, GROUP_AXES, None)
    return jax.shard_map(local_step, mesh=mesh,
                         in_specs=(spec_rows, spec_rows, spec_rows, spec_rows, spec_experts, spec_experts, spec_experts, spec_seqs, spec_heads, spec_heads, spec_heads, spec_experts),
                         out_specs=(spec_rows, spec_rows, spec_rows, spec_seqs, spec_seqs, spec_seqs, spec_seqs),
                         check_vma=False)
```

```python
import functools

import jax
import jax.numpy as jnp
from jax import lax
from jax.experimental import pallas as pl
from jax.experimental.pallas import tpu as pltpu
from jax.sharding import PartitionSpec as P

MESH = pl.DeviceIdType.MESH
GROUP_AXES = ('ei', 'eo')
TOKEN_AXES = ('dp', 'ei', 'eo')
BF = jnp.bfloat16
F32 = jnp.float32

ROWS = 64
TOK = 512
D = 1024
FF = 512
HALF = 512
EXP = 4
TOPK = 8
XA, XT, DY = 0, 1, 2

NT = (((1,), (1,)), ((), ()))
TN = (((0,), (0,)), ((), ()))


def exchange_kernel(x_hbm, dy_hbm, xa_hbm, idx_hbm, gate_hbm, wg_hbm, wu_hbm, wd_hbm, wq_hbm, wk_hbm, wv_hbm, wo_hbm,
                    y_out, dg_out, tox, toy, own_dx, own_at, xt, dyall, hid, dag, dbg, gt,
                    idx_ref, gate_ref, rows, wg, wu, wd, wqkv, wo, wo_in, ctx, ctx_in, osv, act, gfac, gsend, grecv,
                    dgs, dsend, drecv,
                    part, pair, s1, r1, s2, r2,
                    in_sem, w_sem, gs_sem, gr_sem, rs_s, rs_r, ag_s, ag_r, dd_r, hd_s, hd_r):
    y = lax.axis_index('ei')
    o = lax.axis_index('eo')
    z = lax.axis_index('dp')
    x = o // 2
    c = o % 2
    me = y * 4 + o
    q0 = 2 * y + x
    qx = 2 * y + (1 - x)
    qy = 2 * (1 - y) + x
    qd = 2 * (1 - y) + (1 - x)

    def dev(fx, fy, fc):
        xx = (1 - x) if fx else x
        yy = (1 - y) if fy else y
        cc = (1 - c) if fc else c
        return (z, yy, xx * 2 + cc)

    sib, xn, yn = dev(0, 0, 1), dev(1, 0, 0), dev(0, 1, 0)
    rels = [(fx, fy, fc) for fx in (0, 1) for fy in (0, 1) for fc in (0, 1) if fx or fy or fc]

    own = pl.ds(pl.multiple_of(me * ROWS, ROWS), ROWS)
    pltpu.make_async_copy(x_hbm, rows.at[XT, own], in_sem.at[0]).start()
    barrier = pltpu.get_barrier_semaphore()
    for rel in rels:
        pl.semaphore_signal(barrier, inc=1, device_id=dev(*rel), device_id_type=MESH)

    tables = [pltpu.make_async_copy(idx_hbm, idx_ref, in_sem.at[1]), pltpu.make_async_copy(gate_hbm, gate_ref, in_sem.at[2])]
    for cp in tables:
        cp.start()
    for t, src in ((DY, dy_hbm), (XA, xa_hbm)):
        pltpu.make_async_copy(src, rows.at[t, own], in_sem.at[3]).start()

    def expert_load(e):
        return [pltpu.make_async_copy(src.at[e], dst.at[e], w_sem.at[1 + e])
                for src, dst in ((wg_hbm, wg), (wu_hbm, wu), (wd_hbm, wd))]

    wload = [pltpu.make_async_copy(wq_hbm, wqkv.at[0:128], w_sem.at[0]),
             pltpu.make_async_copy(wk_hbm, wqkv.at[128:192], w_sem.at[0]),
             pltpu.make_async_copy(wv_hbm, wqkv.at[192:256], w_sem.at[0]),
             pltpu.make_async_copy(wo_hbm.at[:, 0:HALF], wo.at[0], w_sem.at[0]),
             pltpu.make_async_copy(wo_hbm.at[:, HALF:D], wo.at[1], w_sem.at[0])]

    def blk(t, q, off=0, n=ROWS):
        return rows.at[t, pl.ds(pl.multiple_of(q * 128 + c * ROWS + off, 32), n)]

    def remote(src, dst, ss, rs, where):
        return pltpu.make_async_remote_copy(src, dst, ss, rs, device_id=where, device_id_type=MESH)

    hr = ROWS // 2

    def gather_slot(t, k):
        if 1 <= k <= 6:
            return 3 * t + (0 if k in (1, 3) else 1 if k in (2, 4) else 2)
        return 9 + t if t != XT else {0: 12, 7: 13, 8: 14}.get(k, 10)

    def gather_copies(t):
        def cp(k, ref, where):
            return remote(ref, ref, ag_s.at[0], ag_r.at[gather_slot(t, k)], where)
        return [cp(0, blk(t, q0), sib),
                cp(1, blk(t, q0, 0, hr), xn), cp(2, blk(t, q0, hr, hr), xn),
                cp(3, blk(t, q0, hr, hr), yn), cp(4, blk(t, q0, 0, hr), yn),
                cp(5, blk(t, qx, 0, hr), yn), cp(6, blk(t, qy, hr, hr), xn),
                cp(7, blk(t, qx), sib), cp(8, blk(t, qy), sib),
                cp(9, blk(t, qd, 0, hr), sib), cp(10, blk(t, qd, hr, hr), sib)]

    ag = [gather_copies(t) for t in range(3)]

    def ag_own(t):
        for k in (1, 3, 2, 4, 0):
            ag[t][k].start()

    def ag_own_a(t):
        ag[t][1].start()
        ag[t][3].start()

    def ag_own_b(t):
        for k in (2, 4, 0):
            ag[t][k].start()

    def ag_forward(t):
        ag_rows(t, 1, ROWS).wait_recv()
        ag[t][5].start()
        ag[t][6].start()

    def ag_pair(t):
        ag_rows(t, 2, ROWS).wait_recv()
        ag[t][7].start()
        ag[t][8].start()

    def ag_last(t):
        ag_rows(t, 5, ROWS).wait_recv()
        ag[t][9].start()
        ag[t][10].start()

    def ag_rows(t, k, n):
        ref = rows.at[t, 0:n]
        return remote(ref, ref, ag_s.at[0], ag_r.at[gather_slot(t, k)], sib)

    def tile_copies(send, recv, ss, rs, chip_tiles):
        cps = {}
        for fx, fy, fc in rels:
            where = dev(fx, fy, fc)
            qq = 2 * where[1] + where[2] // 2
            src = send.at[qq] if chip_tiles else send.at[where[1] * 4 + where[2]]
            cps[fx, fy, fc] = remote(src, recv.at[me], ss.at[0], rs.at[0 if chip_tiles else fx + 2 * fy], where)
        return cps

    gate_cps = tile_copies(gsend, grecv, gs_sem, gr_sem, False)
    dg_cps = tile_copies(dsend, drecv, gs_sem, dd_r, True)
    chips = (q0, qx, qy, qd)
    OWN, X, Y, DI = 0, 1, 2, 3
    first = (X, Y)
    second = (Y, X)

    def rs_slot(n, k):
        if k >= 8:
            kind = (k - 8) % 3
            group = 2 if kind == 0 else 1
        else:
            group = 0 if k // 2 == DI else 1
            if n == 1 and k // 2 in (X, Y):
                group = 3 if k == 2 * X else 4 if k == 2 * Y + 1 else 5
        return (-1, 1, 7)[n] + group

    def rs_wait(n, k, count):
        ref = pair.at[n, 0, 0:2] if count == 2 else pair.at[n, :, 0:3] if count == 6 else pair.at[n, 0, 0]
        remote(ref, ref, rs_s.at[0], rs_r.at[rs_slot(n, k)], sib).wait_recv()

    def rs_copies(n):
        def cp(k, src, dst, where):
            return remote(src, dst, rs_s.at[0], rs_r.at[rs_slot(n, k)], where)
        cps = [cp(2 * k + h, part.at[n, 1 - c, h, chips[k]], pair.at[n, h, chips[k]], sib) for k in range(4) for h in range(2)]
        for h in range(2):
            one, two = (xn, yn) if h == 0 else (yn, xn)
            cps += [cp(8 + 3 * h, s1.at[n, h, 0], r1.at[n, h, 0], one), cp(9 + 3 * h, s1.at[n, h, 1], r1.at[n, h, 1], one),
                    cp(10 + 3 * h, s2.at[n, h], r2.at[n, h], two)]
        return cps

    rsc = [rs_copies(n) for n in range(3)]

    def rs_pair(n, k):
        rsc[n][2 * k].start()
        rsc[n][2 * k + 1].start()

    def chip_sum(n, h, k):
        return part[n, c, h, chips[k]] + pair[n, h, chips[k]]

    def rs_far(n):
        rs_wait(n, 2 * DI, 2)
        for h in range(2):
            s1[n, h, 0] = chip_sum(n, h, DI)
            rsc[n][8 + 3 * h].start()

    def rs_near(n, h):
        k = first[h]
        rs_wait(n, 2 * k + h, 1)
        s1[n, h, 1] = chip_sum(n, h, k)
        rsc[n][9 + 3 * h].start()

    def rs_second(n):
        rs_wait(n, 2 * Y, 2)
        rs_wait(n, 8, 2)
        for h in range(2):
            k = second[h]
            s2[n, h] = chip_sum(n, h, k) + r1[n, h, 0]
            rsc[n][10 + 3 * h].start()

    def rs_final(n, out_ref):
        rs_wait(n, 2 * OWN, 6)
        for h in range(2):
            total = chip_sum(n, h, OWN) + r1[n, h, 1] + r2[n, h]
            out_ref[:, h * HALF:(h + 1) * HALF] = total.astype(BF)

    def head_copy(src, dst, slot, where):
        return remote(src, dst, hd_s.at[0], hd_r.at[slot], where)

    wo_cps = [head_copy(wo.at[h, r:r + 64], wo_in.at[h, r:r + 64], h, (xn, yn)[h]) for r in (0, 64) for h in range(2)]
    ctx_cps = [head_copy(ctx.at[q], ctx_in.at[h, i], 2 + h, (xn, yn)[h])
               for h, qn in ((0, qx), (1, qy)) for i, q in ((0, qn), (1, qd))]

    def gate_table(k):
        tiles = grecv.at[0:1 if k == OWN else 2]
        remote(tiles, tiles, gs_sem.at[0], gr_sem.at[k], sib).wait_recv()
        q = chips[k]
        t0, t1 = grecv[2 * q], grecv[2 * q + 1]
        tile = jnp.concatenate([jnp.concatenate([t0[:, :ROWS], t1[:, :ROWS]], axis=1),
                                jnp.concatenate([t0[:, ROWS:], t1[:, ROWS:]], axis=1)], axis=0)
        gt[pl.ds(pl.multiple_of(q * 128, 128), 128), :] = jnp.concatenate([tile, jnp.zeros((120, 128), F32)], axis=0).T

    def pick(tile, e):
        lane = lax.broadcasted_iota(jnp.int32, tile.shape, 1)
        return jnp.sum(jnp.where(lane == e, tile, 0.0), axis=1, keepdims=True)

    def accumulate(n, q, val):
        for cc in range(2):
            for h in range(2):
                part[n, cc, h, q] += val[cc * 64:(cc + 1) * 64, h * HALF:(h + 1) * HALF]

    def experts(step, hooks):
        def body(e, carry):
            step(e)
            for at, fn in hooks.items():
                @pl.when(e == at)
                def _():
                    fn()
            return carry
        lax.fori_loop(0, EXP, body, 0)

    def chip_rows(k):
        return pl.ds(pl.multiple_of(chips[k] * 128, 128), 128)

    def forward(ks, load=False):
        def stack(ref, *at):
            return jnp.concatenate([ref[(*at, chip_rows(k), slice(None))] for k in ks], axis=0)

        def step(e):
            if load:
                pltpu.make_async_copy(wg_hbm.at[0:3], wg.at[0:3], w_sem.at[1 + e]).wait()

            def put(ref, val):
                for i, k in enumerate(ks):
                    ref[e, chip_rows(k), :] = val[i * 128:(i + 1) * 128]

            xs = stack(rows, XT)
            a = jnp.dot(xs, wg[e], preferred_element_type=F32)
            b = jnp.dot(xs, wu[e], preferred_element_type=F32)
            tile = stack(gt)
            mark = pick(tile, e + 4) > 0.5
            sg = jax.nn.sigmoid(a)
            ac = a * sg
            put(act, jnp.where(mark, ac, 0.0))
            put(gfac, jnp.where(mark, b * sg * (1.0 + a * (1.0 - sg)), 0.0))
            hh = jnp.where(mark, ac * b, 0.0).astype(BF)
            put(hid, hh)
            ob = jnp.dot(hh, wd[e], preferred_element_type=F32).astype(BF)
            put(osv, ob)
            yb = pick(tile, e) * ob.astype(F32)
            for i, k in enumerate(ks):
                accumulate(1, chips[k], yb[i * 128:(i + 1) * 128])
        return step

    def backward(qa, qb, base, gates):
        sl = pl.ds(pl.multiple_of(base, 256), 256)

        def step(e):
            g = pick(gt[sl, :], e)
            dyf = rows[DY, sl, :].astype(F32)
            do = (g * dyf).astype(BF)
            dh = lax.dot_general(do, wd[e], NT, preferred_element_type=F32).astype(BF).astype(F32)
            da = (dh * gfac[e, sl, :]).astype(BF)
            db = (dh * act[e, sl, :]).astype(BF)
            dag[e, sl, :] = da
            dbg[e, sl, :] = db
            if gates:
                lane = lax.broadcasted_iota(jnp.int32, (256, 128), 1)
                for r in (slice(0, 256), slice(256, 512)):
                    dg = jnp.sum(rows[DY, r, :].astype(F32) * osv[e, r, :].astype(F32), axis=1, keepdims=True)
                    dgs[r, :] += jnp.where(lane == e, dg, 0.0)
            dx = (lax.dot_general(da, wg[e], NT, preferred_element_type=F32)
                  + lax.dot_general(db, wu[e], NT, preferred_element_type=F32)).astype(BF).astype(F32)
            accumulate(2, qa, dx[0:128])
            accumulate(2, qb, dx[128:256])
        return step

    def attention_context():
        ag_rows(XA, 0, 4 * ROWS).wait_recv()
        causal_r = lax.broadcasted_iota(jnp.int32, (256, 128), 0) % 128
        causal_c = lax.broadcasted_iota(jnp.int32, (256, 128), 1)
        keep = (causal_r >= causal_c) & (causal_r // 64 == causal_c // 64)
        qkv = lax.dot_general(rows[XA], wqkv[...], NT, preferred_element_type=F32).astype(BF)
        qkvs = [qkv[q * 128:(q + 1) * 128] for q in range(4)]
        scs = [lax.dot_general(jnp.concatenate([v[:, 0:64], v[:, 64:128]], axis=0), v[:, 128:192], NT,
                               preferred_element_type=F32) * (64 ** -0.5) for v in qkvs]
        scs = [jnp.where(keep, sc, -1e30) for sc in scs]
        mxs = [jnp.max(sc, axis=1, keepdims=True) for sc in scs]
        exs = [jnp.exp(sc - mx) for sc, mx in zip(scs, mxs)]
        sms = [jnp.sum(ex, axis=1, keepdims=True) for ex in exs]
        prs = [(ex / sm).astype(BF) for ex, sm in zip(exs, sms)]
        ctxs = [jnp.dot(pr, v[:, 192:256], preferred_element_type=F32).astype(BF) for pr, v in zip(prs, qkvs)]
        for q, v in enumerate(ctxs):
            ctx[q] = jnp.concatenate([v[0:128], v[128:256]], axis=1)

    def attention_out():
        for h in range(2):
            head_copy(wo_in.at[h], wo_in.at[h], h, sib).wait_recv()
            both = ctx_in.at[h]
            head_copy(both, both, 2 + h, sib).wait_recv()
            for i, k in ((0, OWN), (1, second[h])):
                out = (jnp.dot(ctx[chips[k]], wo[h], preferred_element_type=F32)
                       + jnp.dot(ctx_in[h, i], wo_in[h], preferred_element_type=F32))
                for cc in range(2):
                    part[0, cc, h, chips[k]] = out[cc * 64:(cc + 1) * 64]
        for h in range(2):
            rsc[0][2 * OWN + h].start()
            rsc[0][2 * second[h] + h].start()

    def leave_attention():
        ref = pair.at[0, 0]
        remote(ref, ref, rs_s.at[0], rs_r.at[rs_slot(0, 2 * OWN)], sib).wait_recv()
        for h, dst in ((0, toy), (1, tox)):
            dst[:, D:D + HALF] = chip_sum(0, h, second[h])
            own_at[:, h * HALF:(h + 1) * HALF] = chip_sum(0, h, OWN)

    def leave_dx():
        n = 2
        rs_wait(n, 2 * OWN, 6)
        rs_wait(n, 8, 2)
        for h in range(2):
            cols = slice(h * HALF, (h + 1) * HALF)
            near = chip_sum(n, h, first[h])
            far = chip_sum(n, h, second[h]) + r1[n, h, 0]
            tox[:, cols] = near if h == 0 else far
            toy[:, cols] = far if h == 0 else near
            own_dx[:, cols] = chip_sum(n, h, OWN)

    pltpu.make_async_copy(x_hbm, rows.at[XT, own], in_sem.at[0]).wait()
    for e in range(EXP):
        for cp in expert_load(e):
            cp.start()
    for cp in wload:
        cp.start()
    pl.semaphore_wait(barrier, len(rels))
    ag_own(XT)
    for cp in tables:
        cp.wait()

    exp_row = lax.broadcasted_iota(jnp.int32, (32, ROWS), 0)
    table = jnp.zeros((32, ROWS), F32)
    marks = jnp.zeros((32, ROWS), F32)
    for j in range(TOPK):
        hit = exp_row == idx_ref[j:j + 1, :]
        table = table + jnp.where(hit, gate_ref[j:j + 1, :], 0.0)
        marks = marks + jnp.where(hit, 1.0, 0.0)
    wide = jnp.concatenate([table, marks], axis=1)
    for d in range(8):
        gsend[d] = wide[d * EXP:(d + 1) * EXP, :]
    grecv[me] = gsend[me]
    for cp in gate_cps.values():
        cp.start()
    pltpu.make_async_copy(wg_hbm.at[0, 0:4 * ROWS], wg.at[0, 0:4 * ROWS], in_sem.at[3]).wait()
    ag_own(XA)
    dgs[...] = jnp.zeros((TOK, 128), F32)
    part[1] = jnp.zeros(part.shape[1:], F32)
    part[2] = jnp.zeros(part.shape[1:], F32)
    gate_table(OWN)
    ag[XT][0].wait_recv()
    experts(forward([OWN], True), {2: lambda: ag_forward(XT)})
    rs_pair(1, OWN)
    ag_pair(XT)
    gate_table(X)
    gate_table(Y)
    ag_own_a(DY)
    ag[XT][7].wait_recv()
    ag[XT][8].wait_recv()
    experts(forward([X, Y]), {0: lambda: (ag_forward(XA), ag_own_b(DY)), 1: lambda: ag_pair(XA), 2: lambda: ag_last(XT)})
    rs_pair(1, X)
    rs_pair(1, Y)
    gate_table(DI)
    ag_forward(DY)
    pltpu.make_async_copy(wg_hbm.at[0, 0:768], wg.at[0, 0:768], w_sem.at[0]).wait()
    for cp in wo_cps[:2]:
        cp.start()
    ag_rows(XT, 9, ROWS).wait_recv()
    experts(forward([DI]), {1: lambda: (rs_near(1, 0), rs_near(1, 1), ag_last(XA)), 2: lambda: ag_pair(DY)})
    rs_pair(1, DI)
    ag_last(DY)
    attention_context()
    rs_far(1)
    for cp in ctx_cps + wo_cps[2:]:
        cp.start()
    ag_rows(DY, 0, 4 * ROWS).wait_recv()
    dyall[...] = rows[DY]
    experts(backward(2 * (1 - y), 2 * (1 - y) + 1, (1 - y) * 256, True), {3: lambda: rs_second(1)})
    rs_pair(2, DI)
    rs_pair(2, Y)
    for q in range(4):
        dsend[q] = dgs[q * 128:(q + 1) * 128, :].T[0:EXP, :]
    drecv[me] = dsend[q0]
    for cp in dg_cps.values():
        cp.start()
    experts(backward(2 * y, 2 * y + 1, y * 256, False), {0: lambda: rs_far(2)})
    rs_pair(2, X)
    rs_pair(2, OWN)
    attention_out()
    rs_wait_dg = drecv.at[0:7]
    remote(rs_wait_dg, rs_wait_dg, gs_sem.at[0], dd_r.at[0], sib).wait_recv()
    both = jnp.concatenate([drecv[d] for d in range(8)], axis=0)
    mine = jnp.where(c == 0, both[:, 0:ROWS], both[:, ROWS:128])
    for j in range(TOPK):
        hit = exp_row == idx_ref[j:j + 1, :]
        dg_out[j:j + 1, :] = jnp.sum(jnp.where(hit, mine, 0.0), axis=0, keepdims=True)
    rs_final(1, y_out)
    leave_attention()
    xt[...] = rows[XT].T
    leave_dx()

    for ref, sem in ((rows.at[:, 0:7 * ROWS], ag_s), (act.at[:, 0:7 * ROWS], rs_s), (gt.at[0:56], gs_sem), (rows.at[:, 0:ROWS], hd_s)):
        remote(ref, ref, sem.at[0], gr_sem.at[0], sib).wait_send()


def exchange(x, dy, xa, idx, gates, wg, wu, wd, wq, wk, wv, wo):
    any_spec = pl.BlockSpec(memory_space=pl.ANY)
    vmem = pl.BlockSpec(memory_space=pltpu.VMEM)
    dma = pltpu.SemaphoreType.DMA
    return pl.pallas_call(
        exchange_kernel,
        name='exchange',
        out_shape=[pltpu.VMEM((ROWS, D), BF), pltpu.VMEM((TOPK, ROWS), F32)] + [pltpu.VMEM((ROWS, D + HALF), F32)] * 2 + [pltpu.VMEM((ROWS, D), F32)] * 2 + [pltpu.VMEM((D, TOK), BF), pltpu.VMEM((TOK, D), BF)]
        + [pltpu.VMEM((EXP, TOK, FF), BF)] * 3 + [pltpu.VMEM((TOK, 128), F32)],
        in_specs=[any_spec] * 12,
        out_specs=[vmem] * 12,
        scratch_shapes=[
            pltpu.VMEM((TOPK, ROWS), jnp.int32), pltpu.VMEM((TOPK, ROWS), F32),
            pltpu.VMEM((3, TOK, D), BF),
            pltpu.VMEM((EXP, D, FF), BF), pltpu.VMEM((EXP, D, FF), BF), pltpu.VMEM((EXP, FF, D), BF),
            pltpu.VMEM((256, D), BF), pltpu.VMEM((2, 128, HALF), BF), pltpu.VMEM((2, 128, HALF), BF),
            pltpu.VMEM((4, 128, 128), BF), pltpu.VMEM((2, 2, 128, 128), BF),
            pltpu.VMEM((EXP, TOK, D), BF),
            pltpu.VMEM((EXP, TOK, FF), F32), pltpu.VMEM((EXP, TOK, FF), F32),
            pltpu.VMEM((8, EXP, 128), F32), pltpu.VMEM((8, EXP, 128), F32),
            pltpu.VMEM((TOK, 128), F32), pltpu.VMEM((4, EXP, 128), F32), pltpu.VMEM((8, EXP, 128), F32),
            pltpu.VMEM((3, 2, 2, 4, ROWS, HALF), F32), pltpu.VMEM((3, 2, 4, ROWS, HALF), F32),
            pltpu.VMEM((3, 2, 2, ROWS, HALF), F32), pltpu.VMEM((3, 2, 2, ROWS, HALF), F32),
            pltpu.VMEM((3, 2, ROWS, HALF), F32), pltpu.VMEM((3, 2, ROWS, HALF), F32),
            dma((4,)), dma((1 + EXP,)), dma((1,)), dma((4,)),
            dma((1,)), dma((10,)), dma((1,)), dma((15,)), dma((1,)), dma((1,)), dma((4,)),
        ],
        compiler_params=pltpu.CompilerParams(collective_id=0, has_side_effects=True, vmem_limit_bytes=50 * 1024 * 1024),
    )(x, dy, xa, idx, gates, wg, wu, wd, wq, wk, wv, wo)


def grads_kernel(xt_ref, dy_ref, gt_ref, h_ref, da_ref, db_ref, y_in, dg_in, dwg_out, dwu_out, dwd_out, y_out, dg_out,
                 gate_buf, up_buf, down_buf, sem, small_sem):
    small = [pltpu.make_async_copy(y_in, y_out, small_sem.at[0]), pltpu.make_async_copy(dg_in, dg_out, small_sem.at[1])]
    for cp in small:
        cp.start()

    def leave(e, slot, n):
        buf, out = ((gate_buf, dwg_out), (up_buf, dwu_out), (down_buf, dwd_out))[n]
        return pltpu.make_async_copy(buf.at[slot], out.at[e], sem.at[n, slot])

    def body(e, carry):
        slot = e % 2

        @pl.when(e >= 2)
        def _():
            for n in range(3):
                leave(e - 2, slot, n).wait()
        gate_buf[slot] = jnp.dot(xt_ref[...], da_ref[e], preferred_element_type=F32)
        leave(e, slot, 0).start()
        up_buf[slot] = jnp.dot(xt_ref[...], db_ref[e], preferred_element_type=F32)
        leave(e, slot, 1).start()
        lane = lax.broadcasted_iota(jnp.int32, (TOK, 128), 1)
        g = jnp.sum(jnp.where(lane == e, gt_ref[...], 0.0), axis=1, keepdims=True)
        do = (g * dy_ref[...].astype(F32)).astype(BF)
        down_buf[slot] = lax.dot_general(h_ref[e], do, TN, preferred_element_type=F32)
        leave(e, slot, 2).start()
        return carry

    lax.fori_loop(0, EXP, body, 0)
    for e in (EXP - 2, EXP - 1):
        for n in range(3):
            leave(e, e % 2, n).wait()
    for cp in small:
        cp.wait()


def weight_grads(*args):
    sds = jax.ShapeDtypeStruct
    args = [pltpu.with_memory_space_constraint(v, pltpu.VMEM) for v in args]
    return pl.pallas_call(
        grads_kernel,
        name='weight_grads',
        out_shape=[sds((EXP, D, FF), F32), sds((EXP, D, FF), F32), sds((EXP, FF, D), F32),
                   sds((ROWS, D), BF), sds((TOPK, ROWS), F32)],
        in_specs=[pl.BlockSpec(memory_space=pltpu.VMEM)] * 8,
        out_specs=[pl.BlockSpec(memory_space=pl.ANY)] * 5,
        scratch_shapes=[pltpu.VMEM((2, D, FF), F32), pltpu.VMEM((2, D, FF), F32), pltpu.VMEM((2, FF, D), F32),
                        pltpu.SemaphoreType.DMA((3, 2)), pltpu.SemaphoreType.DMA((2,))],
        cost_estimate=pl.CostEstimate(flops=3 * 2 * EXP * TOK * D * FF, bytes_accessed=34 * 1024 * 1024, transcendentals=0),
        compiler_params=pltpu.CompilerParams(vmem_limit_bytes=40 * 1024 * 1024),
    )(*args)


def combine_kernel(dx_ref, at_ref, x_ref, y_ref, dx_out, at_out):
    dx_out[...] = (dx_ref[...] + x_ref[:, 0:D] + y_ref[:, 0:D]).astype(BF)
    at_out[:, 0:HALF] = (at_ref[:, 0:HALF] + y_ref[:, D:D + HALF]).astype(BF)
    at_out[:, HALF:D] = (at_ref[:, HALF:D] + x_ref[:, D:D + HALF]).astype(BF)


def combine(*args):
    sds = jax.ShapeDtypeStruct
    args = [pltpu.with_memory_space_constraint(v, pltpu.VMEM) for v in args]
    vmem = pl.BlockSpec(memory_space=pltpu.VMEM)
    return pl.pallas_call(combine_kernel, name='combine', out_shape=[sds((ROWS, D), BF)] * 2,
                          in_specs=[vmem] * 4, out_specs=[vmem] * 2)(*args)


def solution(mesh):
    def local_step(x_tokens, expert_idx, gate_vals, dy_tokens, w_gate, w_up, w_down, x_attn, w_query, w_key, w_value, w_out):
        y_p, dg_p, to_x, to_y, own_dx, own_at, xt, dyall, h, da, db, gt = exchange(
            x_tokens, dy_tokens, x_attn.reshape(ROWS, D), expert_idx.T, gate_vals.T, w_gate, w_up, w_down,
            w_query.transpose(1, 2, 0).reshape(128, D), w_key.transpose(1, 2, 0).reshape(64, D),
            w_value.transpose(1, 2, 0).reshape(64, D), w_out.reshape(128, D))
        from_x = lax.ppermute(to_x, GROUP_AXES, [(g, g ^ 2) for g in range(8)])
        from_y = lax.ppermute(to_y, GROUP_AXES, [(g, g ^ 4) for g in range(8)])
        dwg, dwu, dwd, y_t, dg = weight_grads(xt, dyall, gt, h, da, db, y_p, dg_p)
        dx_t, at = combine(own_dx, own_at, from_x, from_y)
        return y_t, dx_t, dg.T, dwg, dwu, dwd, at.reshape(1, ROWS, D)

    spec_rows = P(TOKEN_AXES, None)
    spec_seqs = P(TOKEN_AXES, None, None)
    spec_experts = P(GROUP_AXES, None, None)
    spec_heads = P(None, GROUP_AXES, None)
    return jax.shard_map(local_step, mesh=mesh,
                         in_specs=(spec_rows, spec_rows, spec_rows, spec_rows, spec_experts, spec_experts, spec_experts, spec_seqs, spec_heads, spec_heads, spec_heads, spec_experts),
                         out_specs=(spec_rows, spec_rows, spec_rows, spec_seqs, spec_seqs, spec_seqs, spec_seqs),
                         check_vma=False)
```

```python
import functools

import jax
import jax.numpy as jnp
from jax import lax
from jax.experimental import pallas as pl
from jax.experimental.pallas import tpu as pltpu
from jax.sharding import PartitionSpec as P

MESH = pl.DeviceIdType.MESH
GROUP_AXES = ('ei', 'eo')
TOKEN_AXES = ('dp', 'ei', 'eo')
BF = jnp.bfloat16
F32 = jnp.float32

ROWS = 64
TOK = 512
D = 1024
FF = 512
HALF = 512
EXP = 4
TOPK = 8
XA, XT, DY = 0, 1, 2

NT = (((1,), (1,)), ((), ()))
TN = (((0,), (0,)), ((), ()))


def exchange_kernel(x_hbm, dy_hbm, xa_hbm, idx_hbm, gate_hbm, wg_hbm, wu_hbm, wd_hbm, wq_hbm, wk_hbm, wv_hbm, wo_hbm,
                    y_out, dg_out, tox, toy, own_dx, own_at, xt, dyall, hid, dag, dbg, gt,
                    idx_ref, gate_ref, rows, wg, wu, wd, wqkv, wo, wo_in, ctx, ctx_in, osv, act, gfac, gsend, grecv,
                    dgs, dsend, drecv,
                    part, pair, s1, r1, s2, r2,
                    in_sem, w_sem, gs_sem, gr_sem, rs_s, rs_r, ag_s, ag_r, dd_r, hd_s, hd_r):
    y = lax.axis_index('ei')
    o = lax.axis_index('eo')
    z = lax.axis_index('dp')
    x = o // 2
    c = o % 2
    me = y * 4 + o
    q0 = 2 * y + x
    qx = 2 * y + (1 - x)
    qy = 2 * (1 - y) + x
    qd = 2 * (1 - y) + (1 - x)

    def dev(fx, fy, fc):
        xx = (1 - x) if fx else x
        yy = (1 - y) if fy else y
        cc = (1 - c) if fc else c
        return (z, yy, xx * 2 + cc)

    sib, xn, yn = dev(0, 0, 1), dev(1, 0, 0), dev(0, 1, 0)
    rels = [(fx, fy, fc) for fx in (0, 1) for fy in (0, 1) for fc in (0, 1) if fx or fy or fc]

    own = pl.ds(pl.multiple_of(me * ROWS, ROWS), ROWS)
    pltpu.make_async_copy(x_hbm, rows.at[XT, own], in_sem.at[0]).start()
    barrier = pltpu.get_barrier_semaphore()
    for rel in rels:
        pl.semaphore_signal(barrier, inc=1, device_id=dev(*rel), device_id_type=MESH)

    tables = [pltpu.make_async_copy(idx_hbm, idx_ref, in_sem.at[1]), pltpu.make_async_copy(gate_hbm, gate_ref, in_sem.at[2])]
    for cp in tables:
        cp.start()
    for t, src in ((DY, dy_hbm), (XA, xa_hbm)):
        pltpu.make_async_copy(src, rows.at[t, own], in_sem.at[3]).start()

    def expert_load(e):
        return [pltpu.make_async_copy(src.at[e], dst.at[e], w_sem.at[1 + e])
                for src, dst in ((wg_hbm, wg), (wu_hbm, wu), (wd_hbm, wd))]

    wload = [pltpu.make_async_copy(wq_hbm, wqkv.at[0:128], w_sem.at[0]),
             pltpu.make_async_copy(wk_hbm, wqkv.at[128:192], w_sem.at[0]),
             pltpu.make_async_copy(wv_hbm, wqkv.at[192:256], w_sem.at[0]),
             pltpu.make_async_copy(wo_hbm.at[:, 0:HALF], wo.at[0], w_sem.at[0]),
             pltpu.make_async_copy(wo_hbm.at[:, HALF:D], wo.at[1], w_sem.at[0])]

    def blk(t, q, off=0, n=ROWS):
        return rows.at[t, pl.ds(pl.multiple_of(q * 128 + c * ROWS + off, 32), n)]

    def remote(src, dst, ss, rs, where):
        return pltpu.make_async_remote_copy(src, dst, ss, rs, device_id=where, device_id_type=MESH)

    hr = ROWS // 2

    def gather_slot(t, k):
        if 1 <= k <= 6:
            return 3 * t + (0 if k in (1, 3) else 1 if k in (2, 4) else 2)
        return 9 + t if t != XT else {0: 12, 7: 13, 8: 14}.get(k, 10)

    def gather_copies(t):
        def cp(k, ref, where):
            return remote(ref, ref, ag_s.at[0], ag_r.at[gather_slot(t, k)], where)
        return [cp(0, blk(t, q0), sib),
                cp(1, blk(t, q0, 0, hr), xn), cp(2, blk(t, q0, hr, hr), xn),
                cp(3, blk(t, q0, hr, hr), yn), cp(4, blk(t, q0, 0, hr), yn),
                cp(5, blk(t, qx, 0, hr), yn), cp(6, blk(t, qy, hr, hr), xn),
                cp(7, blk(t, qx), sib), cp(8, blk(t, qy), sib),
                cp(9, blk(t, qd, 0, hr), sib), cp(10, blk(t, qd, hr, hr), sib)]

    ag = [gather_copies(t) for t in range(3)]

    def ag_own(t):
        for k in (1, 3, 2, 4, 0):
            ag[t][k].start()

    def ag_own_a(t):
        ag[t][1].start()
        ag[t][3].start()

    def ag_own_b(t):
        for k in (2, 4, 0):
            ag[t][k].start()

    def ag_forward(t):
        ag_rows(t, 1, ROWS).wait_recv()
        ag[t][5].start()
        ag[t][6].start()

    def ag_pair(t):
        ag_rows(t, 2, ROWS).wait_recv()
        ag[t][7].start()
        ag[t][8].start()

    def ag_last(t):
        ag_rows(t, 5, ROWS).wait_recv()
        ag[t][9].start()
        ag[t][10].start()

    def ag_rows(t, k, n):
        ref = rows.at[t, 0:n]
        return remote(ref, ref, ag_s.at[0], ag_r.at[gather_slot(t, k)], sib)

    def tile_copies(send, recv, ss, rs, chip_tiles):
        cps = {}
        for fx, fy, fc in rels:
            where = dev(fx, fy, fc)
            qq = 2 * where[1] + where[2] // 2
            src = send.at[qq] if chip_tiles else send.at[where[1] * 4 + where[2]]
            cps[fx, fy, fc] = remote(src, recv.at[me], ss.at[0], rs.at[0 if chip_tiles else fx + 2 * fy], where)
        return cps

    gate_cps = tile_copies(gsend, grecv, gs_sem, gr_sem, False)
    dg_cps = tile_copies(dsend, drecv, gs_sem, dd_r, True)
    chips = (q0, qx, qy, qd)
    OWN, X, Y, DI = 0, 1, 2, 3
    first = (X, Y)
    second = (Y, X)

    def rs_slot(n, k):
        if k >= 8:
            kind = (k - 8) % 3
            group = 2 if kind == 0 else 1
        else:
            group = 0 if k // 2 == DI else 1
            if n == 1 and k // 2 in (X, Y):
                group = 3 if k == 2 * X else 4 if k == 2 * Y + 1 else 5
        return (-1, 1, 7)[n] + group

    def rs_wait(n, k, count):
        ref = pair.at[n, 0, 0:2] if count == 2 else pair.at[n, :, 0:3] if count == 6 else pair.at[n, 0, 0]
        remote(ref, ref, rs_s.at[0], rs_r.at[rs_slot(n, k)], sib).wait_recv()

    def rs_copies(n):
        def cp(k, src, dst, where):
            return remote(src, dst, rs_s.at[0], rs_r.at[rs_slot(n, k)], where)
        cps = [cp(2 * k + h, part.at[n, 1 - c, h, chips[k]], pair.at[n, h, chips[k]], sib) for k in range(4) for h in range(2)]
        for h in range(2):
            one, two = (xn, yn) if h == 0 else (yn, xn)
            cps += [cp(8 + 3 * h, s1.at[n, h, 0], r1.at[n, h, 0], one), cp(9 + 3 * h, s1.at[n, h, 1], r1.at[n, h, 1], one),
                    cp(10 + 3 * h, s2.at[n, h], r2.at[n, h], two)]
        return cps

    rsc = [rs_copies(n) for n in range(3)]

    def rs_pair(n, k):
        rsc[n][2 * k].start()
        rsc[n][2 * k + 1].start()

    def chip_sum(n, h, k):
        return part[n, c, h, chips[k]] + pair[n, h, chips[k]]

    def rs_far(n):
        rs_wait(n, 2 * DI, 2)
        for h in range(2):
            s1[n, h, 0] = chip_sum(n, h, DI)
            rsc[n][8 + 3 * h].start()

    def rs_near(n, h):
        k = first[h]
        rs_wait(n, 2 * k + h, 1)
        s1[n, h, 1] = chip_sum(n, h, k)
        rsc[n][9 + 3 * h].start()

    def rs_second(n):
        rs_wait(n, 2 * Y, 2)
        rs_wait(n, 8, 2)
        for h in range(2):
            k = second[h]
            s2[n, h] = chip_sum(n, h, k) + r1[n, h, 0]
            rsc[n][10 + 3 * h].start()

    def rs_final(n, out_ref):
        rs_wait(n, 2 * OWN, 6)
        for h in range(2):
            total = chip_sum(n, h, OWN) + r1[n, h, 1] + r2[n, h]
            out_ref[:, h * HALF:(h + 1) * HALF] = total.astype(BF)

    def head_copy(src, dst, slot, where):
        return remote(src, dst, hd_s.at[0], hd_r.at[slot], where)

    wo_cps = [head_copy(wo.at[h, r:r + 64], wo_in.at[h, r:r + 64], h, (xn, yn)[h]) for r in (0, 64) for h in range(2)]
    ctx_cps = [head_copy(ctx.at[q], ctx_in.at[h, i], 2 + h, (xn, yn)[h])
               for h, qn in ((0, qx), (1, qy)) for i, q in ((0, qn), (1, qd))]

    def gate_table(k):
        tiles = grecv.at[0:1 if k == OWN else 2]
        remote(tiles, tiles, gs_sem.at[0], gr_sem.at[k], sib).wait_recv()
        q = chips[k]
        t0, t1 = grecv[2 * q], grecv[2 * q + 1]
        tile = jnp.concatenate([jnp.concatenate([t0[:, :ROWS], t1[:, :ROWS]], axis=1),
                                jnp.concatenate([t0[:, ROWS:], t1[:, ROWS:]], axis=1)], axis=0)
        gt[pl.ds(pl.multiple_of(q * 128, 128), 128), :] = jnp.concatenate([tile, jnp.zeros((120, 128), F32)], axis=0).T

    def pick(tile, e):
        lane = lax.broadcasted_iota(jnp.int32, tile.shape, 1)
        return jnp.sum(jnp.where(lane == e, tile, 0.0), axis=1, keepdims=True)

    def accumulate(n, q, val):
        for cc in range(2):
            for h in range(2):
                part[n, cc, h, q] += val[cc * 64:(cc + 1) * 64, h * HALF:(h + 1) * HALF]

    def experts(step, hooks):
        def body(e, carry):
            step(e)
            for at, fn in hooks.items():
                @pl.when(e == at)
                def _():
                    fn()
            return carry
        lax.fori_loop(0, EXP, body, 0)

    def chip_rows(k):
        return pl.ds(pl.multiple_of(chips[k] * 128, 128), 128)

    def forward(ks, load=False):
        def stack(ref, *at):
            return jnp.concatenate([ref[(*at, chip_rows(k), slice(None))] for k in ks], axis=0)

        def step(e):
            if load:
                pltpu.make_async_copy(wg_hbm.at[0:3], wg.at[0:3], w_sem.at[1 + e]).wait()

            def put(ref, val):
                for i, k in enumerate(ks):
                    ref[e, chip_rows(k), :] = val[i * 128:(i + 1) * 128]

            xs = stack(rows, XT)
            a = jnp.dot(xs, wg[e], preferred_element_type=F32)
            b = jnp.dot(xs, wu[e], preferred_element_type=F32)
            tile = stack(gt)
            mark = pick(tile, e + 4) > 0.5
            sg = jax.nn.sigmoid(a)
            ac = a * sg
            put(act, jnp.where(mark, ac, 0.0))
            put(gfac, jnp.where(mark, b * sg * (1.0 + a * (1.0 - sg)), 0.0))
            hh = jnp.where(mark, ac * b, 0.0).astype(BF)
            put(hid, hh)
            ob = jnp.dot(hh, wd[e], preferred_element_type=F32).astype(BF)
            put(osv, ob)
            yb = pick(tile, e) * ob.astype(F32)
            for i, k in enumerate(ks):
                accumulate(1, chips[k], yb[i * 128:(i + 1) * 128])
        return step

    def backward(qa, qb, base, gates):
        sl = pl.ds(pl.multiple_of(base, 256), 256)

        def step(e):
            g = pick(gt[sl, :], e)
            dyf = rows[DY, sl, :].astype(F32)
            do = (g * dyf).astype(BF)
            dh = lax.dot_general(do, wd[e], NT, preferred_element_type=F32).astype(BF).astype(F32)
            da = (dh * gfac[e, sl, :]).astype(BF)
            db = (dh * act[e, sl, :]).astype(BF)
            dag[e, sl, :] = da
            dbg[e, sl, :] = db
            if gates:
                lane = lax.broadcasted_iota(jnp.int32, (256, 128), 1)
                for r in (slice(0, 256), slice(256, 512)):
                    dg = jnp.sum(rows[DY, r, :].astype(F32) * osv[e, r, :].astype(F32), axis=1, keepdims=True)
                    dgs[r, :] += jnp.where(lane == e, dg, 0.0)
            dx = (lax.dot_general(da, wg[e], NT, preferred_element_type=F32)
                  + lax.dot_general(db, wu[e], NT, preferred_element_type=F32)).astype(BF).astype(F32)
            accumulate(2, qa, dx[0:128])
            accumulate(2, qb, dx[128:256])
        return step

    def attention_context():
        ag_rows(XA, 0, 4 * ROWS).wait_recv()
        causal_r = lax.broadcasted_iota(jnp.int32, (256, 128), 0) % 128
        causal_c = lax.broadcasted_iota(jnp.int32, (256, 128), 1)
        keep = (causal_r >= causal_c) & (causal_r // 64 == causal_c // 64)
        qkv = lax.dot_general(rows[XA], wqkv[...], NT, preferred_element_type=F32).astype(BF)
        qkvs = [qkv[q * 128:(q + 1) * 128] for q in range(4)]
        scs = [lax.dot_general(jnp.concatenate([v[:, 0:64], v[:, 64:128]], axis=0), v[:, 128:192], NT,
                               preferred_element_type=F32) * (64 ** -0.5) for v in qkvs]
        scs = [jnp.where(keep, sc, -1e30) for sc in scs]
        mxs = [jnp.max(sc, axis=1, keepdims=True) for sc in scs]
        exs = [jnp.exp(sc - mx) for sc, mx in zip(scs, mxs)]
        sms = [jnp.sum(ex, axis=1, keepdims=True) for ex in exs]
        prs = [(ex / sm).astype(BF) for ex, sm in zip(exs, sms)]
        ctxs = [jnp.dot(pr, v[:, 192:256], preferred_element_type=F32).astype(BF) for pr, v in zip(prs, qkvs)]
        for q, v in enumerate(ctxs):
            ctx[q] = jnp.concatenate([v[0:128], v[128:256]], axis=1)

    def attention_out():
        for h in range(2):
            head_copy(wo_in.at[h], wo_in.at[h], h, sib).wait_recv()
            both = ctx_in.at[h]
            head_copy(both, both, 2 + h, sib).wait_recv()
            for i, k in ((0, OWN), (1, second[h])):
                out = (jnp.dot(ctx[chips[k]], wo[h], preferred_element_type=F32)
                       + jnp.dot(ctx_in[h, i], wo_in[h], preferred_element_type=F32))
                for cc in range(2):
                    part[0, cc, h, chips[k]] = out[cc * 64:(cc + 1) * 64]
        for h in range(2):
            rsc[0][2 * OWN + h].start()
            rsc[0][2 * second[h] + h].start()

    def leave_attention():
        ref = pair.at[0, 0]
        remote(ref, ref, rs_s.at[0], rs_r.at[rs_slot(0, 2 * OWN)], sib).wait_recv()
        for h, dst in ((0, toy), (1, tox)):
            dst[:, D:D + HALF] = chip_sum(0, h, second[h])
            own_at[:, h * HALF:(h + 1) * HALF] = chip_sum(0, h, OWN)

    def leave_dx():
        n = 2
        rs_wait(n, 2 * OWN, 6)
        rs_wait(n, 8, 2)
        for h in range(2):
            cols = slice(h * HALF, (h + 1) * HALF)
            near = chip_sum(n, h, first[h])
            far = chip_sum(n, h, second[h]) + r1[n, h, 0]
            tox[:, cols] = near if h == 0 else far
            toy[:, cols] = far if h == 0 else near
            own_dx[:, cols] = chip_sum(n, h, OWN)

    pltpu.make_async_copy(x_hbm, rows.at[XT, own], in_sem.at[0]).wait()
    for e in range(EXP):
        for cp in expert_load(e):
            cp.start()
    for cp in wload:
        cp.start()
    pl.semaphore_wait(barrier, len(rels))
    ag_own(XT)
    for cp in tables:
        cp.wait()

    exp_row = lax.broadcasted_iota(jnp.int32, (32, ROWS), 0)
    table = jnp.zeros((32, ROWS), F32)
    marks = jnp.zeros((32, ROWS), F32)
    for j in range(TOPK):
        hit = exp_row == idx_ref[j:j + 1, :]
        table = table + jnp.where(hit, gate_ref[j:j + 1, :], 0.0)
        marks = marks + jnp.where(hit, 1.0, 0.0)
    wide = jnp.concatenate([table, marks], axis=1)
    for d in range(8):
        gsend[d] = wide[d * EXP:(d + 1) * EXP, :]
    grecv[me] = gsend[me]
    for cp in gate_cps.values():
        cp.start()
    pltpu.make_async_copy(wg_hbm.at[0, 0:4 * ROWS], wg.at[0, 0:4 * ROWS], in_sem.at[3]).wait()
    ag_own(XA)
    dgs[...] = jnp.zeros((TOK, 128), F32)
    part[1] = jnp.zeros(part.shape[1:], F32)
    part[2] = jnp.zeros(part.shape[1:], F32)
    gate_table(OWN)
    ag[XT][0].wait_recv()
    experts(forward([OWN], True), {2: lambda: ag_forward(XT)})
    rs_pair(1, OWN)
    ag_pair(XT)
    gate_table(X)
    gate_table(Y)
    ag_own_a(DY)
    ag[XT][7].wait_recv()
    ag[XT][8].wait_recv()
    experts(forward([X, Y]), {0: lambda: (ag_forward(XA), ag_own_b(DY)), 1: lambda: ag_pair(XA), 2: lambda: ag_last(XT)})
    rs_pair(1, X)
    rs_pair(1, Y)
    gate_table(DI)
    ag_forward(DY)
    pltpu.make_async_copy(wg_hbm.at[0, 0:768], wg.at[0, 0:768], w_sem.at[0]).wait()
    for cp in wo_cps[:2]:
        cp.start()
    ag_rows(XT, 9, ROWS).wait_recv()
    experts(forward([DI]), {1: lambda: (rs_near(1, 0), rs_near(1, 1), ag_last(XA)), 2: lambda: ag_pair(DY)})
    rs_pair(1, DI)
    ag_last(DY)
    attention_context()
    rs_far(1)
    for cp in ctx_cps + wo_cps[2:]:
        cp.start()
    ag_rows(DY, 0, 4 * ROWS).wait_recv()
    dyall[...] = rows[DY]
    experts(backward(2 * (1 - y), 2 * (1 - y) + 1, (1 - y) * 256, True), {3: lambda: rs_second(1)})
    rs_pair(2, DI)
    rs_pair(2, Y)
    for q in range(4):
        dsend[q] = dgs[q * 128:(q + 1) * 128, :].T[0:EXP, :]
    drecv[me] = dsend[q0]
    for cp in dg_cps.values():
        cp.start()
    experts(backward(2 * y, 2 * y + 1, y * 256, False), {0: lambda: rs_far(2)})
    rs_pair(2, X)
    rs_pair(2, OWN)
    attention_out()
    rs_wait_dg = drecv.at[0:7]
    remote(rs_wait_dg, rs_wait_dg, gs_sem.at[0], dd_r.at[0], sib).wait_recv()
    both = jnp.concatenate([drecv[d] for d in range(8)], axis=0)
    mine = jnp.where(c == 0, both[:, 0:ROWS], both[:, ROWS:128])
    for j in range(TOPK):
        hit = exp_row == idx_ref[j:j + 1, :]
        dg_out[j:j + 1, :] = jnp.sum(jnp.where(hit, mine, 0.0), axis=0, keepdims=True)
    rs_final(1, y_out)
    leave_attention()
    xt[...] = rows[XT].T
    leave_dx()

    for ref, sem in ((rows.at[:, 0:7 * ROWS], ag_s), (act.at[:, 0:7 * ROWS], rs_s), (gt.at[0:56], gs_sem), (rows.at[:, 0:ROWS], hd_s)):
        remote(ref, ref, sem.at[0], gr_sem.at[0], sib).wait_send()


def exchange(x, dy, xa, idx, gates, wg, wu, wd, wq, wk, wv, wo):
    any_spec = pl.BlockSpec(memory_space=pl.ANY)
    vmem = pl.BlockSpec(memory_space=pltpu.VMEM)
    dma = pltpu.SemaphoreType.DMA
    return pl.pallas_call(
        exchange_kernel,
        name='exchange',
        out_shape=[pltpu.VMEM((ROWS, D), BF), pltpu.VMEM((TOPK, ROWS), F32)] + [pltpu.VMEM((ROWS, D + HALF), F32)] * 2 + [pltpu.VMEM((ROWS, D), F32)] * 2 + [pltpu.VMEM((D, TOK), BF), pltpu.VMEM((TOK, D), BF)]
        + [pltpu.VMEM((EXP, TOK, FF), BF)] * 3 + [pltpu.VMEM((TOK, 128), F32)],
        in_specs=[any_spec] * 12,
        out_specs=[vmem] * 12,
        scratch_shapes=[
            pltpu.VMEM((TOPK, ROWS), jnp.int32), pltpu.VMEM((TOPK, ROWS), F32),
            pltpu.VMEM((3, TOK, D), BF),
            pltpu.VMEM((EXP, D, FF), BF), pltpu.VMEM((EXP, D, FF), BF), pltpu.VMEM((EXP, FF, D), BF),
            pltpu.VMEM((256, D), BF), pltpu.VMEM((2, 128, HALF), BF), pltpu.VMEM((2, 128, HALF), BF),
            pltpu.VMEM((4, 128, 128), BF), pltpu.VMEM((2, 2, 128, 128), BF),
            pltpu.VMEM((EXP, TOK, D), BF),
            pltpu.VMEM((EXP, TOK, FF), F32), pltpu.VMEM((EXP, TOK, FF), F32),
            pltpu.VMEM((8, EXP, 128), F32), pltpu.VMEM((8, EXP, 128), F32),
            pltpu.VMEM((TOK, 128), F32), pltpu.VMEM((4, EXP, 128), F32), pltpu.VMEM((8, EXP, 128), F32),
            pltpu.VMEM((3, 2, 2, 4, ROWS, HALF), F32), pltpu.VMEM((3, 2, 4, ROWS, HALF), F32),
            pltpu.VMEM((3, 2, 2, ROWS, HALF), F32), pltpu.VMEM((3, 2, 2, ROWS, HALF), F32),
            pltpu.VMEM((3, 2, ROWS, HALF), F32), pltpu.VMEM((3, 2, ROWS, HALF), F32),
            dma((4,)), dma((1 + EXP,)), dma((1,)), dma((4,)),
            dma((1,)), dma((10,)), dma((1,)), dma((15,)), dma((1,)), dma((1,)), dma((4,)),
        ],
        compiler_params=pltpu.CompilerParams(collective_id=0, has_side_effects=True, vmem_limit_bytes=50 * 1024 * 1024),
    )(x, dy, xa, idx, gates, wg, wu, wd, wq, wk, wv, wo)


def grads_kernel(xt_ref, dy_ref, gt_ref, h_ref, da_ref, db_ref, y_in, dg_in, dwg_out, dwu_out, dwd_out, y_out, dg_out,
                 gate_buf, up_buf, down_buf, sem, small_sem):
    small = [pltpu.make_async_copy(y_in, y_out, small_sem.at[0]), pltpu.make_async_copy(dg_in, dg_out, small_sem.at[1])]
    for cp in small:
        cp.start()

    def leave(e, slot, n):
        buf, out = ((gate_buf, dwg_out), (up_buf, dwu_out), (down_buf, dwd_out))[n]
        return pltpu.make_async_copy(buf.at[slot], out.at[e], sem.at[n, slot])

    def body(e, carry):
        slot = e % 2

        @pl.when(e >= 2)
        def _():
            for n in range(3):
                leave(e - 2, slot, n).wait()
        gate_buf[slot] = jnp.dot(xt_ref[...], da_ref[e], preferred_element_type=F32)
        leave(e, slot, 0).start()
        up_buf[slot] = jnp.dot(xt_ref[...], db_ref[e], preferred_element_type=F32)
        leave(e, slot, 1).start()
        lane = lax.broadcasted_iota(jnp.int32, (TOK, 128), 1)
        g = jnp.sum(jnp.where(lane == e, gt_ref[...], 0.0), axis=1, keepdims=True)
        do = (g * dy_ref[...].astype(F32)).astype(BF)
        down_buf[slot] = lax.dot_general(h_ref[e], do, TN, preferred_element_type=F32)
        leave(e, slot, 2).start()
        return carry

    lax.fori_loop(0, EXP, body, 0)
    for e in (EXP - 2, EXP - 1):
        for n in range(3):
            leave(e, e % 2, n).wait()
    for cp in small:
        cp.wait()


def weight_grads(*args):
    sds = jax.ShapeDtypeStruct
    args = [pltpu.with_memory_space_constraint(v, pltpu.VMEM) for v in args]
    return pl.pallas_call(
        grads_kernel,
        name='weight_grads',
        out_shape=[sds((EXP, D, FF), F32), sds((EXP, D, FF), F32), sds((EXP, FF, D), F32),
                   sds((ROWS, D), BF), sds((TOPK, ROWS), F32)],
        in_specs=[pl.BlockSpec(memory_space=pltpu.VMEM)] * 8,
        out_specs=[pl.BlockSpec(memory_space=pl.ANY)] * 5,
        scratch_shapes=[pltpu.VMEM((2, D, FF), F32), pltpu.VMEM((2, D, FF), F32), pltpu.VMEM((2, FF, D), F32),
                        pltpu.SemaphoreType.DMA((3, 2)), pltpu.SemaphoreType.DMA((2,))],
        cost_estimate=pl.CostEstimate(flops=3 * 2 * EXP * TOK * D * FF, bytes_accessed=34 * 1024 * 1024, transcendentals=0),
        compiler_params=pltpu.CompilerParams(vmem_limit_bytes=40 * 1024 * 1024),
    )(*args)


def combine_kernel(dx_ref, at_ref, x_ref, y_ref, dx_out, at_out, dx_buf, at_buf, sem):
    dx_cp = pltpu.make_async_copy(dx_buf, dx_out, sem.at[0])
    at_cp = pltpu.make_async_copy(at_buf, at_out, sem.at[1])
    dx_buf[...] = (dx_ref[...] + x_ref[:, 0:D] + y_ref[:, 0:D]).astype(BF)
    dx_cp.start()
    at_buf[:, 0:HALF] = (at_ref[:, 0:HALF] + y_ref[:, D:D + HALF]).astype(BF)
    at_buf[:, HALF:D] = (at_ref[:, HALF:D] + x_ref[:, D:D + HALF]).astype(BF)
    at_cp.start()
    dx_cp.wait()
    at_cp.wait()


def combine(*args):
    sds = jax.ShapeDtypeStruct
    args = [pltpu.with_memory_space_constraint(v, pltpu.VMEM) for v in args]
    return pl.pallas_call(combine_kernel, name='combine', out_shape=[sds((ROWS, D), BF)] * 2,
                          in_specs=[pl.BlockSpec(memory_space=pltpu.VMEM)] * 4,
                          out_specs=[pl.BlockSpec(memory_space=pl.ANY)] * 2,
                          scratch_shapes=[pltpu.VMEM((ROWS, D), BF), pltpu.VMEM((ROWS, D), BF), pltpu.SemaphoreType.DMA((2,))])(*args)


def solution(mesh):
    def local_step(x_tokens, expert_idx, gate_vals, dy_tokens, w_gate, w_up, w_down, x_attn, w_query, w_key, w_value, w_out):
        y_p, dg_p, to_x, to_y, own_dx, own_at, xt, dyall, h, da, db, gt = exchange(
            x_tokens, dy_tokens, x_attn.reshape(ROWS, D), expert_idx.T, gate_vals.T, w_gate, w_up, w_down,
            w_query.transpose(1, 2, 0).reshape(128, D), w_key.transpose(1, 2, 0).reshape(64, D),
            w_value.transpose(1, 2, 0).reshape(64, D), w_out.reshape(128, D))
        from_x = lax.ppermute(to_x, GROUP_AXES, [(g, g ^ 2) for g in range(8)])
        from_y = lax.ppermute(to_y, GROUP_AXES, [(g, g ^ 4) for g in range(8)])
        dwg, dwu, dwd, y_t, dg = weight_grads(xt, dyall, gt, h, da, db, y_p, dg_p)
        dx_t, at = combine(own_dx, own_at, from_x, from_y)
        return y_t, dx_t, dg.T, dwg, dwu, dwd, at.reshape(1, ROWS, D)

    spec_rows = P(TOKEN_AXES, None)
    spec_seqs = P(TOKEN_AXES, None, None)
    spec_experts = P(GROUP_AXES, None, None)
    spec_heads = P(None, GROUP_AXES, None)
    return jax.shard_map(local_step, mesh=mesh,
                         in_specs=(spec_rows, spec_rows, spec_rows, spec_rows, spec_experts, spec_experts, spec_experts, spec_seqs, spec_heads, spec_heads, spec_heads, spec_experts),
                         out_specs=(spec_rows, spec_rows, spec_rows, spec_seqs, spec_seqs, spec_seqs, spec_seqs),
                         check_vma=False)
```

```python
import functools

import jax
import jax.numpy as jnp
from jax import lax
from jax.experimental import pallas as pl
from jax.experimental.pallas import tpu as pltpu
from jax.sharding import PartitionSpec as P

MESH = pl.DeviceIdType.MESH
GROUP_AXES = ('ei', 'eo')
TOKEN_AXES = ('dp', 'ei', 'eo')
BF = jnp.bfloat16
F32 = jnp.float32

ROWS = 64
TOK = 512
D = 1024
FF = 512
HALF = 512
EXP = 4
TOPK = 8
XA, XT, DY = 0, 1, 2

NT = (((1,), (1,)), ((), ()))
TN = (((0,), (0,)), ((), ()))


def exchange_kernel(x_hbm, dy_hbm, xa_hbm, idx_hbm, gate_hbm, wg_hbm, wu_hbm, wd_hbm, wq_hbm, wk_hbm, wv_hbm, wo_hbm,
                    y_out, dg_out, tox, toy, own_dx, own_at, xt, dyall, hid, dag, dbg, gt,
                    idx_ref, gate_ref, rows, wg, wu, wd, wqkv, wo, wo_in, ctx, ctx_in, osv, act, gfac, gsend, grecv,
                    dgs, dsend, drecv,
                    part, pair, s1, r1, s2, r2,
                    in_sem, w_sem, gs_sem, gr_sem, rs_s, rs_r, ag_s, ag_r, dd_r, hd_s, hd_r):
    y = lax.axis_index('ei')
    o = lax.axis_index('eo')
    z = lax.axis_index('dp')
    x = o // 2
    c = o % 2
    me = y * 4 + o
    q0 = 2 * y + x
    qx = 2 * y + (1 - x)
    qy = 2 * (1 - y) + x
    qd = 2 * (1 - y) + (1 - x)

    def dev(fx, fy, fc):
        xx = (1 - x) if fx else x
        yy = (1 - y) if fy else y
        cc = (1 - c) if fc else c
        return (z, yy, xx * 2 + cc)

    sib, xn, yn = dev(0, 0, 1), dev(1, 0, 0), dev(0, 1, 0)
    rels = [(fx, fy, fc) for fx in (0, 1) for fy in (0, 1) for fc in (0, 1) if fx or fy or fc]

    own = pl.ds(pl.multiple_of(me * ROWS, ROWS), ROWS)
    pltpu.make_async_copy(x_hbm, rows.at[XT, own], in_sem.at[0]).start()
    barrier = pltpu.get_barrier_semaphore()
    for rel in rels:
        pl.semaphore_signal(barrier, inc=1, device_id=dev(*rel), device_id_type=MESH)

    tables = [pltpu.make_async_copy(idx_hbm, idx_ref, in_sem.at[1]), pltpu.make_async_copy(gate_hbm, gate_ref, in_sem.at[2])]
    for cp in tables:
        cp.start()
    for t, src in ((DY, dy_hbm), (XA, xa_hbm)):
        pltpu.make_async_copy(src, rows.at[t, own], in_sem.at[3]).start()

    def expert_load(e):
        return [pltpu.make_async_copy(src.at[e], dst.at[e], w_sem.at[1 + e])
                for src, dst in ((wg_hbm, wg), (wu_hbm, wu), (wd_hbm, wd))]

    wload = [pltpu.make_async_copy(wq_hbm, wqkv.at[0:128], w_sem.at[0]),
             pltpu.make_async_copy(wk_hbm, wqkv.at[128:192], w_sem.at[0]),
             pltpu.make_async_copy(wv_hbm, wqkv.at[192:256], w_sem.at[0]),
             pltpu.make_async_copy(wo_hbm.at[:, 0:HALF], wo.at[0], w_sem.at[0]),
             pltpu.make_async_copy(wo_hbm.at[:, HALF:D], wo.at[1], w_sem.at[0])]

    def blk(t, q, off=0, n=ROWS):
        return rows.at[t, pl.ds(pl.multiple_of(q * 128 + c * ROWS + off, 32), n)]

    def remote(src, dst, ss, rs, where):
        return pltpu.make_async_remote_copy(src, dst, ss, rs, device_id=where, device_id_type=MESH)

    hr = ROWS // 2

    def gather_slot(t, k):
        if 1 <= k <= 6:
            return 3 * t + (0 if k in (1, 3) else 1 if k in (2, 4) else 2)
        return 9 + t if t != XT else {0: 12, 7: 13, 8: 14}.get(k, 10)

    def gather_copies(t):
        def cp(k, ref, where):
            return remote(ref, ref, ag_s.at[0], ag_r.at[gather_slot(t, k)], where)
        return [cp(0, blk(t, q0), sib),
                cp(1, blk(t, q0, 0, hr), xn), cp(2, blk(t, q0, hr, hr), xn),
                cp(3, blk(t, q0, hr, hr), yn), cp(4, blk(t, q0, 0, hr), yn),
                cp(5, blk(t, qx, 0, hr), yn), cp(6, blk(t, qy, hr, hr), xn),
                cp(7, blk(t, qx), sib), cp(8, blk(t, qy), sib),
                cp(9, blk(t, qd, 0, hr), sib), cp(10, blk(t, qd, hr, hr), sib)]

    ag = [gather_copies(t) for t in range(3)]

    def ag_own(t):
        for k in (1, 3, 2, 4, 0):
            ag[t][k].start()

    def ag_own_a(t):
        ag[t][1].start()
        ag[t][3].start()

    def ag_own_b(t):
        for k in (2, 4, 0):
            ag[t][k].start()

    def ag_forward(t):
        ag_rows(t, 1, ROWS).wait_recv()
        ag[t][5].start()
        ag[t][6].start()

    def ag_pair(t):
        ag_rows(t, 2, ROWS).wait_recv()
        ag[t][7].start()
        ag[t][8].start()

    def ag_last(t):
        ag_rows(t, 5, ROWS).wait_recv()
        ag[t][9].start()
        ag[t][10].start()

    def ag_rows(t, k, n):
        ref = rows.at[t, 0:n]
        return remote(ref, ref, ag_s.at[0], ag_r.at[gather_slot(t, k)], sib)

    def tile_copies(send, recv, ss, rs, chip_tiles):
        cps = {}
        for fx, fy, fc in rels:
            where = dev(fx, fy, fc)
            qq = 2 * where[1] + where[2] // 2
            src = send.at[qq] if chip_tiles else send.at[where[1] * 4 + where[2]]
            cps[fx, fy, fc] = remote(src, recv.at[me], ss.at[0], rs.at[0 if chip_tiles else fx + 2 * fy], where)
        return cps

    gate_cps = tile_copies(gsend, grecv, gs_sem, gr_sem, False)
    dg_cps = tile_copies(dsend, drecv, gs_sem, dd_r, True)
    chips = (q0, qx, qy, qd)
    OWN, X, Y, DI = 0, 1, 2, 3
    first = (X, Y)
    second = (Y, X)

    def rs_slot(n, k):
        if k >= 8:
            kind = (k - 8) % 3
            group = 2 if kind == 0 else 1
        else:
            group = 0 if k // 2 == DI else 1
            if n == 1 and k // 2 in (X, Y):
                group = 3 if k == 2 * X else 4 if k == 2 * Y + 1 else 5
        return (-1, 1, 7)[n] + group

    def rs_wait(n, k, count):
        ref = pair.at[n, 0, 0:2] if count == 2 else pair.at[n, :, 0:3] if count == 6 else pair.at[n, 0, 0]
        remote(ref, ref, rs_s.at[0], rs_r.at[rs_slot(n, k)], sib).wait_recv()

    def rs_copies(n):
        def cp(k, src, dst, where):
            return remote(src, dst, rs_s.at[0], rs_r.at[rs_slot(n, k)], where)
        cps = [cp(2 * k + h, part.at[n, 1 - c, h, chips[k]], pair.at[n, h, chips[k]], sib) for k in range(4) for h in range(2)]
        for h in range(2):
            one, two = (xn, yn) if h == 0 else (yn, xn)
            cps += [cp(8 + 3 * h, s1.at[n, h, 0], r1.at[n, h, 0], one), cp(9 + 3 * h, s1.at[n, h, 1], r1.at[n, h, 1], one),
                    cp(10 + 3 * h, s2.at[n, h], r2.at[n, h], two)]
        return cps

    rsc = [rs_copies(n) for n in range(3)]

    def rs_pair(n, k):
        rsc[n][2 * k].start()
        rsc[n][2 * k + 1].start()

    def chip_sum(n, h, k):
        return part[n, c, h, chips[k]] + pair[n, h, chips[k]]

    def rs_far(n):
        rs_wait(n, 2 * DI, 2)
        for h in range(2):
            s1[n, h, 0] = chip_sum(n, h, DI)
            rsc[n][8 + 3 * h].start()

    def rs_near(n, h):
        k = first[h]
        rs_wait(n, 2 * k + h, 1)
        s1[n, h, 1] = chip_sum(n, h, k)
        rsc[n][9 + 3 * h].start()

    def rs_second(n):
        rs_wait(n, 2 * Y, 2)
        rs_wait(n, 8, 2)
        for h in range(2):
            k = second[h]
            s2[n, h] = chip_sum(n, h, k) + r1[n, h, 0]
            rsc[n][10 + 3 * h].start()

    def rs_final(n, out_ref):
        rs_wait(n, 2 * OWN, 6)
        for h in range(2):
            total = chip_sum(n, h, OWN) + r1[n, h, 1] + r2[n, h]
            out_ref[:, h * HALF:(h + 1) * HALF] = total.astype(BF)

    def head_copy(src, dst, slot, where):
        return remote(src, dst, hd_s.at[0], hd_r.at[slot], where)

    wo_cps = [head_copy(wo.at[h, r:r + 64], wo_in.at[h, r:r + 64], h, (xn, yn)[h]) for r in (0, 64) for h in range(2)]
    ctx_cps = [head_copy(ctx.at[q], ctx_in.at[h, i], 2 + h, (xn, yn)[h])
               for h, qn in ((0, qx), (1, qy)) for i, q in ((0, qn), (1, qd))]

    def gate_table(k):
        tiles = grecv.at[0:1 if k == OWN else 2]
        remote(tiles, tiles, gs_sem.at[0], gr_sem.at[k], sib).wait_recv()
        q = chips[k]
        t0, t1 = grecv[2 * q], grecv[2 * q + 1]
        tile = jnp.concatenate([jnp.concatenate([t0[:, :ROWS], t1[:, :ROWS]], axis=1),
                                jnp.concatenate([t0[:, ROWS:], t1[:, ROWS:]], axis=1)], axis=0)
        gt[pl.ds(pl.multiple_of(q * 128, 128), 128), :] = jnp.concatenate([tile, jnp.zeros((120, 128), F32)], axis=0).T

    def pick(tile, e):
        lane = lax.broadcasted_iota(jnp.int32, tile.shape, 1)
        return jnp.sum(jnp.where(lane == e, tile, 0.0), axis=1, keepdims=True)

    def accumulate(n, q, val):
        for cc in range(2):
            for h in range(2):
                part[n, cc, h, q] += val[cc * 64:(cc + 1) * 64, h * HALF:(h + 1) * HALF]

    def experts(step, hooks):
        def body(e, carry):
            step(e)
            for at, fn in hooks.items():
                @pl.when(e == at)
                def _():
                    fn()
            return carry
        lax.fori_loop(0, EXP, body, 0)

    def chip_rows(k):
        return pl.ds(pl.multiple_of(chips[k] * 128, 128), 128)

    def forward(ks, load=False):
        def stack(ref, *at):
            return jnp.concatenate([ref[(*at, chip_rows(k), slice(None))] for k in ks], axis=0)

        def step(e):
            if load:
                pltpu.make_async_copy(wg_hbm.at[0:3], wg.at[0:3], w_sem.at[1 + e]).wait()

            def put(ref, val):
                for i, k in enumerate(ks):
                    ref[e, chip_rows(k), :] = val[i * 128:(i + 1) * 128]

            xs = stack(rows, XT)
            a = jnp.dot(xs, wg[e], preferred_element_type=F32)
            b = jnp.dot(xs, wu[e], preferred_element_type=F32)
            tile = stack(gt)
            mark = pick(tile, e + 4) > 0.5
            sg = jax.nn.sigmoid(a)
            ac = a * sg
            put(act, jnp.where(mark, ac, 0.0))
            put(gfac, jnp.where(mark, b * sg * (1.0 + a * (1.0 - sg)), 0.0))
            hh = jnp.where(mark, ac * b, 0.0).astype(BF)
            put(hid, hh)
            ob = jnp.dot(hh, wd[e], preferred_element_type=F32).astype(BF)
            put(osv, ob)
            yb = pick(tile, e) * ob.astype(F32)
            for i, k in enumerate(ks):
                accumulate(1, chips[k], yb[i * 128:(i + 1) * 128])
        return step

    def backward(qa, qb, base, gates):
        sl = pl.ds(pl.multiple_of(base, 256), 256)

        def step(e):
            g = pick(gt[sl, :], e)
            dyf = rows[DY, sl, :].astype(F32)
            do = (g * dyf).astype(BF)
            dh = lax.dot_general(do, wd[e], NT, preferred_element_type=F32).astype(BF).astype(F32)
            da = (dh * gfac[e, sl, :]).astype(BF)
            db = (dh * act[e, sl, :]).astype(BF)
            dag[e, sl, :] = da
            dbg[e, sl, :] = db
            if gates:
                lane = lax.broadcasted_iota(jnp.int32, (256, 128), 1)
                for r in (slice(0, 256), slice(256, 512)):
                    dg = jnp.sum(rows[DY, r, :].astype(F32) * osv[e, r, :].astype(F32), axis=1, keepdims=True)
                    dgs[r, :] += jnp.where(lane == e, dg, 0.0)
            dx = (lax.dot_general(da, wg[e], NT, preferred_element_type=F32)
                  + lax.dot_general(db, wu[e], NT, preferred_element_type=F32)).astype(BF).astype(F32)
            accumulate(2, qa, dx[0:128])
            accumulate(2, qb, dx[128:256])
        return step

    def attention_context():
        ag_rows(XA, 0, 4 * ROWS).wait_recv()
        causal_r = lax.broadcasted_iota(jnp.int32, (256, 128), 0) % 128
        causal_c = lax.broadcasted_iota(jnp.int32, (256, 128), 1)
        keep = (causal_r >= causal_c) & (causal_r // 64 == causal_c // 64)
        qkv = lax.dot_general(rows[XA], wqkv[...], NT, preferred_element_type=F32).astype(BF)
        qkvs = [qkv[q * 128:(q + 1) * 128] for q in range(4)]
        scs = [lax.dot_general(jnp.concatenate([v[:, 0:64], v[:, 64:128]], axis=0), v[:, 128:192], NT,
                               preferred_element_type=F32) * (64 ** -0.5) for v in qkvs]
        scs = [jnp.where(keep, sc, -1e30) for sc in scs]
        mxs = [jnp.max(sc, axis=1, keepdims=True) for sc in scs]
        exs = [jnp.exp(sc - mx) for sc, mx in zip(scs, mxs)]
        sms = [jnp.sum(ex, axis=1, keepdims=True) for ex in exs]
        prs = [(ex / sm).astype(BF) for ex, sm in zip(exs, sms)]
        ctxs = [jnp.dot(pr, v[:, 192:256], preferred_element_type=F32).astype(BF) for pr, v in zip(prs, qkvs)]
        for q, v in enumerate(ctxs):
            ctx[q] = jnp.concatenate([v[0:128], v[128:256]], axis=1)

    def attention_out():
        for h in range(2):
            head_copy(wo_in.at[h], wo_in.at[h], h, sib).wait_recv()
            both = ctx_in.at[h]
            head_copy(both, both, 2 + h, sib).wait_recv()
            for i, k in ((0, OWN), (1, second[h])):
                out = (jnp.dot(ctx[chips[k]], wo[h], preferred_element_type=F32)
                       + jnp.dot(ctx_in[h, i], wo_in[h], preferred_element_type=F32))
                for cc in range(2):
                    part[0, cc, h, chips[k]] = out[cc * 64:(cc + 1) * 64]
        for h in range(2):
            rsc[0][2 * OWN + h].start()
            rsc[0][2 * second[h] + h].start()

    def leave_attention():
        ref = pair.at[0, 0]
        remote(ref, ref, rs_s.at[0], rs_r.at[rs_slot(0, 2 * OWN)], sib).wait_recv()
        for h, dst in ((0, toy), (1, tox)):
            dst[:, D:D + HALF] = chip_sum(0, h, second[h])
            own_at[:, h * HALF:(h + 1) * HALF] = chip_sum(0, h, OWN)

    def leave_dx():
        n = 2
        rs_wait(n, 2 * OWN, 6)
        rs_wait(n, 8, 2)
        for h in range(2):
            cols = slice(h * HALF, (h + 1) * HALF)
            near = chip_sum(n, h, first[h])
            far = chip_sum(n, h, second[h]) + r1[n, h, 0]
            tox[:, cols] = near if h == 0 else far
            toy[:, cols] = far if h == 0 else near
            own_dx[:, cols] = chip_sum(n, h, OWN)

    pltpu.make_async_copy(x_hbm, rows.at[XT, own], in_sem.at[0]).wait()
    for e in range(EXP):
        for cp in expert_load(e):
            cp.start()
    for cp in wload:
        cp.start()
    pl.semaphore_wait(barrier, len(rels))
    ag_own(XT)
    for cp in tables:
        cp.wait()

    exp_row = lax.broadcasted_iota(jnp.int32, (32, ROWS), 0)
    table = jnp.zeros((32, ROWS), F32)
    marks = jnp.zeros((32, ROWS), F32)
    for j in range(TOPK):
        hit = exp_row == idx_ref[j:j + 1, :]
        table = table + jnp.where(hit, gate_ref[j:j + 1, :], 0.0)
        marks = marks + jnp.where(hit, 1.0, 0.0)
    wide = jnp.concatenate([table, marks], axis=1)
    for d in range(8):
        gsend[d] = wide[d * EXP:(d + 1) * EXP, :]
    grecv[me] = gsend[me]
    for cp in gate_cps.values():
        cp.start()
    pltpu.make_async_copy(wg_hbm.at[0, 0:4 * ROWS], wg.at[0, 0:4 * ROWS], in_sem.at[3]).wait()
    ag_own(XA)
    dgs[...] = jnp.zeros((TOK, 128), F32)
    part[1] = jnp.zeros(part.shape[1:], F32)
    part[2] = jnp.zeros(part.shape[1:], F32)
    gate_table(OWN)
    ag[XT][0].wait_recv()
    experts(forward([OWN], True), {2: lambda: ag_forward(XT)})
    rs_pair(1, OWN)
    ag_pair(XT)
    gate_table(X)
    gate_table(Y)
    ag_own_a(DY)
    ag[XT][7].wait_recv()
    ag[XT][8].wait_recv()
    experts(forward([X, Y]), {0: lambda: (ag_forward(XA), ag_own_b(DY)), 1: lambda: ag_pair(XA), 2: lambda: (ag_last(XT), ag_forward(DY))})
    rs_pair(1, X)
    rs_pair(1, Y)
    gate_table(DI)
    pltpu.make_async_copy(wg_hbm.at[0, 0:768], wg.at[0, 0:768], w_sem.at[0]).wait()
    for cp in wo_cps[:2]:
        cp.start()
    ag_rows(XT, 9, ROWS).wait_recv()
    experts(forward([DI]), {1: lambda: (rs_near(1, 0), rs_near(1, 1), ag_last(XA)), 2: lambda: ag_pair(DY)})
    rs_pair(1, DI)
    ag_last(DY)
    attention_context()
    rs_far(1)
    for cp in ctx_cps + wo_cps[2:]:
        cp.start()
    ag_rows(DY, 0, 4 * ROWS).wait_recv()
    dyall[...] = rows[DY]
    experts(backward(2 * (1 - y), 2 * (1 - y) + 1, (1 - y) * 256, True), {3: lambda: rs_second(1)})
    rs_pair(2, DI)
    rs_pair(2, Y)
    for q in range(4):
        dsend[q] = dgs[q * 128:(q + 1) * 128, :].T[0:EXP, :]
    drecv[me] = dsend[q0]
    for cp in dg_cps.values():
        cp.start()
    experts(backward(2 * y, 2 * y + 1, y * 256, False), {0: lambda: rs_far(2)})
    rs_pair(2, X)
    rs_pair(2, OWN)
    attention_out()
    rs_wait_dg = drecv.at[0:7]
    remote(rs_wait_dg, rs_wait_dg, gs_sem.at[0], dd_r.at[0], sib).wait_recv()
    both = jnp.concatenate([drecv[d] for d in range(8)], axis=0)
    mine = jnp.where(c == 0, both[:, 0:ROWS], both[:, ROWS:128])
    for j in range(TOPK):
        hit = exp_row == idx_ref[j:j + 1, :]
        dg_out[j:j + 1, :] = jnp.sum(jnp.where(hit, mine, 0.0), axis=0, keepdims=True)
    rs_final(1, y_out)
    leave_attention()
    xt[...] = rows[XT].T
    leave_dx()

    for ref, sem in ((rows.at[:, 0:7 * ROWS], ag_s), (act.at[:, 0:7 * ROWS], rs_s), (gt.at[0:56], gs_sem), (rows.at[:, 0:ROWS], hd_s)):
        remote(ref, ref, sem.at[0], gr_sem.at[0], sib).wait_send()


def exchange(x, dy, xa, idx, gates, wg, wu, wd, wq, wk, wv, wo):
    any_spec = pl.BlockSpec(memory_space=pl.ANY)
    vmem = pl.BlockSpec(memory_space=pltpu.VMEM)
    dma = pltpu.SemaphoreType.DMA
    return pl.pallas_call(
        exchange_kernel,
        name='exchange',
        out_shape=[pltpu.VMEM((ROWS, D), BF), pltpu.VMEM((TOPK, ROWS), F32)] + [pltpu.VMEM((ROWS, D + HALF), F32)] * 2 + [pltpu.VMEM((ROWS, D), F32)] * 2 + [pltpu.VMEM((D, TOK), BF), pltpu.VMEM((TOK, D), BF)]
        + [pltpu.VMEM((EXP, TOK, FF), BF)] * 3 + [pltpu.VMEM((TOK, 128), F32)],
        in_specs=[any_spec] * 12,
        out_specs=[vmem] * 12,
        scratch_shapes=[
            pltpu.VMEM((TOPK, ROWS), jnp.int32), pltpu.VMEM((TOPK, ROWS), F32),
            pltpu.VMEM((3, TOK, D), BF),
            pltpu.VMEM((EXP, D, FF), BF), pltpu.VMEM((EXP, D, FF), BF), pltpu.VMEM((EXP, FF, D), BF),
            pltpu.VMEM((256, D), BF), pltpu.VMEM((2, 128, HALF), BF), pltpu.VMEM((2, 128, HALF), BF),
            pltpu.VMEM((4, 128, 128), BF), pltpu.VMEM((2, 2, 128, 128), BF),
            pltpu.VMEM((EXP, TOK, D), BF),
            pltpu.VMEM((EXP, TOK, FF), F32), pltpu.VMEM((EXP, TOK, FF), F32),
            pltpu.VMEM((8, EXP, 128), F32), pltpu.VMEM((8, EXP, 128), F32),
            pltpu.VMEM((TOK, 128), F32), pltpu.VMEM((4, EXP, 128), F32), pltpu.VMEM((8, EXP, 128), F32),
            pltpu.VMEM((3, 2, 2, 4, ROWS, HALF), F32), pltpu.VMEM((3, 2, 4, ROWS, HALF), F32),
            pltpu.VMEM((3, 2, 2, ROWS, HALF), F32), pltpu.VMEM((3, 2, 2, ROWS, HALF), F32),
            pltpu.VMEM((3, 2, ROWS, HALF), F32), pltpu.VMEM((3, 2, ROWS, HALF), F32),
            dma((4,)), dma((1 + EXP,)), dma((1,)), dma((4,)),
            dma((1,)), dma((10,)), dma((1,)), dma((15,)), dma((1,)), dma((1,)), dma((4,)),
        ],
        compiler_params=pltpu.CompilerParams(collective_id=0, has_side_effects=True, vmem_limit_bytes=50 * 1024 * 1024),
    )(x, dy, xa, idx, gates, wg, wu, wd, wq, wk, wv, wo)


def grads_kernel(xt_ref, dy_ref, gt_ref, h_ref, da_ref, db_ref, y_in, dg_in, dwg_out, dwu_out, dwd_out, y_out, dg_out,
                 gate_buf, up_buf, down_buf, sem, small_sem):
    small = [pltpu.make_async_copy(y_in, y_out, small_sem.at[0]), pltpu.make_async_copy(dg_in, dg_out, small_sem.at[1])]
    for cp in small:
        cp.start()

    def leave(e, slot, n):
        buf, out = ((gate_buf, dwg_out), (up_buf, dwu_out), (down_buf, dwd_out))[n]
        return pltpu.make_async_copy(buf.at[slot], out.at[e], sem.at[n, slot])

    def body(e, carry):
        slot = e % 2

        @pl.when(e >= 2)
        def _():
            for n in range(3):
                leave(e - 2, slot, n).wait()
        gate_buf[slot] = jnp.dot(xt_ref[...], da_ref[e], preferred_element_type=F32)
        leave(e, slot, 0).start()
        up_buf[slot] = jnp.dot(xt_ref[...], db_ref[e], preferred_element_type=F32)
        leave(e, slot, 1).start()
        lane = lax.broadcasted_iota(jnp.int32, (TOK, 128), 1)
        g = jnp.sum(jnp.where(lane == e, gt_ref[...], 0.0), axis=1, keepdims=True)
        do = (g * dy_ref[...].astype(F32)).astype(BF)
        down_buf[slot] = lax.dot_general(h_ref[e], do, TN, preferred_element_type=F32)
        leave(e, slot, 2).start()
        return carry

    lax.fori_loop(0, EXP, body, 0)
    for e in (EXP - 2, EXP - 1):
        for n in range(3):
            leave(e, e % 2, n).wait()
    for cp in small:
        cp.wait()


def weight_grads(*args):
    sds = jax.ShapeDtypeStruct
    args = [pltpu.with_memory_space_constraint(v, pltpu.VMEM) for v in args]
    return pl.pallas_call(
        grads_kernel,
        name='weight_grads',
        out_shape=[sds((EXP, D, FF), F32), sds((EXP, D, FF), F32), sds((EXP, FF, D), F32),
                   sds((ROWS, D), BF), sds((TOPK, ROWS), F32)],
        in_specs=[pl.BlockSpec(memory_space=pltpu.VMEM)] * 8,
        out_specs=[pl.BlockSpec(memory_space=pl.ANY)] * 5,
        scratch_shapes=[pltpu.VMEM((2, D, FF), F32), pltpu.VMEM((2, D, FF), F32), pltpu.VMEM((2, FF, D), F32),
                        pltpu.SemaphoreType.DMA((3, 2)), pltpu.SemaphoreType.DMA((2,))],
        cost_estimate=pl.CostEstimate(flops=3 * 2 * EXP * TOK * D * FF, bytes_accessed=34 * 1024 * 1024, transcendentals=0),
        compiler_params=pltpu.CompilerParams(vmem_limit_bytes=40 * 1024 * 1024),
    )(*args)


def combine_kernel(dx_ref, at_ref, x_ref, y_ref, dx_out, at_out, dx_buf, at_buf, sem):
    dx_cp = pltpu.make_async_copy(dx_buf, dx_out, sem.at[0])
    at_cp = pltpu.make_async_copy(at_buf, at_out, sem.at[1])
    dx_buf[...] = (dx_ref[...] + x_ref[:, 0:D] + y_ref[:, 0:D]).astype(BF)
    dx_cp.start()
    at_buf[:, 0:HALF] = (at_ref[:, 0:HALF] + y_ref[:, D:D + HALF]).astype(BF)
    at_buf[:, HALF:D] = (at_ref[:, HALF:D] + x_ref[:, D:D + HALF]).astype(BF)
    at_cp.start()
    dx_cp.wait()
    at_cp.wait()


def combine(*args):
    sds = jax.ShapeDtypeStruct
    args = [pltpu.with_memory_space_constraint(v, pltpu.VMEM) for v in args]
    return pl.pallas_call(combine_kernel, name='combine', out_shape=[sds((ROWS, D), BF)] * 2,
                          in_specs=[pl.BlockSpec(memory_space=pltpu.VMEM)] * 4,
                          out_specs=[pl.BlockSpec(memory_space=pl.ANY)] * 2,
                          scratch_shapes=[pltpu.VMEM((ROWS, D), BF), pltpu.VMEM((ROWS, D), BF), pltpu.SemaphoreType.DMA((2,))])(*args)


def solution(mesh):
    def local_step(x_tokens, expert_idx, gate_vals, dy_tokens, w_gate, w_up, w_down, x_attn, w_query, w_key, w_value, w_out):
        y_p, dg_p, to_x, to_y, own_dx, own_at, xt, dyall, h, da, db, gt = exchange(
            x_tokens, dy_tokens, x_attn.reshape(ROWS, D), expert_idx.T, gate_vals.T, w_gate, w_up, w_down,
            w_query.transpose(1, 2, 0).reshape(128, D), w_key.transpose(1, 2, 0).reshape(64, D),
            w_value.transpose(1, 2, 0).reshape(64, D), w_out.reshape(128, D))
        from_x = lax.ppermute(to_x, GROUP_AXES, [(g, g ^ 2) for g in range(8)])
        from_y = lax.ppermute(to_y, GROUP_AXES, [(g, g ^ 4) for g in range(8)])
        dwg, dwu, dwd, y_t, dg = weight_grads(xt, dyall, gt, h, da, db, y_p, dg_p)
        dx_t, at = combine(own_dx, own_at, from_x, from_y)
        return y_t, dx_t, dg.T, dwg, dwu, dwd, at.reshape(1, ROWS, D)

    spec_rows = P(TOKEN_AXES, None)
    spec_seqs = P(TOKEN_AXES, None, None)
    spec_experts = P(GROUP_AXES, None, None)
    spec_heads = P(None, GROUP_AXES, None)
    return jax.shard_map(local_step, mesh=mesh,
                         in_specs=(spec_rows, spec_rows, spec_rows, spec_rows, spec_experts, spec_experts, spec_experts, spec_seqs, spec_heads, spec_heads, spec_heads, spec_experts),
                         out_specs=(spec_rows, spec_rows, spec_rows, spec_seqs, spec_seqs, spec_seqs, spec_seqs),
                         check_vma=False)
```
